8 devices in a mesh: dp: 1 (over z), sp: 8 (over x, y, core).
Axes of the slice: x: 2, y: 2, z: 1, core: 2. Of those that a mesh axis runs over, the one named last changes fastest.
Arguments:
- x: bfloat16 [8192, 2048], P(('dp', 'sp'))
- gain: bfloat16 [2048], replicated
- wq: bfloat16 [2048, 2048], P('sp')
- wk: bfloat16 [2048, 256], P('sp')
- wv: bfloat16 [2048, 256], P('sp')
- wo: bfloat16 [2048, 2048], P('sp')
Outputs:
- output: bfloat16 [8192, 2048], P(('dp', 'sp'))
All inputs are finite; a program needn't handle non-finite values.
Results may differ from the reference program's by a relative error of at most 0.012.
Values are sent between devices in bfloat16 or wider.
A program may use at most 2 GiB of HBM per device.

```python
import jax
import jax.numpy as jnp
from jax import lax

ROWS = 8192
D = 2048
HEADS = 8
KV_HEADS = 1
HEAD = 256
THETA = 10000


def setup_inputs(seed: int = 0, part: int = 0) -> dict:
    kx, kn, kq, kk, kv, ko = jax.random.split(jax.random.key(seed), 6)

    def weights(key, rows, columns):
        return jax.random.normal(key, (rows, columns), jnp.float32) * rows**-0.5

    drawn = {
        "x": jax.random.normal(jax.random.fold_in(kx, part), (ROWS, D), jnp.float32),
        "gain": 1 + 0.1 * jax.random.normal(kn, (D,), jnp.float32),
        "wq": 2 * weights(kq, D, HEADS * HEAD),
        "wk": 2 * weights(kk, D, KV_HEADS * HEAD),
        "wv": 4 * weights(kv, D, KV_HEADS * HEAD),
        "wo": weights(ko, HEADS * HEAD, D),
    }
    return {k: v.astype(jnp.bfloat16) for k, v in drawn.items()}


def normed(x, gain):
    wide = x.astype(jnp.float32)
    scale = lax.rsqrt(jnp.mean(wide * wide, -1, keepdims=True) + 1e-6)
    return (wide * scale * gain.astype(jnp.float32)).astype(jnp.bfloat16)


def turned(t, place, theta):
    half = t.shape[-1] // 2
    angle = place.astype(jnp.float32)[:, None] * theta ** (-jnp.arange(half, dtype=jnp.float32) / half)
    cos, sin = jnp.cos(angle)[:, None], jnp.sin(angle)[:, None]
    a, b = t[..., :half].astype(jnp.float32), t[..., half:].astype(jnp.float32)
    return jnp.concatenate([a * cos - b * sin, b * cos + a * sin], -1).astype(jnp.bfloat16)


def matmul(a, w):
    return jnp.dot(a, w, preferred_element_type=jnp.float32).astype(jnp.bfloat16)


def einsum(form, a, b):
    return jnp.einsum(form, a.astype(jnp.float32), b.astype(jnp.float32))


def attention(q, k, v):
    scores = einsum("tgsd,ugd->gstu", q, k) * q.shape[-1] ** -0.5
    token = jnp.arange(q.shape[0])
    scores = jnp.where(token[:, None] >= token, scores, -jnp.inf)
    weights = jax.nn.softmax(scores, -1).astype(jnp.bfloat16)
    return einsum("gstu,ugd->tgsd", weights, v).astype(jnp.bfloat16)


def reference(x, gain, wq, wk, wv, wo):
    a, place = normed(x, gain), jnp.arange(ROWS)
    q = turned(matmul(a, wq).reshape(ROWS, HEADS, HEAD), place, THETA).reshape(ROWS, KV_HEADS, -1, HEAD)
    k = turned(matmul(a, wk).reshape(ROWS, KV_HEADS, HEAD), place, THETA)
    v = matmul(a, wv).reshape(ROWS, KV_HEADS, HEAD)
    seen = attention(q, k, v).reshape(ROWS, HEADS * HEAD)
    return (x.astype(jnp.float32) + jnp.dot(seen, wo, preferred_element_type=jnp.float32)).astype(jnp.bfloat16)
```

```python
import functools

import jax
import jax.numpy as jnp
from jax import lax
from jax.experimental import pallas as pl
from jax.experimental.pallas import tpu as pltpu
from jax.sharding import PartitionSpec as P

NEG = -1e30
HIDDEN = 2 * NEG
LOG2E = 1.4426950408889634
HEAD = 256
THETA = 10000
W = 512
B = 512
F32, BF16 = jnp.float32, jnp.bfloat16


def _dot(a, b, ca, cb):
    return lax.dot_general(a, b, (((ca,), (cb,)), ((), ())), preferred_element_type=F32)


def _kernel(x_h, gain_ref, freq_ref, wq_h, wk_h, wv_h, wo_h, y_h,
            a_s, x_s, wq_s, w_s, kv_s, q_s, wo_s, cos_s, sin_s, mix_s, top_s,
            loc, s_a, r_a, s_w, r_w, s_q, r_q, s_kv, r_kv, f_kv, g_kv, s_wo, r_wo, f_wo, g_wo, s_o, r_o):
    me = lax.axis_index("sp")
    c = lax.rem(me, 2)
    p = lax.div(me, 2)
    px, py = lax.div(p, 2), lax.rem(p, 2)
    cx, cy, cd = 2 * (1 - px) + py, 2 * px + 1 - py, 2 * (1 - px) + 1 - py
    chips = (cx, cy, cd)
    mate = 2 * p + 1 - c
    xn, yn = 2 * cx + c, 2 * cy + c
    own = 1024

    def remote(src, dst, ss, rs, dev):
        return pltpu.make_async_remote_copy(src_ref=src, dst_ref=dst, send_sem=ss, recv_sem=rs, device_id={"sp": dev},
                                            device_id_type=pl.DeviceIdType.MESH)

    def arrived(ref, sem):
        pltpu.make_async_copy(ref, ref, sem).wait()

    def rows(i, n):
        return pl.ds(pl.multiple_of(i * n, n), n)

    loads = [pltpu.make_async_copy(x_h.at[rows(i, 256), :], x_s.at[rows(i, 256), :], loc.at[i]) for i in range(4)]
    for t in loads:
        t.start()

    barrier = pltpu.get_barrier_semaphore()
    for dev in (mate, 2 * cx, 2 * cx + 1, 2 * cy, 2 * cy + 1):
        pl.semaphore_signal(barrier, inc=1, device_id={"sp": dev}, device_id_type=pl.DeviceIdType.MESH)
    pl.semaphore_wait(barrier, 5)

    w_mine = w_s.at[rows(me, 256), :]
    for t, w_h in enumerate((wk_h, wv_h)):
        remote(w_h, w_mine, s_w.at[t], r_w.at[c], 2 * cx + t).start()
        remote(w_h, w_mine, s_w.at[2 + t], r_w.at[2 + c], 2 * cy + t).start()

        @pl.when(c == t)
        def _():
            pltpu.make_async_copy(w_h, w_mine, loc.at[4]).start()

        @pl.when(c != t)
        def _():
            remote(w_h, w_mine, s_w.at[4], r_w.at[6], mate).start()

    def wq_part(core, j):
        return wq_h.at[:, pl.ds(pl.multiple_of((4 * core + j) * 256, 256), 256)]

    def wq_own(j, t):
        dst = wq_s.at[j, rows(me, 256), :]
        return [remote(wq_part(t, j), dst, s_q.at[j, t], r_q.at[j, c], 2 * cx + t),
                remote(wq_part(t, j), dst, s_q.at[j, 2 + t], r_q.at[j, 2 + c], 2 * cy + t)]

    def wq_mate(j):
        return remote(wq_part(1 - c, j), wq_s.at[j, rows(me, 256), :], s_q.at[j, 4], r_q.at[j, 6], mate)

    def wq_local(j):
        return pltpu.make_async_copy(wq_part(c, j), wq_s.at[j, rows(me, 256), :], loc.at[5 + j])

    def wq_relay(j):
        fx, fy = wq_s.at[j, rows(2 * cx, 256), :], wq_s.at[j, rows(2 * cy + 1, 256), :]
        return [remote(fx, fx, s_q.at[j, 5], r_q.at[j, 4], yn), remote(fy, fy, s_q.at[j, 6], r_q.at[j, 5], xn)]

    def start(ts):
        for t in ts:
            t.start()

    def a_rows(i):
        return a_s.at[pl.ds(pl.multiple_of(c * own + i * 256, 256), 256), :]

    def a_copy(i):
        return remote(a_rows(i), a_rows(i), s_a.at[i], r_a.at[i], mate)

    gain = gain_ref[...].astype(F32)
    for i in range(4):
        loads[i].wait()

        def norm(n, _):
            at = pl.multiple_of(i * 256 + n * 64, 64)
            wide = x_s[pl.ds(at, 64), :].astype(F32)
            scale = lax.rsqrt(jnp.mean(wide * wide, -1, keepdims=True) + 1e-6)
            a_s[pl.ds(pl.multiple_of(c * own + at, 64), 64), :] = (wide * scale * gain).astype(BF16)

        lax.fori_loop(0, 4, norm, None)
        a_copy(i).start()

    def angles(n, _):
        at = pl.multiple_of(n * 64, 64)
        place = (p * 2048 + at + lax.broadcasted_iota(jnp.int32, (64, 128), 0)).astype(F32)
        angle = place * freq_ref[...]
        cos_s[pl.ds(at, 64), :] = jnp.cos(angle)
        sin_s[pl.ds(at, 64), :] = jnp.sin(angle)

    lax.fori_loop(0, 16, angles, None)

    for i in range(4):
        arrived(w_s.at[rows(0, 256), :], r_w.at[i])
    fx, fy = w_s.at[rows(2 * cx, 256), :], w_s.at[rows(2 * cy + 1, 256), :]
    relays_w = [remote(fx, fx, s_w.at[5], r_w.at[4], yn), remote(fy, fy, s_w.at[6], r_w.at[5], xn)]
    start(relays_w)
    start(wq_own(0, 0) + wq_own(0, 1) + wq_own(1, 0))
    for j in range(4):
        wq_mate(j).start()
        wq_local(j).start()
    lax.fori_loop(16, 32, angles, None)
    for i in range(4):
        arrived(a_rows(0), r_a.at[i])
        arrived(a_rows(0), s_a.at[i])
    arrived(w_mine, loc.at[4])
    for i in (6, 4, 5):
        arrived(w_mine, r_w.at[i])

    def turn(r, at):
        r = r.astype(BF16).astype(F32)
        lo, hi = r[:, :128], r[:, 128:]
        cos, sin = cos_s[pl.ds(at, r.shape[0]), :], sin_s[pl.ds(at, r.shape[0]), :]
        return jnp.concatenate([lo * cos - hi * sin, hi * cos + lo * sin], -1).astype(BF16)

    def kv_fwd(n):
        ref = kv_s.at[c, n]
        return remote(ref, ref, f_kv.at[n], g_kv.at[n], mate)

    def kv_own(i, way):
        ref = kv_s.at[c, 4 * p + i]
        return remote(ref, ref, s_kv.at[4 * way + i], r_kv.at[4 * way + i], (xn, yn)[way])

    def kvproj(i, _):
        at = pl.multiple_of(i * B, B)
        r = _dot(a_s[pl.ds(at, B), :], w_s[...], 1, 0)

        @pl.when(c == 0)
        def _():
            kv_s[0, 4 * p + i] = turn(r, at)

        @pl.when(c == 1)
        def _():
            v = r.astype(BF16)
            kv_s[1, 4 * p + i, :256, :] = v[:256].T
            kv_s[1, 4 * p + i, 256:, :] = v[256:].T

        kv_fwd(4 * p + i).start()

    lax.fori_loop(0, 4, kvproj, None)

    e = HEAD**-0.5 * LOG2E
    ones = jnp.ones((8, 256), BF16)

    def strips(n, todo):
        scores = [_dot(kv_s[0, n], q_s[pl.ds(at, W), :], 1, 1) for at, _, _ in todo]
        weights, keeps = [], []
        for (at, new, edge), s in zip(todo, scores):
            if edge:
                s = jnp.where(lax.broadcasted_iota(jnp.int32, (B, W), 1) >= lax.broadcasted_iota(jnp.int32, (B, W), 0), s, HIDDEN)
            top = s.max(axis=0, keepdims=True)
            if not new:
                old = top_s[:, pl.ds(at, W)]
                top = jnp.maximum(old, top)
                keeps.append(jnp.exp2((old - top) * e))
            else:
                keeps.append(None)
            top_s[:, pl.ds(at, W)] = top
            weights.append(jnp.exp2((s - top) * e).astype(BF16))
        for (at, _, _), w, keep in zip(todo, weights, keeps):
            va = jnp.concatenate([kv_s[1, n, :256, :], ones], 0)
            vb = jnp.concatenate([kv_s[1, n, 256:, :], ones], 0)
            more = _dot(va, w[:256], 1, 0) + _dot(vb, w[256:], 1, 0)
            mix_s[:, pl.ds(at, W)] = more if keep is None else mix_s[:, pl.ds(at, W)] * keep + more

    for i in range(4):
        arrived(kv_s.at[0, 0], g_kv.at[4 * p + i])

    def head(j, _):
        @pl.when(j < 4)
        def _():
            for i in (0, 1, 2, 3):
                arrived(wq_s.at[j, rows(0, 256), :], r_q.at[j, i])
            start(wq_relay(j))

            @pl.when(j < 3)
            def _():
                start(wq_own(j + 1, 1))

            @pl.when(j < 2)
            def _():
                start(wq_own(j + 2, 0))

            @pl.when(j == 2)
            def _():
                start([kv_own(0, 0), kv_own(0, 1)])

            @pl.when(j == 3)
            def _():
                start([kv_own(i, way) for i in (1, 2, 3) for way in (0, 1)])

        @pl.when(j > 0)
        def _():
            base = (j - 1) * 2048
            at = [pl.multiple_of(base + t * W, W) for t in range(4)]
            for n in range(4):
                strips(4 * p + n, [(at[t], n == 0, t == n) for t in range(n, 4)])

        @pl.when(j < 4)
        def _():
            arrived(wq_s.at[j, rows(0, 256), :], loc.at[5 + j])
            for i in (6, 4, 5):
                arrived(wq_s.at[j, rows(0, 256), :], r_q.at[j, i])

            def project(n, _):
                at = pl.multiple_of(n * 512, 512)
                r = _dot(a_s[pl.ds(at, 512), :], wq_s[j], 1, 0)
                q_s[pl.ds(pl.multiple_of(j * 2048 + at, 512), 512), :] = turn(r, at)

            lax.fori_loop(0, 4, project, None)

    lax.fori_loop(0, 5, head, None)

    def wo_rows(dev, half):
        return pl.ds(pl.multiple_of(dev * 256 + half * 128, 128), 128)

    def wo_own(half, way):
        return remote(wo_h.at[rows(half, 128), :], wo_s.at[wo_rows(me, half), :], s_wo.at[2 * way + half], r_wo.at[2 * way + half],
                      (xn, yn, mate)[way])

    def wo_local(half):
        return pltpu.make_async_copy(wo_h.at[rows(half, 128), :], wo_s.at[wo_rows(me, half), :], loc.at[9 + half])

    def wo_fwd(k, half):
        ref = wo_s.at[wo_rows((xn, yn, 2 * cd + c)[k], half), :]
        return remote(ref, ref, f_wo.at[2 * k + half], g_wo.at[2 * k + half], mate)

    def wo_relay(way):
        ref = wo_s.at[wo_rows((xn, yn)[way], way), :]
        return remote(ref, ref, s_wo.at[6 + way], r_wo.at[6 + way], (yn, xn)[way])

    wo_any = wo_s.at[rows(0, 128), :]
    piece_any = kv_s.at[0, 0]

    def place_of(s):
        way, i = lax.rem(s, 2), lax.div(s, 2)
        near = jnp.where(way == 0, cx, cy)
        chip = jnp.where(s < 8, near, cd)
        i = jnp.where(s < 8, i, s - 8)
        return 4 * chip + i, chip

    def take(s):
        n, _ = place_of(s)
        near = 4 * lax.rem(s, 2) + lax.div(s, 2)
        slot = jnp.where(s < 8, near, s)
        arrived(piece_any, r_kv.at[slot])
        kv_fwd(n).start()
        ref = kv_s.at[c, n]

        @pl.when((lax.rem(s, 2) == 0) & (s < 4))
        def _():
            i = lax.div(s, 2)
            remote(ref, ref, s_kv.at[8 + i], r_kv.at[8 + i], yn).start()

        @pl.when((lax.rem(s, 2) == 1) & (s >= 4) & (s < 8))
        def _():
            i = lax.div(s, 2)
            remote(ref, ref, s_kv.at[8 + i], r_kv.at[8 + i], xn).start()

    take(jnp.int32(0))

    def other(s, _):
        @pl.when(s < 11)
        def _():
            take(s + 1)

        @pl.when(s == 3)
        def _():
            for half in range(2):
                wo_local(half).start()
                for way in range(3):
                    wo_own(half, way).start()

        @pl.when(s == 8)
        def _():
            for way in range(2):
                arrived(wo_any, r_wo.at[2 * way + way])
                wo_relay(way).start()
                wo_fwd(way, way).start()

        @pl.when(s == 9)
        def _():
            for way in range(2):
                arrived(wo_any, r_wo.at[2 * way + 1 - way])
                wo_fwd(way, 1 - way).start()

        n, chip = place_of(s)
        arrived(piece_any, g_kv.at[n])

        @pl.when(chip < p)
        def _():
            def group(g, _):
                strips(n, [(pl.multiple_of(g * 4096 + t * W, W), False, False) for t in range(8)])

            lax.fori_loop(0, 2, group, None)

    lax.fori_loop(0, 12, other, None)

    for half in range(2):
        arrived(wo_any, r_wo.at[6 + half])
        wo_fwd(2, half).start()

    def seen(j, half, u):
        at = pl.multiple_of(j * 2048 + half * own + u * 512, 512)
        m = mix_s[:, pl.ds(at, 512)]
        return (m[:256] * (1 / m[256:257])).astype(BF16).T

    def o_copy(j):
        return remote(a_s.at[own:, pl.ds(pl.multiple_of(j * 256, 256), 256)],
                      a_s.at[:own, pl.ds(pl.multiple_of((4 * c + j) * 256, 256), 256)], s_o.at[j], r_o.at[j], mate)

    def finish_mate(j, _):
        for u in range(2):
            a_s[own + u * 512 : own + (u + 1) * 512, pl.ds(pl.multiple_of(j * 256, 256), 256)] = seen(j, 1 - c, u)
        o_copy(j).start()

    def finish_own(j, _):
        for u in range(2):
            a_s[u * 512 : (u + 1) * 512, pl.ds(pl.multiple_of((4 * c + j) * 256, 256), 256)] = seen(j, c, u)

    lax.fori_loop(0, 4, finish_mate, None)
    lax.fori_loop(0, 4, finish_own, None)
    for half in range(2):
        arrived(wo_any, loc.at[9 + half])
        arrived(wo_any, r_wo.at[4 + half])
        for k in range(3):
            arrived(wo_any, g_wo.at[2 * k + half])
    for j in range(4):
        arrived(a_s.at[:own, :256], r_o.at[j])

    def y_copy(i):
        return pltpu.make_async_copy(x_s.at[rows(i, 256), :], y_h.at[rows(i, 256), :], loc.at[i])

    def out(i, _):
        at = pl.multiple_of(i * 256, 256)
        for n in range(4):
            cols = slice(512 * n, 512 * (n + 1))
            r = _dot(a_s[pl.ds(at, 256), :], wo_s[:, cols], 1, 0)
            x_s[pl.ds(at, 256), cols] = (x_s[pl.ds(at, 256), cols].astype(F32) + r).astype(BF16)
        y_copy(i).start()

    lax.fori_loop(0, 4, out, None)

    def left(ref, sem):
        pltpu.make_async_copy(ref, ref, sem).wait()

    for i in range(4):
        left(a_s.at[:own, :256], s_o.at[i])
        for k in range(7):
            left(wq_s.at[0, rows(0, 256), :], s_q.at[i, k])
    for i in range(7):
        left(w_mine, s_w.at[i])
    for i in range(12):
        left(piece_any, s_kv.at[i])
    for i in range(16):
        left(piece_any, f_kv.at[i])
    for i in range(8):
        left(wo_any, s_wo.at[i])
    for i in range(6):
        left(wo_any, f_wo.at[i])
    for i in range(4):
        y_copy(i).wait()


def solution(mesh):
    def step(x, gain, wq, wk, wv, wo):
        half = HEAD // 2
        freq = (THETA ** (-jnp.arange(half, dtype=F32) / half))[None]
        hbm, vmem = pl.BlockSpec(memory_space=pl.ANY), pl.BlockSpec(memory_space=pltpu.VMEM)
        dma = pltpu.SemaphoreType.DMA
        return pl.pallas_call(
            _kernel,
            out_shape=jax.ShapeDtypeStruct(x.shape, x.dtype),
            in_specs=[hbm, vmem, vmem, hbm, hbm, hbm, hbm],
            out_specs=hbm,
            scratch_shapes=[
                pltpu.VMEM((2048, 2048), BF16),
                pltpu.VMEM((1024, 2048), BF16),
                pltpu.VMEM((4, 2048, 256), BF16),
                pltpu.VMEM((2048, 256), BF16),
                pltpu.VMEM((2, 16, B, 256), BF16),
                pltpu.VMEM((4 * 2048, 256), BF16),
                pltpu.VMEM((2048, 2048), BF16),
                pltpu.VMEM((2048, 128), F32),
                pltpu.VMEM((2048, 128), F32),
                pltpu.VMEM((264, 4 * 2048), F32),
                pltpu.VMEM((1, 4 * 2048), F32),
                dma((11,)),
                dma((4,)), dma((4,)),
                dma((7,)), dma((7,)),
                dma((4, 7)), dma((4, 7)),
                dma((12,)), dma((12,)), dma((16,)), dma((16,)),
                dma((8,)), dma((8,)), dma((6,)), dma((6,)),
                dma((4,)), dma((4,)),
            ],
            compiler_params=pltpu.CompilerParams(collective_id=0, has_side_effects=True, vmem_limit_bytes=67043328),
            name="half_layer",
        )(x, gain[None], freq, wq, wk, wv, wo)

    tokens, whole = P(("dp", "sp"), None), P("sp", None)
    return jax.shard_map(
        step,
        mesh=mesh,
        in_specs=(tokens, P(None), whole, whole, whole, whole),
        out_specs=tokens,
        check_vma=False,
    )
```

```python
import jax
import jax.numpy as jnp
import numpy as np
from jax import lax
from jax.experimental import pallas as pl
from jax.experimental.pallas import tpu as pltpu
from jax.sharding import PartitionSpec as P

NEG = -1e30
HIDDEN = 2 * NEG
LOG2E = 1.4426950408889634
HEAD = 256
THETA = 10000
W = 512
B = 512
F32, BF16 = jnp.float32, jnp.bfloat16


def _dot(a, b, ca, cb):
    return lax.dot_general(a, b, (((ca,), (cb,)), ((), ())), preferred_element_type=F32)


def _kernel(x_h, gain_ref, freq_ref, wq_h, wk_h, wv_h, wo_h, y_h,
            a_s, x_s, wq_s, w_s, kv_s, q_s, wo_s, cos_s, sin_s, mix_s, top_s,
            loc, s_a, r_a, s_w, r_w, s_q, r_q, s_kv, r_kv, f_kv, g_kv, s_wo, r_wo, f_wo, g_wo, s_o, r_o):
    me = lax.axis_index("sp")
    c = lax.rem(me, 2)
    p = lax.div(me, 2)
    px, py = lax.div(p, 2), lax.rem(p, 2)
    cx, cy, cd = 2 * (1 - px) + py, 2 * px + 1 - py, 2 * (1 - px) + 1 - py
    chips = (cx, cy, cd)
    mate = 2 * p + 1 - c
    xn, yn = 2 * cx + c, 2 * cy + c
    own = 1024

    def remote(src, dst, ss, rs, dev):
        return pltpu.make_async_remote_copy(src_ref=src, dst_ref=dst, send_sem=ss, recv_sem=rs, device_id={"sp": dev},
                                            device_id_type=pl.DeviceIdType.MESH)

    def arrived(ref, sem):
        pltpu.make_async_copy(ref, ref, sem).wait()

    def rows(i, n):
        return pl.ds(pl.multiple_of(i * n, n), n)

    loads = [pltpu.make_async_copy(x_h.at[rows(i, 256), :], x_s.at[rows(i, 256), :], loc.at[i]) for i in range(4)]
    for t in loads:
        t.start()

    barrier = pltpu.get_barrier_semaphore()
    for dev in (mate, 2 * cx, 2 * cx + 1, 2 * cy, 2 * cy + 1):
        pl.semaphore_signal(barrier, inc=1, device_id={"sp": dev}, device_id_type=pl.DeviceIdType.MESH)
    pl.semaphore_wait(barrier, 5)

    w_mine = w_s.at[rows(me, 256), :]
    for t, w_h in enumerate((wk_h, wv_h)):
        remote(w_h, w_mine, s_w.at[t], r_w.at[c], 2 * cx + t).start()
        remote(w_h, w_mine, s_w.at[2 + t], r_w.at[2 + c], 2 * cy + t).start()

        @pl.when(c == t)
        def _():
            pltpu.make_async_copy(w_h, w_mine, loc.at[4]).start()

        @pl.when(c != t)
        def _():
            remote(w_h, w_mine, s_w.at[4], r_w.at[6], mate).start()

    def wq_part(core, j):
        return wq_h.at[:, pl.ds(pl.multiple_of((4 * core + j) * 256, 256), 256)]

    def wq_own(j, t):
        dst = wq_s.at[j, rows(me, 256), :]
        return [remote(wq_part(t, j), dst, s_q.at[j, t], r_q.at[j, c], 2 * cx + t),
                remote(wq_part(t, j), dst, s_q.at[j, 2 + t], r_q.at[j, 2 + c], 2 * cy + t)]

    def wq_mate(j):
        return remote(wq_part(1 - c, j), wq_s.at[j, rows(me, 256), :], s_q.at[j, 4], r_q.at[j, 6], mate)

    def wq_local(j):
        return pltpu.make_async_copy(wq_part(c, j), wq_s.at[j, rows(me, 256), :], loc.at[5 + j])

    def wq_relay(j):
        fx, fy = wq_s.at[j, rows(2 * cx, 256), :], wq_s.at[j, rows(2 * cy + 1, 256), :]
        return [remote(fx, fx, s_q.at[j, 5], r_q.at[j, 4], yn), remote(fy, fy, s_q.at[j, 6], r_q.at[j, 5], xn)]

    def start(ts):
        for t in ts:
            t.start()

    def a_rows(i):
        return a_s.at[pl.ds(pl.multiple_of(c * own + i * 256, 256), 256), :]

    def a_copy(i):
        return remote(a_rows(i), a_rows(i), s_a.at[i], r_a.at[i], mate)

    start(wq_own(0, 0))
    gain = gain_ref[...].astype(F32)[None]
    for i in range(4):
        loads[i].wait()

        def norm(n, _):
            at = pl.multiple_of(i * 256 + n * 64, 64)
            wide = x_s[pl.ds(at, 64), :].astype(F32)
            scale = lax.rsqrt(jnp.mean(wide * wide, -1, keepdims=True) + 1e-6)
            a_s[pl.ds(pl.multiple_of(c * own + at, 64), 64), :] = (wide * scale * gain).astype(BF16)

        lax.fori_loop(0, 4, norm, None)
        a_copy(i).start()

    def angles(n, _):
        at = pl.multiple_of(n * 64, 64)
        place = (p * 2048 + at + lax.broadcasted_iota(jnp.int32, (64, 128), 0)).astype(F32)
        angle = place * freq_ref[...]
        cos_s[pl.ds(at, 64), :] = jnp.cos(angle)
        sin_s[pl.ds(at, 64), :] = jnp.sin(angle)

    lax.fori_loop(0, 16, angles, None)

    for i in range(4):
        arrived(w_s.at[rows(0, 256), :], r_w.at[i])
    fx, fy = w_s.at[rows(2 * cx, 256), :], w_s.at[rows(2 * cy + 1, 256), :]
    relays_w = [remote(fx, fx, s_w.at[5], r_w.at[4], yn), remote(fy, fy, s_w.at[6], r_w.at[5], xn)]
    start(relays_w)
    start(wq_own(0, 1))
    for j in range(4):
        wq_mate(j).start()
        wq_local(j).start()
    lax.fori_loop(16, 32, angles, None)
    for i in range(4):
        arrived(a_rows(0), r_a.at[i])
        arrived(a_rows(0), s_a.at[i])
    arrived(w_mine, loc.at[4])
    for i in (6, 4, 5):
        arrived(w_mine, r_w.at[i])

    def turn(r, at):
        r = r.astype(BF16).astype(F32)
        lo, hi = r[:, :128], r[:, 128:]
        cos, sin = cos_s[pl.ds(at, r.shape[0]), :], sin_s[pl.ds(at, r.shape[0]), :]
        return jnp.concatenate([lo * cos - hi * sin, hi * cos + lo * sin], -1).astype(BF16)

    def kv_fwd(n):
        ref = kv_s.at[c, n]
        return remote(ref, ref, f_kv.at[n], g_kv.at[n], mate)

    def kv_own(i, way):
        ref = kv_s.at[c, 4 * p + i]
        return remote(ref, ref, s_kv.at[4 * way + i], r_kv.at[4 * way + i], (xn, yn)[way])

    def kvproj(i, _):
        at = pl.multiple_of(i * B, B)
        r = _dot(a_s[pl.ds(at, B), :], w_s[...], 1, 0)

        @pl.when(c == 0)
        def _():
            kv_s[0, 4 * p + i] = turn(r, at)

        @pl.when(c == 1)
        def _():
            v = r.astype(BF16)
            kv_s[1, 4 * p + i, :256, :] = v[:256].T
            kv_s[1, 4 * p + i, 256:, :] = v[256:].T

        kv_fwd(4 * p + i).start()

    lax.fori_loop(0, 4, kvproj, None)

    e = HEAD**-0.5 * LOG2E
    ones = jnp.ones((8, 256), BF16)

    def strips(n, todo):
        scores = [_dot(kv_s[0, n], q_s[pl.ds(at, W), :], 1, 1) for at, _, _ in todo]
        weights, keeps = [], []
        for (at, new, edge), s in zip(todo, scores):
            if edge:
                s = jnp.where(lax.broadcasted_iota(jnp.int32, (B, W), 1) >= lax.broadcasted_iota(jnp.int32, (B, W), 0), s, HIDDEN)
            top = s.max(axis=0, keepdims=True)
            if not new:
                old = top_s[:, pl.ds(at, W)]
                top = jnp.maximum(old, top)
                keeps.append(jnp.exp2((old - top) * e))
            else:
                keeps.append(None)
            top_s[:, pl.ds(at, W)] = top
            weights.append(jnp.exp2((s - top) * e).astype(BF16))
        for (at, _, _), w, keep in zip(todo, weights, keeps):
            va = jnp.concatenate([kv_s[1, n, :256, :], ones], 0)
            vb = jnp.concatenate([kv_s[1, n, 256:, :], ones], 0)
            more = _dot(va, w[:256], 1, 0) + _dot(vb, w[256:], 1, 0)
            mix_s[:, pl.ds(at, W)] = more if keep is None else mix_s[:, pl.ds(at, W)] * keep + more

    for i in range(4):
        arrived(kv_s.at[0, 0], g_kv.at[4 * p + i])

    def head(j, _):
        @pl.when(j < 4)
        def _():
            for i in (0, 1, 2, 3):
                arrived(wq_s.at[j, rows(0, 256), :], r_q.at[j, i])
            start(wq_relay(j))

            @pl.when(j == 0)
            def _():
                start(wq_own(1, 0))

            @pl.when(j < 3)
            def _():
                start(wq_own(j + 1, 1))

            @pl.when(j < 2)
            def _():
                start(wq_own(j + 2, 0))

            for way, at_0 in enumerate((px == 0, py == 0)):

                @pl.when((j == 3) & at_0)
                def _():
                    start([kv_own(i, way) for i in range(4)])

        @pl.when(j > 0)
        def _():
            base = (j - 1) * 2048
            at = [pl.multiple_of(base + t * W, W) for t in range(4)]
            for n in range(4):
                strips(4 * p + n, [(at[t], n == 0, t == n) for t in range(n, 4)])

        @pl.when(j < 4)
        def _():
            arrived(wq_s.at[j, rows(0, 256), :], loc.at[5 + j])
            for i in (6, 4, 5):
                arrived(wq_s.at[j, rows(0, 256), :], r_q.at[j, i])

            def project(n, _):
                at = pl.multiple_of(n * 512, 512)
                r = _dot(a_s[pl.ds(at, 512), :], wq_s[j], 1, 0)
                q_s[pl.ds(pl.multiple_of(j * 2048 + at, 512), 512), :] = turn(r, at)

            lax.fori_loop(0, 4, project, None)

    lax.fori_loop(0, 5, head, None)

    def wo_rows(dev, half):
        return pl.ds(pl.multiple_of(dev * 256 + half * 128, 128), 128)

    def wo_own(half, way):
        return remote(wo_h.at[rows(half, 128), :], wo_s.at[wo_rows(me, half), :], s_wo.at[2 * way + half], r_wo.at[2 * way + half],
                      (xn, yn, mate)[way])

    def wo_local(half):
        return pltpu.make_async_copy(wo_h.at[rows(half, 128), :], wo_s.at[wo_rows(me, half), :], loc.at[9 + half])

    def wo_fwd(k, half):
        ref = wo_s.at[wo_rows((xn, yn, 2 * cd + c)[k], half), :]
        return remote(ref, ref, f_wo.at[2 * k + half], g_wo.at[2 * k + half], mate)

    def wo_relay(way):
        ref = wo_s.at[wo_rows((xn, yn)[way], way), :]
        return remote(ref, ref, s_wo.at[6 + way], r_wo.at[6 + way], (yn, xn)[way])

    wo_any = wo_s.at[rows(0, 128), :]
    piece_any = kv_s.at[0, 0]

    def place_of(s):
        way, i = lax.rem(s, 2), lax.div(s, 2)
        near = jnp.where(way == 0, cx, cy)
        chip = jnp.where(s < 8, near, cd)
        i = jnp.where(s < 8, i, s - 8)
        return 4 * chip + i, chip

    def take(s):
        n, chip = place_of(s)
        near = 4 * lax.rem(s, 2) + lax.div(s, 2)
        slot = jnp.where(s < 8, near, s)
        ref = kv_s.at[c, n]
        i = lax.div(s, 2)
        odd = lax.rem(s, 2)

        @pl.when(chip < p)
        def _():
            arrived(piece_any, r_kv.at[slot])
            kv_fwd(n).start()

        @pl.when((p == 2) & (odd == 0) & (s < 4) | (p == 3) & (odd == 0) & (s < 8))
        def _():
            remote(ref, ref, s_kv.at[8 + i], r_kv.at[8 + i], yn).start()

        @pl.when((p == 1) & (odd == 1) & (s >= 4) & (s < 8))
        def _():
            remote(ref, ref, s_kv.at[8 + i], r_kv.at[8 + i], xn).start()

    def seen(j, half, u):
        at = pl.multiple_of(j * 2048 + half * own + u * 512, 512)
        m = mix_s[:, pl.ds(at, 512)]
        return (m[:256] * (1 / m[256:257])).astype(BF16).T

    def o_copy(j):
        return remote(a_s.at[own:, pl.ds(pl.multiple_of(j * 256, 256), 256)],
                      a_s.at[:own, pl.ds(pl.multiple_of((4 * c + j) * 256, 256), 256)], s_o.at[j], r_o.at[j], mate)

    def finish_mate(j, _):
        for u in range(2):
            a_s[own + u * 512 : own + (u + 1) * 512, pl.ds(pl.multiple_of(j * 256, 256), 256)] = seen(j, 1 - c, u)
        o_copy(j).start()

    def finish_own(j, _):
        for u in range(2):
            a_s[u * 512 : (u + 1) * 512, pl.ds(pl.multiple_of((4 * c + j) * 256, 256), 256)] = seen(j, c, u)

    take(jnp.int32(0))

    def other(s, _):
        @pl.when(s < 11)
        def _():
            take(s + 1)

        @pl.when(s == 3)
        def _():
            start([wo_own(0, 0), wo_own(1, 1), wo_own(1, 0), wo_own(0, 1)])
            for half in range(2):
                wo_local(half).start()
                wo_own(half, 2).start()

        @pl.when(s == 6)
        def _():
            for way in range(2):
                arrived(wo_any, r_wo.at[2 * way + way])
                wo_relay(way).start()
                wo_fwd(way, way).start()

        @pl.when(s == 9)
        def _():
            for way in range(2):
                arrived(wo_any, r_wo.at[2 * way + 1 - way])
                wo_fwd(way, 1 - way).start()

        @pl.when(s == 10)
        def _():
            for half in range(2):
                arrived(wo_any, r_wo.at[6 + half])
                wo_fwd(2, half).start()

        @pl.when(s == 11)
        def _():
            arrived(wo_any, g_wo.at[0])

        n, chip = place_of(s)

        @pl.when(chip < p)
        def _():
            arrived(piece_any, g_kv.at[n])

        def group(g, _):
            @pl.when(chip < p)
            def _():
                strips(n, [(pl.multiple_of(g * 4096 + t * W, W), False, False) for t in range(8)])

            @pl.when(s == 11)
            def _():
                lax.fori_loop(2 * g, 2 * g + 2, finish_mate, None)

        lax.fori_loop(0, 2, group, None)

    lax.fori_loop(0, 12, other, None)
    lax.fori_loop(0, 4, finish_own, None)
    for half in range(2):
        arrived(wo_any, loc.at[9 + half])
        arrived(wo_any, r_wo.at[4 + half])
        for k in range(3):
            if (k, half) != (0, 0):
                arrived(wo_any, g_wo.at[2 * k + half])
    for j in range(4):
        arrived(a_s.at[:own, :256], r_o.at[j])

    def y_copy(i):
        return pltpu.make_async_copy(x_s.at[rows(i, 256), :], y_h.at[rows(i, 256), :], loc.at[i])

    def out(i, _):
        at = pl.multiple_of(i * 256, 256)
        for n in range(4):
            cols = slice(512 * n, 512 * (n + 1))
            r = _dot(a_s[pl.ds(at, 256), :], wo_s[:, cols], 1, 0)
            x_s[pl.ds(at, 256), cols] = (x_s[pl.ds(at, 256), cols].astype(F32) + r).astype(BF16)
        y_copy(i).start()

    lax.fori_loop(0, 4, out, None)

    def left(ref, sem):
        pltpu.make_async_copy(ref, ref, sem).wait()

    for i in range(4):
        left(a_s.at[:own, :256], s_o.at[i])
        for k in range(7):
            left(wq_s.at[0, rows(0, 256), :], s_q.at[i, k])
    for i in range(7):
        left(w_mine, s_w.at[i])
    for lot, sent in enumerate((px == 0, py == 0, p > 0)):

        @pl.when(sent)
        def _():
            def one(i, _):
                left(piece_any, s_kv.at[4 * lot + i])

            lo, hi = (0, 4) if lot < 2 else (jnp.where(p == 1, 2, 0), jnp.where(p == 2, 2, 4))
            lax.fori_loop(lo, hi, one, None)

    def forwarded(i, _):
        left(piece_any, f_kv.at[i])

    lax.fori_loop(0, 4 * p + 4, forwarded, None)
    for i in range(8):
        left(wo_any, s_wo.at[i])
    for i in range(6):
        left(wo_any, f_wo.at[i])
    for i in range(4):
        y_copy(i).wait()


def solution(mesh):
    def step(x, gain, wq, wk, wv, wo):
        half = HEAD // 2
        freq = np.asarray([THETA ** (-i / half) for i in range(half)], np.float32)[None]
        hbm, vmem = pl.BlockSpec(memory_space=pl.ANY), pl.BlockSpec(memory_space=pltpu.VMEM)
        dma = pltpu.SemaphoreType.DMA
        return pl.pallas_call(
            _kernel,
            out_shape=jax.ShapeDtypeStruct(x.shape, x.dtype),
            in_specs=[hbm, vmem, vmem, hbm, hbm, hbm, hbm],
            out_specs=hbm,
            scratch_shapes=[
                pltpu.VMEM((2048, 2048), BF16),
                pltpu.VMEM((1024, 2048), BF16),
                pltpu.VMEM((4, 2048, 256), BF16),
                pltpu.VMEM((2048, 256), BF16),
                pltpu.VMEM((2, 16, B, 256), BF16),
                pltpu.VMEM((4 * 2048, 256), BF16),
                pltpu.VMEM((2048, 2048), BF16),
                pltpu.VMEM((2048, 128), F32),
                pltpu.VMEM((2048, 128), F32),
                pltpu.VMEM((264, 4 * 2048), F32),
                pltpu.VMEM((1, 4 * 2048), F32),
                dma((11,)),
                dma((4,)), dma((4,)),
                dma((7,)), dma((7,)),
                dma((4, 7)), dma((4, 7)),
                dma((12,)), dma((12,)), dma((16,)), dma((16,)),
                dma((8,)), dma((8,)), dma((6,)), dma((6,)),
                dma((4,)), dma((4,)),
            ],
            compiler_params=pltpu.CompilerParams(collective_id=0, has_side_effects=True, vmem_limit_bytes=67043328),
            name="half_layer",
        )(x, gain, freq, wq, wk, wv, wo)

    tokens, whole = P(("dp", "sp"), None), P("sp", None)
    return jax.shard_map(
        step,
        mesh=mesh,
        in_specs=(tokens, P(None), whole, whole, whole, whole),
        out_specs=tokens,
        check_vma=False,
    )
```

```python
import jax
import jax.numpy as jnp
import numpy as np
from jax import lax
from jax.experimental import pallas as pl
from jax.experimental.pallas import tpu as pltpu
from jax.sharding import PartitionSpec as P

NEG = -1e30
HIDDEN = 2 * NEG
LOG2E = 1.4426950408889634
HEAD = 256
THETA = 10000
W = 256
B = 1024
F32, BF16 = jnp.float32, jnp.bfloat16


def _dot(a, b, ca, cb):
    return lax.dot_general(a, b, (((ca,), (cb,)), ((), ())), preferred_element_type=F32)


def _kernel(x_h, gain_ref, freq_ref, wq_h, wk_h, wv_h, wo_h, y_h,
            a_s, x_s, wq_s, w_s, kv_s, q_s, cos_s, sin_s, acc_s, top_s, sum_s,
            loc, s_a, r_a, s_w, r_w, s_q, r_q, s_kv, r_kv, f_kv, g_kv, s_wo, r_wo, f_wo, g_wo, s_o, r_o, free):
    me = lax.axis_index("sp")
    c = lax.rem(me, 2)
    p = lax.div(me, 2)
    px, py = lax.div(p, 2), lax.rem(p, 2)
    cx, cy, cd = 2 * (1 - px) + py, 2 * px + 1 - py, 2 * (1 - px) + 1 - py
    chips = (cx, cy, cd)
    mate = 2 * p + 1 - c
    xn, yn = 2 * cx + c, 2 * cy + c
    own = 1024

    def remote(src, dst, ss, rs, dev):
        return pltpu.make_async_remote_copy(src_ref=src, dst_ref=dst, send_sem=ss, recv_sem=rs, device_id={"sp": dev},
                                            device_id_type=pl.DeviceIdType.MESH)

    def arrived(ref, sem):
        pltpu.make_async_copy(ref, ref, sem).wait()

    def rows(i, n):
        return pl.ds(pl.multiple_of(i * n, n), n)

    loads = [pltpu.make_async_copy(x_h.at[rows(i, 256), :], x_s.at[rows(i, 256), :], loc.at[i]) for i in range(4)]
    for t in loads:
        t.start()

    barrier = pltpu.get_barrier_semaphore()
    for dev in (mate, 2 * cx, 2 * cx + 1, 2 * cy, 2 * cy + 1):
        pl.semaphore_signal(barrier, inc=1, device_id={"sp": dev}, device_id_type=pl.DeviceIdType.MESH)
    pl.semaphore_wait(barrier, 5)

    w_mine = w_s.at[rows(me, 256), :]
    for t, w_h in enumerate((wk_h, wv_h)):
        remote(w_h, w_mine, s_w.at[t], r_w.at[c], 2 * cx + t).start()
        remote(w_h, w_mine, s_w.at[2 + t], r_w.at[2 + c], 2 * cy + t).start()

        @pl.when(c == t)
        def _():
            pltpu.make_async_copy(w_h, w_mine, loc.at[4]).start()

        @pl.when(c != t)
        def _():
            remote(w_h, w_mine, s_w.at[4], r_w.at[6], mate).start()

    def wq_part(core, j):
        return wq_h.at[:, pl.ds(pl.multiple_of((4 * core + j) * 256, 256), 256)]

    def wq_own(j, t):
        dst = wq_s.at[j, rows(me, 256), :]
        return [remote(wq_part(t, j), dst, s_q.at[j, t], r_q.at[j, c], 2 * cx + t),
                remote(wq_part(t, j), dst, s_q.at[j, 2 + t], r_q.at[j, 2 + c], 2 * cy + t)]

    def wq_mate(j):
        return remote(wq_part(1 - c, j), wq_s.at[j, rows(me, 256), :], s_q.at[j, 4], r_q.at[j, 6], mate)

    def wq_local(j):
        return pltpu.make_async_copy(wq_part(c, j), wq_s.at[j, rows(me, 256), :], loc.at[5 + j])

    def wq_relay(j):
        fx, fy = wq_s.at[j, rows(2 * cx, 256), :], wq_s.at[j, rows(2 * cy + 1, 256), :]
        return [remote(fx, fx, s_q.at[j, 5], r_q.at[j, 4], yn), remote(fy, fy, s_q.at[j, 6], r_q.at[j, 5], xn)]

    def start(ts):
        for t in ts:
            t.start()

    def a_rows(i):
        return a_s.at[pl.ds(pl.multiple_of(c * own + i * 256, 256), 256), :]

    def a_copy(i):
        return remote(a_rows(i), a_rows(i), s_a.at[i], r_a.at[i], mate)

    start(wq_own(0, 0))
    gain = gain_ref[...].astype(F32)[None]
    for i in range(4):
        loads[i].wait()

        def norm(n, _):
            at = pl.multiple_of(i * 256 + n * 64, 64)
            wide = x_s[pl.ds(at, 64), :].astype(F32)
            scale = lax.rsqrt(jnp.mean(wide * wide, -1, keepdims=True) + 1e-6)
            a_s[pl.ds(pl.multiple_of(c * own + at, 64), 64), :] = (wide * scale * gain).astype(BF16)

        lax.fori_loop(0, 4, norm, None)
        a_copy(i).start()

    def angles(n, _):
        at = pl.multiple_of(n * 64, 64)
        place = (p * 2048 + at + lax.broadcasted_iota(jnp.int32, (64, 128), 0)).astype(F32)
        angle = place * freq_ref[...]
        cos_s[pl.ds(at, 64), :] = jnp.cos(angle)
        sin_s[pl.ds(at, 64), :] = jnp.sin(angle)

    lax.fori_loop(0, 16, angles, None)

    for i in range(4):
        arrived(w_s.at[rows(0, 256), :], r_w.at[i])
    fx, fy = w_s.at[rows(2 * cx, 256), :], w_s.at[rows(2 * cy + 1, 256), :]
    relays_w = [remote(fx, fx, s_w.at[5], r_w.at[4], yn), remote(fy, fy, s_w.at[6], r_w.at[5], xn)]
    start(relays_w)
    start(wq_own(0, 1))
    for j in range(4):
        wq_mate(j).start()
        wq_local(j).start()
    lax.fori_loop(16, 32, angles, None)
    for i in range(4):
        arrived(a_rows(0), r_a.at[i])
        arrived(a_rows(0), s_a.at[i])
    arrived(w_mine, loc.at[4])
    for i in (6, 4, 5):
        arrived(w_mine, r_w.at[i])

    def turn(r, at):
        r = r.astype(BF16).astype(F32)
        lo, hi = r[:, :128], r[:, 128:]
        cos, sin = cos_s[pl.ds(at, r.shape[0]), :], sin_s[pl.ds(at, r.shape[0]), :]
        return jnp.concatenate([lo * cos - hi * sin, hi * cos + lo * sin], -1).astype(BF16)

    def piece(n):
        return kv_s.at[c, rows(n, B), :]

    def kv_fwd(n):
        return remote(piece(n), piece(n), f_kv.at[n], g_kv.at[n], mate)

    def kv_own(i, way):
        ref = piece(2 * p + i)
        return remote(ref, ref, s_kv.at[2 * way + i], r_kv.at[2 * way + i], (xn, yn)[way])

    def kvproj(i, _):
        at = pl.multiple_of(i * 512, 512)
        to = pl.ds(pl.multiple_of(p * 2048 + at, 512), 512)
        r = _dot(a_s[pl.ds(at, 512), :], w_s[...], 1, 0)

        @pl.when(c == 0)
        def _():
            kv_s[0, to, :] = turn(r, at)

        @pl.when(c == 1)
        def _():
            kv_s[1, to, :] = r.astype(BF16)

        @pl.when(lax.rem(i, 2) == 1)
        def _():
            kv_fwd(2 * p + lax.div(i, 2)).start()

    lax.fori_loop(0, 4, kvproj, None)

    e = HEAD**-0.5 * LOG2E

    def strips(todo, new):
        scores = [[_dot(q_s[pl.ds(at, W), :], kv_s[0, pl.ds(k, n), :], 1, 1) for k, n in keys] for at, keys, _ in todo]
        weights, keeps = [], []
        for (at, keys, edge), parts in zip(todo, scores):
            s = [t[:, i : i + 128] for t in parts for i in range(0, t.shape[1], 128)]
            if edge:
                gap = lax.broadcasted_iota(jnp.int32, (W, 128), 0) - lax.broadcasted_iota(jnp.int32, (W, 128), 1)
                s[-2] = jnp.where(gap >= 0, s[-2], HIDDEN)
                s[-1] = jnp.where(gap >= 128, s[-1], HIDDEN)
            most = s[0]
            for t in s[1:]:
                most = jnp.maximum(most, t)
            top = jnp.broadcast_to(most.max(axis=1, keepdims=True), (W, 128))
            if not new:
                old = top_s[pl.ds(at, W), :]
                top = jnp.maximum(old, top)
                keeps.append(jnp.exp2((old - top) * e))
            top_s[pl.ds(at, W), :] = top
            w = [jnp.exp2((t - top) * e) for t in s]
            total = w[0]
            for t in w[1:]:
                total = total + t
            sum_s[pl.ds(at, W), :] = total if new else sum_s[pl.ds(at, W), :] * keeps[-1] + total
            weights.append(jnp.concatenate([t.astype(BF16) for t in w], 1))
        for i, (at, keys, _) in enumerate(todo):
            more, col = None, 0
            for k, n in keys:
                r = _dot(weights[i][:, col : col + n], kv_s[1, pl.ds(k, n), :], 1, 0)
                more, col = r if more is None else more + r, col + n
            acc_s[pl.ds(at, W), :] = more if new else acc_s[pl.ds(at, W), :] * jnp.concatenate([keeps[i], keeps[i]], 1) + more

    for i in range(2):
        arrived(piece(0), g_kv.at[2 * p + i])

    def head(j, _):
        @pl.when(j < 4)
        def _():
            for i in (0, 1, 2, 3):
                arrived(wq_s.at[j, rows(0, 256), :], r_q.at[j, i])
            start(wq_relay(j))

            @pl.when(j == 0)
            def _():
                start(wq_own(1, 0))

            @pl.when(j < 3)
            def _():
                start(wq_own(j + 1, 1))

            @pl.when(j < 2)
            def _():
                start(wq_own(j + 2, 0))

            for way, at_0 in enumerate((px == 0, py == 0)):

                @pl.when((j == 3) & at_0)
                def _():
                    start([kv_own(i, way) for i in range(2)])

        @pl.when(j > 0)
        def _():
            base, first = (j - 1) * 2048, pl.multiple_of(p * 2048, 2048)
            strips([(pl.multiple_of(base + i * W, W), [(first, (i + 1) * W)], True) for i in range(7, -1, -1)], True)

        @pl.when(j < 4)
        def _():
            arrived(wq_s.at[j, rows(0, 256), :], loc.at[5 + j])
            for i in (6, 4, 5):
                arrived(wq_s.at[j, rows(0, 256), :], r_q.at[j, i])

            def project(n, _):
                at = pl.multiple_of(n * 512, 512)
                r = _dot(a_s[pl.ds(at, 512), :], wq_s[j], 1, 0)
                q_s[pl.ds(pl.multiple_of(j * 2048 + at, 512), 512), :] = turn(r, at)

            lax.fori_loop(0, 4, project, None)

    lax.fori_loop(0, 5, head, None)

    for j in range(4):
        for k in (5, 6):
            arrived(wq_s.at[0, rows(0, 256), :], s_q.at[j, k])
    for dev in (xn, yn, mate):
        pl.semaphore_signal(free, inc=1, device_id={"sp": dev}, device_id_type=pl.DeviceIdType.MESH)

    def wo_rows(dev, half):
        return pl.ds(pl.multiple_of(dev * 256 + half * 128, 128), 128)

    def wo_own(half, way):
        return remote(wo_h.at[rows(half, 128), :], a_s.at[wo_rows(me, half), :], s_wo.at[2 * way + half], r_wo.at[2 * way + half],
                      (xn, yn, mate)[way])

    def wo_local(half):
        return pltpu.make_async_copy(wo_h.at[rows(half, 128), :], a_s.at[wo_rows(me, half), :], loc.at[9 + half])

    def wo_fwd(k, half):
        ref = a_s.at[wo_rows((xn, yn, 2 * cd + c)[k], half), :]
        return remote(ref, ref, f_wo.at[2 * k + half], g_wo.at[2 * k + half], mate)

    def wo_relay(way):
        ref = a_s.at[wo_rows((xn, yn)[way], way), :]
        return remote(ref, ref, s_wo.at[6 + way], r_wo.at[6 + way], (yn, xn)[way])

    wo_any = a_s.at[rows(0, 128), :]
    piece_any = piece(0)

    def take(k):
        way, i = (k % 2, k // 2) if k < 4 else (2, k - 4)
        chip = chips[way]
        ref = piece(2 * chip + i)
        slot = 2 * way + i

        @pl.when(chip < p)
        def _():
            arrived(piece_any, r_kv.at[slot])
            kv_fwd(2 * chip + i).start()

        if way == 0:

            @pl.when((p == 3) | (p == 2) & (i == 0))
            def _():
                remote(ref, ref, s_kv.at[4 + i], r_kv.at[4 + i], yn).start()

        if way == 1 and i == 1:

            @pl.when(p == 1)
            def _():
                remote(ref, ref, s_kv.at[4 + i], r_kv.at[4 + i], xn).start()

    def o_copy(j):
        h = 4 * c + j
        dst = wq_s.at[lax.div(h, 2), pl.ds(pl.multiple_of(lax.rem(h, 2) * own, own), own), :]
        return remote(q_s.at[pl.ds(pl.multiple_of(j * 2048 + (1 - c) * own, own), own), :], dst, s_o.at[j], r_o.at[j], mate)

    def other(n, _):
        t, g = lax.div(n, 8), lax.rem(n, 8)
        j, half = lax.rem(g, 4), jnp.where(g < 4, 1 - c, c)
        first = pl.multiple_of(j * 2048 + half * own, own)

        @pl.when(n == 0)
        def _():
            take(0)
            take(1)

        @pl.when((n == 0) & (p < 3) | (n == 6) & (p == 3))
        def _():
            take(2)
            take(3)

        @pl.when((n == 6) & (p == 2) | (n == 10) & (p == 3))
        def _():
            take(4)
            take(5)

        @pl.when(n == 1)
        def _():
            pl.semaphore_wait(free, 3)
            start([wo_own(0, 0), wo_own(1, 1), wo_own(1, 0), wo_own(0, 1)])
            for half in range(2):
                wo_local(half).start()
                wo_own(half, 2).start()

        @pl.when(n == 13)
        def _():
            for way in range(2):
                arrived(wo_any, r_wo.at[2 * way + way])
                wo_relay(way).start()
                wo_fwd(way, way).start()

        @pl.when(n == 16)
        def _():
            for way in range(2):
                arrived(wo_any, r_wo.at[2 * way + 1 - way])
                wo_fwd(way, 1 - way).start()

        @pl.when(n == 20)
        def _():
            for half in range(2):
                arrived(wo_any, r_wo.at[6 + half])
                wo_fwd(2, half).start()

        lone = jnp.where(p == 3, cd, jnp.where(p == 1, cy, jnp.where(t == 0, cx, cd)))
        both = (p == 3) & (t < 2)
        n_a, n_b = jnp.where(both, 2 * cx + t, 2 * lone), jnp.where(both, 2 * cy + t, 2 * lone + 1)

        @pl.when((t < p) & (g == 0))
        def _():
            arrived(piece_any, g_kv.at[n_a])
            arrived(piece_any, g_kv.at[n_b])

        @pl.when(t < p)
        def _():
            keys = [(pl.multiple_of(n_a * B, B), B), (pl.multiple_of(n_b * B, B), B)]
            strips([(pl.multiple_of(first + i * W, W), keys, False) for i in range(4)], False)

        def seen(i):
            at = pl.ds(pl.multiple_of(first + i * W, W), W)
            return (acc_s[at, :] * (1 / sum_s[at, :].sum(axis=1, keepdims=True))).astype(BF16)

        @pl.when((t == 2) & (g < 4))
        def _():
            for i in range(4):
                q_s[pl.ds(pl.multiple_of(first + i * W, W), W), :] = seen(i)
            o_copy(j).start()

        @pl.when((t == 2) & (g >= 4))
        def _():
            h = 4 * c + j
            for i in range(4):
                wq_s[lax.div(h, 2), pl.ds(pl.multiple_of(lax.rem(h, 2) * own + i * W, W), W), :] = seen(i)

    lax.fori_loop(0, 24, other, None)
    for half in range(2):
        arrived(wo_any, loc.at[9 + half])
        arrived(wo_any, r_wo.at[4 + half])
        for k in range(3):
            arrived(wo_any, g_wo.at[2 * k + half])
    for j in range(4):
        arrived(q_s.at[:own, :], r_o.at[j])

    def y_copy(i):
        return pltpu.make_async_copy(x_s.at[rows(i, 256), :], y_h.at[rows(i, 256), :], loc.at[i])

    def out(i, _):
        at = pl.multiple_of(i * 256, 256)
        seen = jnp.concatenate([wq_s[h // 2, pl.ds(pl.multiple_of(h % 2 * own + at, 256), 256), :] for h in range(8)], 1)
        for n in range(4):
            cols = slice(512 * n, 512 * (n + 1))
            r = _dot(seen, a_s[:, cols], 1, 0)
            x_s[pl.ds(at, 256), cols] = (x_s[pl.ds(at, 256), cols].astype(F32) + r).astype(BF16)
        y_copy(i).start()

    lax.fori_loop(0, 4, out, None)

    def left(ref, sem):
        pltpu.make_async_copy(ref, ref, sem).wait()

    for i in range(4):
        left(q_s.at[:own, :], s_o.at[i])
        for k in range(5):
            left(wq_s.at[0, rows(0, 256), :], s_q.at[i, k])
    for i in range(7):
        left(w_mine, s_w.at[i])
    for lot, sent in enumerate((px == 0, py == 0, p > 0)):

        @pl.when(sent)
        def _():
            def one(i, _):
                left(piece_any, s_kv.at[2 * lot + i])

            lo, hi = (0, 2) if lot < 2 else (jnp.where(p == 1, 1, 0), jnp.where(p == 2, 1, 2))
            lax.fori_loop(lo, hi, one, None)

    def forwarded(i, _):
        left(piece_any, f_kv.at[i])

    lax.fori_loop(0, 2 * p + 2, forwarded, None)
    for i in range(8):
        left(wo_any, s_wo.at[i])
    for i in range(6):
        left(wo_any, f_wo.at[i])
    for i in range(4):
        y_copy(i).wait()


def solution(mesh):
    def step(x, gain, wq, wk, wv, wo):
        half = HEAD // 2
        freq = np.asarray([THETA ** (-i / half) for i in range(half)], np.float32)[None]
        hbm, vmem = pl.BlockSpec(memory_space=pl.ANY), pl.BlockSpec(memory_space=pltpu.VMEM)
        dma = pltpu.SemaphoreType.DMA
        return pl.pallas_call(
            _kernel,
            out_shape=jax.ShapeDtypeStruct(x.shape, x.dtype),
            in_specs=[hbm, vmem, vmem, hbm, hbm, hbm, hbm],
            out_specs=hbm,
            scratch_shapes=[
                pltpu.VMEM((2048, 2048), BF16),
                pltpu.VMEM((1024, 2048), BF16),
                pltpu.VMEM((4, 2048, 256), BF16),
                pltpu.VMEM((2048, 256), BF16),
                pltpu.VMEM((2, 8192, 256), BF16),
                pltpu.VMEM((4 * 2048, 256), BF16),
                pltpu.VMEM((2048, 128), F32),
                pltpu.VMEM((2048, 128), F32),
                pltpu.VMEM((4 * 2048, 256), F32),
                pltpu.VMEM((4 * 2048, 128), F32),
                pltpu.VMEM((4 * 2048, 128), F32),
                dma((11,)),
                dma((4,)), dma((4,)),
                dma((7,)), dma((7,)),
                dma((4, 7)), dma((4, 7)),
                dma((6,)), dma((6,)), dma((8,)), dma((8,)),
                dma((8,)), dma((8,)), dma((6,)), dma((6,)),
                dma((4,)), dma((4,)),
                pltpu.SemaphoreType.REGULAR,
            ],
            compiler_params=pltpu.CompilerParams(collective_id=0, has_side_effects=True, vmem_limit_bytes=67043328),
            name="half_layer",
        )(x, gain, freq, wq, wk, wv, wo)

    tokens, whole = P(("dp", "sp"), None), P("sp", None)
    return jax.shard_map(
        step,
        mesh=mesh,
        in_specs=(tokens, P(None), whole, whole, whole, whole),
        out_specs=tokens,
        check_vma=False,
    )
```

```python
import jax
import jax.numpy as jnp
import numpy as np
from jax import lax
from jax.experimental import pallas as pl
from jax.experimental.pallas import tpu as pltpu
from jax.sharding import PartitionSpec as P

NEG = -1e30
HIDDEN = 2 * NEG
LOG2E = 1.4426950408889634
HEAD = 256
THETA = 10000
W = 256
B = 1024
F32, BF16 = jnp.float32, jnp.bfloat16


def _dot(a, b, ca, cb):
    return lax.dot_general(a, b, (((ca,), (cb,)), ((), ())), preferred_element_type=F32)


def _kernel(x_h, gain_ref, freq_ref, wq_h, wk_h, wv_h, wo_h, y_h,
            a_s, x_s, wq_s, w_s, kv_s, q_s, cos_s, sin_s, acc_s, top_s, sum_s,
            loc, s_a, r_a, s_w, r_w, s_q, r_q, s_kv, r_kv, f_kv, g_kv, s_wo, r_wo, f_wo, g_wo, s_o, r_o, free):
    me = lax.axis_index("sp")
    c = lax.rem(me, 2)
    p = lax.div(me, 2)
    px, py = lax.div(p, 2), lax.rem(p, 2)
    cx, cy, cd = 2 * (1 - px) + py, 2 * px + 1 - py, 2 * (1 - px) + 1 - py
    chips = (cx, cy, cd)
    mate = 2 * p + 1 - c
    xn, yn = 2 * cx + c, 2 * cy + c
    own = 1024

    def remote(src, dst, ss, rs, dev):
        return pltpu.make_async_remote_copy(src_ref=src, dst_ref=dst, send_sem=ss, recv_sem=rs, device_id={"sp": dev},
                                            device_id_type=pl.DeviceIdType.MESH)

    def arrived(ref, sem):
        pltpu.make_async_copy(ref, ref, sem).wait()

    def rows(i, n):
        return pl.ds(pl.multiple_of(i * n, n), n)

    loads = [pltpu.make_async_copy(x_h.at[rows(i, 256), :], x_s.at[rows(i, 256), :], loc.at[i]) for i in range(4)]
    for t in loads:
        t.start()

    barrier = pltpu.get_barrier_semaphore()
    for dev in (mate, 2 * cx, 2 * cx + 1, 2 * cy, 2 * cy + 1):
        pl.semaphore_signal(barrier, inc=1, device_id={"sp": dev}, device_id_type=pl.DeviceIdType.MESH)
    pl.semaphore_wait(barrier, 5)

    w_mine = w_s.at[rows(me, 256), :]
    for t, w_h in enumerate((wk_h, wv_h)):
        remote(w_h, w_mine, s_w.at[t], r_w.at[c], 2 * cx + t).start()
        remote(w_h, w_mine, s_w.at[2 + t], r_w.at[2 + c], 2 * cy + t).start()

        @pl.when(c == t)
        def _():
            pltpu.make_async_copy(w_h, w_mine, loc.at[4]).start()

        @pl.when(c != t)
        def _():
            remote(w_h, w_mine, s_w.at[4], r_w.at[6], mate).start()

    def wq_part(core, j):
        return wq_h.at[:, pl.ds(pl.multiple_of((4 * core + j) * 256, 256), 256)]

    def wq_own(j, t):
        dst = wq_s.at[j, rows(me, 256), :]
        return [remote(wq_part(t, j), dst, s_q.at[j, t], r_q.at[j, c], 2 * cx + t),
                remote(wq_part(t, j), dst, s_q.at[j, 2 + t], r_q.at[j, 2 + c], 2 * cy + t)]

    def wq_mate(j):
        return remote(wq_part(1 - c, j), wq_s.at[j, rows(me, 256), :], s_q.at[j, 4], r_q.at[j, 6], mate)

    def wq_local(j):
        return pltpu.make_async_copy(wq_part(c, j), wq_s.at[j, rows(me, 256), :], loc.at[5 + j])

    def wq_relay(j):
        fx, fy = wq_s.at[j, rows(2 * cx, 256), :], wq_s.at[j, rows(2 * cy + 1, 256), :]
        return [remote(fx, fx, s_q.at[j, 5], r_q.at[j, 4], yn), remote(fy, fy, s_q.at[j, 6], r_q.at[j, 5], xn)]

    def start(ts):
        for t in ts:
            t.start()

    def a_rows(i):
        return a_s.at[pl.ds(pl.multiple_of(c * own + i * 256, 256), 256), :]

    def a_copy(i):
        return remote(a_rows(i), a_rows(i), s_a.at[i], r_a.at[i], mate)

    start(wq_own(0, 0))
    gain = gain_ref[...].astype(F32)[None]
    for i in range(4):
        loads[i].wait()

        def norm(n, _):
            at = pl.multiple_of(i * 256 + n * 64, 64)
            wide = x_s[pl.ds(at, 64), :].astype(F32)
            scale = lax.rsqrt(jnp.mean(wide * wide, -1, keepdims=True) + 1e-6)
            a_s[pl.ds(pl.multiple_of(c * own + at, 64), 64), :] = (wide * scale * gain).astype(BF16)

        lax.fori_loop(0, 4, norm, None)
        a_copy(i).start()

    def angles(n, _):
        at = pl.multiple_of(n * 64, 64)
        place = (p * 2048 + at + lax.broadcasted_iota(jnp.int32, (64, 128), 0)).astype(F32)
        angle = place * freq_ref[...]
        cos_s[pl.ds(at, 64), :] = jnp.cos(angle)
        sin_s[pl.ds(at, 64), :] = jnp.sin(angle)

    lax.fori_loop(0, 16, angles, None)

    for i in range(4):
        arrived(w_s.at[rows(0, 256), :], r_w.at[i])
    fx, fy = w_s.at[rows(2 * cx, 256), :], w_s.at[rows(2 * cy + 1, 256), :]
    relays_w = [remote(fx, fx, s_w.at[5], r_w.at[4], yn), remote(fy, fy, s_w.at[6], r_w.at[5], xn)]
    start(relays_w)
    start(wq_own(0, 1) + wq_own(1, 0))
    for j in range(4):
        wq_mate(j).start()
        wq_local(j).start()
    lax.fori_loop(16, 32, angles, None)
    for i in range(4):
        arrived(a_rows(0), r_a.at[i])
        arrived(a_rows(0), s_a.at[i])
    arrived(w_mine, loc.at[4])
    for i in (6, 4, 5):
        arrived(w_mine, r_w.at[i])

    def turn(r, at):
        r = r.astype(BF16).astype(F32)
        lo, hi = r[:, :128], r[:, 128:]
        cos, sin = cos_s[pl.ds(at, r.shape[0]), :], sin_s[pl.ds(at, r.shape[0]), :]
        return jnp.concatenate([lo * cos - hi * sin, hi * cos + lo * sin], -1).astype(BF16)

    def piece(n):
        return kv_s.at[c, rows(n, B), :]

    def kv_fwd(n):
        return remote(piece(n), piece(n), f_kv.at[n], g_kv.at[n], mate)

    def kv_own(i, way):
        ref = piece(2 * p + i)
        return remote(ref, ref, s_kv.at[2 * way + i], r_kv.at[2 * way + i], (xn, yn)[way])

    def kvproj(i, _):
        at = pl.multiple_of(i * 512, 512)
        to = pl.ds(pl.multiple_of(p * 2048 + at, 512), 512)
        r = _dot(a_s[pl.ds(at, 512), :], w_s[...], 1, 0)

        @pl.when(c == 0)
        def _():
            kv_s[0, to, :] = turn(r, at)

        @pl.when(c == 1)
        def _():
            kv_s[1, to, :] = r.astype(BF16)

        @pl.when(lax.rem(i, 2) == 1)
        def _():
            kv_fwd(2 * p + lax.div(i, 2)).start()

    lax.fori_loop(0, 4, kvproj, None)

    e = HEAD**-0.5 * LOG2E

    def strips(todo, new):
        scores = [[_dot(q_s[pl.ds(at, W), :], kv_s[0, pl.ds(k, n), :], 1, 1) for k, n in keys] for at, keys, _ in todo]
        weights, keeps = [], []
        for (at, keys, edge), parts in zip(todo, scores):
            s = [t[:, i : i + 128] for t in parts for i in range(0, t.shape[1], 128)]
            if edge:
                gap = lax.broadcasted_iota(jnp.int32, (W, 128), 0) - lax.broadcasted_iota(jnp.int32, (W, 128), 1)
                s[-2] = jnp.where(gap >= 0, s[-2], HIDDEN)
                s[-1] = jnp.where(gap >= 128, s[-1], HIDDEN)
            most = s[0]
            for t in s[1:]:
                most = jnp.maximum(most, t)
            top = jnp.broadcast_to(most.max(axis=1, keepdims=True), (W, 128))
            if not new:
                old = top_s[pl.ds(at, W), :]
                top = jnp.maximum(old, top)
                keeps.append(jnp.exp2((old - top) * e))
            top_s[pl.ds(at, W), :] = top
            w = [jnp.exp2((t - top) * e) for t in s]
            total = w[0]
            for t in w[1:]:
                total = total + t
            sum_s[pl.ds(at, W), :] = total if new else sum_s[pl.ds(at, W), :] * keeps[-1] + total
            weights.append(jnp.concatenate([t.astype(BF16) for t in w], 1))
        for i, (at, keys, _) in enumerate(todo):
            more, col = None, 0
            for k, n in keys:
                r = _dot(weights[i][:, col : col + n], kv_s[1, pl.ds(k, n), :], 1, 0)
                more, col = r if more is None else more + r, col + n
            acc_s[pl.ds(at, W), :] = more if new else acc_s[pl.ds(at, W), :] * jnp.concatenate([keeps[i], keeps[i]], 1) + more

    def wo_rows(dev, half):
        return pl.ds(pl.multiple_of(dev * 256 + half * 128, 128), 128)

    def wo_own(half, way):
        return remote(wo_h.at[rows(half, 128), :], a_s.at[wo_rows(me, half), :], s_wo.at[2 * way + half], r_wo.at[2 * way + half],
                      (xn, yn, mate)[way])

    def wo_local(half):
        return pltpu.make_async_copy(wo_h.at[rows(half, 128), :], a_s.at[wo_rows(me, half), :], loc.at[9 + half])

    def wo_fwd(k, half):
        ref = a_s.at[wo_rows((xn, yn, 2 * cd + c)[k], half), :]
        return remote(ref, ref, f_wo.at[2 * k + half], g_wo.at[2 * k + half], mate)

    def wo_relay(way):
        ref = a_s.at[wo_rows((xn, yn)[way], way), :]
        return remote(ref, ref, s_wo.at[6 + way], r_wo.at[6 + way], (yn, xn)[way])

    wo_any = a_s.at[rows(0, 128), :]
    piece_any = piece(0)

    def take(k):
        way, i = (k % 2, k // 2) if k < 4 else (2, k - 4)
        chip = chips[way]
        ref = piece(2 * chip + i)
        slot = 2 * way + i

        @pl.when(chip < p)
        def _():
            arrived(piece_any, r_kv.at[slot])
            kv_fwd(2 * chip + i).start()

        if way == 0:

            @pl.when((p == 3) | (p == 2) & (i == 0))
            def _():
                remote(ref, ref, s_kv.at[4 + i], r_kv.at[4 + i], yn).start()

        if way == 1 and i == 1:

            @pl.when(p == 1)
            def _():
                remote(ref, ref, s_kv.at[4 + i], r_kv.at[4 + i], xn).start()

    def o_copy(j):
        h = 4 * c + j
        dst = wq_s.at[lax.div(h, 2), pl.ds(pl.multiple_of(lax.rem(h, 2) * own, own), own), :]
        return remote(q_s.at[pl.ds(pl.multiple_of(j * 2048 + (1 - c) * own, own), own), :], dst, s_o.at[j], r_o.at[j], mate)

    def wq_pass(j):
        for i in (0, 1, 2, 3):
            arrived(wq_s.at[j, rows(0, 256), :], r_q.at[j, i])
        start(wq_relay(j))

    def work(m, _):
        late = m >= 11
        j = jnp.where(late, m - 9, m)
        heads = (m < 3) | late & (m < 14)
        projects = heads & (m != 2) & (m != 13)

        def at_step(n):
            return pl.when(m == n)

        @at_step(0)
        def _():
            wq_pass(0)
            start(wq_own(1, 1))

        @at_step(1)
        def _():
            wq_pass(1)
            for way, at_0 in enumerate((px == 0, py == 0)):

                @pl.when(at_0)
                def _():
                    start([kv_own(i, way) for i in range(2)])

            start(wq_own(2, 0) + wq_own(2, 1) + wq_own(3, 0) + wq_own(3, 1))
            for i in range(2):
                arrived(piece(0), g_kv.at[2 * p + i])

        @at_step(9)
        def _():
            wq_pass(2)

        @at_step(11)
        def _():
            wq_pass(3)

        @pl.when(heads & (m != 0) & (m != 11))
        def _():
            base, first = (j - 1) * 2048, pl.multiple_of(p * 2048, 2048)
            strips([(pl.multiple_of(base + i * W, W), [(first, (i + 1) * W)], True) for i in range(7, -1, -1)], True)

        @pl.when(projects)
        def _():
            arrived(wq_s.at[j, rows(0, 256), :], loc.at[5 + j])
            for i in (6, 4, 5):
                arrived(wq_s.at[j, rows(0, 256), :], r_q.at[j, i])

            def project(n, _):
                at = pl.multiple_of(n * 512, 512)
                r = _dot(a_s[pl.ds(at, 512), :], wq_s[j], 1, 0)
                q_s[pl.ds(pl.multiple_of(j * 2048 + at, 512), 512), :] = turn(r, at)

            lax.fori_loop(0, 4, project, None)

        @at_step(3)
        def _():
            take(0)
            take(1)

        @at_step(7)
        def _():
            take(2)
            take(3)

        @at_step(14)
        def _():
            for n in range(4):
                for k in (5, 6):
                    arrived(wq_s.at[0, rows(0, 256), :], s_q.at[n, k])
            for dev in (xn, yn, mate):
                pl.semaphore_signal(free, inc=1, device_id={"sp": dev}, device_id_type=pl.DeviceIdType.MESH)

        @at_step(15)
        def _():
            pl.semaphore_wait(free, 3)
            start([wo_own(0, 0), wo_own(1, 1), wo_own(1, 0), wo_own(0, 1)])
            for half in range(2):
                wo_local(half).start()
                wo_own(half, 2).start()

        @at_step(18)
        def _():
            take(4)
            take(5)

        @at_step(21)
        def _():
            for way in range(2):
                arrived(wo_any, r_wo.at[2 * way + way])
                wo_relay(way).start()
                wo_fwd(way, way).start()

        @at_step(24)
        def _():
            for way in range(2):
                arrived(wo_any, r_wo.at[2 * way + 1 - way])
                wo_fwd(way, 1 - way).start()

        @at_step(27)
        def _():
            for half in range(2):
                arrived(wo_any, r_wo.at[6 + half])
                wo_fwd(2, half).start()

        last = m >= 22
        n = jnp.where(last, m - 22, jnp.where(late, m - 14, m - 3))
        t = jnp.where(last, 2, lax.div(n, 4))
        j = jnp.where(last, lax.rem(n, 4), 2 * jnp.where(late, 1, 0) + lax.div(lax.rem(n, 4), 2))
        half = jnp.where(last, jnp.where(n < 4, 1 - c, c), lax.rem(n, 2))
        first = pl.multiple_of(j * 2048 + half * own, own)
        lone = jnp.where(p == 1, cy, jnp.where(last, cd, cx))
        both = (p == 3) & (t < 2)
        n_a, n_b = jnp.where(both, 2 * cx + t, 2 * lone), jnp.where(both, 2 * cy + t, 2 * lone + 1)
        active = jnp.logical_not(heads) & ((p == 3) | (p == 2) & (t > 0) | (p == 1) & (t == 1))

        @pl.when(active & ((m == 3) | (m == 7) | (m == 22)))
        def _():
            arrived(piece_any, g_kv.at[n_a])
            arrived(piece_any, g_kv.at[n_b])

        @pl.when(active)
        def _():
            keys = [(pl.multiple_of(n_a * B, B), B), (pl.multiple_of(n_b * B, B), B)]
            strips([(pl.multiple_of(first + i * W, W), keys, False) for i in range(4)], False)

        def seen(i):
            at = pl.ds(pl.multiple_of(first + i * W, W), W)
            return (acc_s[at, :] * (1 / sum_s[at, :].sum(axis=1, keepdims=True))).astype(BF16)

        @pl.when(last & (n < 4))
        def _():
            for i in range(4):
                q_s[pl.ds(pl.multiple_of(first + i * W, W), W), :] = seen(i)
            o_copy(j).start()

        @pl.when(last & (n >= 4))
        def _():
            h = 4 * c + j
            for i in range(4):
                wq_s[lax.div(h, 2), pl.ds(pl.multiple_of(lax.rem(h, 2) * own + i * W, W), W), :] = seen(i)

    lax.fori_loop(0, 30, work, None)
    for half in range(2):
        arrived(wo_any, loc.at[9 + half])
        arrived(wo_any, r_wo.at[4 + half])
        for k in range(3):
            arrived(wo_any, g_wo.at[2 * k + half])
    for j in range(4):
        arrived(q_s.at[:own, :], r_o.at[j])

    def y_copy(i):
        return pltpu.make_async_copy(x_s.at[rows(i, 256), :], y_h.at[rows(i, 256), :], loc.at[i])

    def out(i, _):
        at = pl.multiple_of(i * 256, 256)
        seen = jnp.concatenate([wq_s[h // 2, pl.ds(pl.multiple_of(h % 2 * own + at, 256), 256), :] for h in range(8)], 1)
        for n in range(4):
            cols = slice(512 * n, 512 * (n + 1))
            r = _dot(seen, a_s[:, cols], 1, 0)
            x_s[pl.ds(at, 256), cols] = (x_s[pl.ds(at, 256), cols].astype(F32) + r).astype(BF16)
        y_copy(i).start()

    lax.fori_loop(0, 4, out, None)

    def left(ref, sem):
        pltpu.make_async_copy(ref, ref, sem).wait()

    for i in range(4):
        left(q_s.at[:own, :], s_o.at[i])
        for k in range(5):
            left(wq_s.at[0, rows(0, 256), :], s_q.at[i, k])
    for i in range(7):
        left(w_mine, s_w.at[i])
    for lot, sent in enumerate((px == 0, py == 0, p > 0)):

        @pl.when(sent)
        def _():
            def one(i, _):
                left(piece_any, s_kv.at[2 * lot + i])

            lo, hi = (0, 2) if lot < 2 else (jnp.where(p == 1, 1, 0), jnp.where(p == 2, 1, 2))
            lax.fori_loop(lo, hi, one, None)

    def forwarded(i, _):
        left(piece_any, f_kv.at[i])

    lax.fori_loop(0, 2 * p + 2, forwarded, None)
    for i in range(8):
        left(wo_any, s_wo.at[i])
    for i in range(6):
        left(wo_any, f_wo.at[i])
    for i in range(4):
        y_copy(i).wait()


def solution(mesh):
    def step(x, gain, wq, wk, wv, wo):
        half = HEAD // 2
        freq = np.asarray([THETA ** (-i / half) for i in range(half)], np.float32)[None]
        hbm, vmem = pl.BlockSpec(memory_space=pl.ANY), pl.BlockSpec(memory_space=pltpu.VMEM)
        dma = pltpu.SemaphoreType.DMA
        return pl.pallas_call(
            _kernel,
            out_shape=jax.ShapeDtypeStruct(x.shape, x.dtype),
            in_specs=[hbm, vmem, vmem, hbm, hbm, hbm, hbm],
            out_specs=hbm,
            scratch_shapes=[
                pltpu.VMEM((2048, 2048), BF16),
                pltpu.VMEM((1024, 2048), BF16),
                pltpu.VMEM((4, 2048, 256), BF16),
                pltpu.VMEM((2048, 256), BF16),
                pltpu.VMEM((2, 8192, 256), BF16),
                pltpu.VMEM((4 * 2048, 256), BF16),
                pltpu.VMEM((2048, 128), F32),
                pltpu.VMEM((2048, 128), F32),
                pltpu.VMEM((4 * 2048, 256), F32),
                pltpu.VMEM((4 * 2048, 128), F32),
                pltpu.VMEM((4 * 2048, 128), F32),
                dma((11,)),
                dma((4,)), dma((4,)),
                dma((7,)), dma((7,)),
                dma((4, 7)), dma((4, 7)),
                dma((6,)), dma((6,)), dma((8,)), dma((8,)),
                dma((8,)), dma((8,)), dma((6,)), dma((6,)),
                dma((4,)), dma((4,)),
                pltpu.SemaphoreType.REGULAR,
            ],
            compiler_params=pltpu.CompilerParams(collective_id=0, has_side_effects=True, vmem_limit_bytes=67043328),
            name="half_layer",
        )(x, gain, freq, wq, wk, wv, wo)

    tokens, whole = P(("dp", "sp"), None), P("sp", None)
    return jax.shard_map(
        step,
        mesh=mesh,
        in_specs=(tokens, P(None), whole, whole, whole, whole),
        out_specs=tokens,
        check_vma=False,
    )
```

```python
import jax
import jax.numpy as jnp
import numpy as np
from jax import lax
from jax.experimental import pallas as pl
from jax.experimental.pallas import tpu as pltpu
from jax.sharding import PartitionSpec as P

NEG = -1e30
HIDDEN = 2 * NEG
LOG2E = 1.4426950408889634
HEAD = 256
THETA = 10000
W = 256
B = 1024
F32, BF16 = jnp.float32, jnp.bfloat16


def _dot(a, b, ca, cb):
    return lax.dot_general(a, b, (((ca,), (cb,)), ((), ())), preferred_element_type=F32)


def _kernel(x_h, gain_ref, freq_ref, wq_h, wk_h, wv_h, wo_h, y_h,
            a_s, x_s, wq_s, kv_s, q_s, wo_s, cos_s, sin_s, acc_s, top_s, sum_s,
            loc, s_a, r_a, s_w, r_w, s_q, r_q, s_kv, r_kv, f_kv, g_kv, s_wo, r_wo, f_wo, g_wo, s_o, r_o, free):
    me = lax.axis_index("sp")
    c = lax.rem(me, 2)
    p = lax.div(me, 2)
    px, py = lax.div(p, 2), lax.rem(p, 2)
    cx, cy, cd = 2 * (1 - px) + py, 2 * px + 1 - py, 2 * (1 - px) + 1 - py
    chips = (cx, cy, cd)
    mate = 2 * p + 1 - c
    xn, yn = 2 * cx + c, 2 * cy + c
    own = 1024
    w_s = wo_s.at[:, :256]

    def remote(src, dst, ss, rs, dev):
        return pltpu.make_async_remote_copy(src_ref=src, dst_ref=dst, send_sem=ss, recv_sem=rs, device_id={"sp": dev},
                                            device_id_type=pl.DeviceIdType.MESH)

    def arrived(ref, sem):
        pltpu.make_async_copy(ref, ref, sem).wait()

    def rows(i, n):
        return pl.ds(pl.multiple_of(i * n, n), n)

    loads = [pltpu.make_async_copy(x_h.at[rows(i, 256), :], x_s.at[rows(i, 256), :], loc.at[i]) for i in range(4)]
    for t in loads:
        t.start()

    barrier = pltpu.get_barrier_semaphore()
    for dev in (mate, 2 * cx, 2 * cx + 1, 2 * cy, 2 * cy + 1):
        pl.semaphore_signal(barrier, inc=1, device_id={"sp": dev}, device_id_type=pl.DeviceIdType.MESH)
    pl.semaphore_wait(barrier, 5)

    w_mine = w_s.at[rows(me, 256), :]
    for t, w_h in enumerate((wk_h, wv_h)):
        remote(w_h, w_mine, s_w.at[t], r_w.at[c], 2 * cx + t).start()
        remote(w_h, w_mine, s_w.at[2 + t], r_w.at[2 + c], 2 * cy + t).start()

        @pl.when(c == t)
        def _():
            pltpu.make_async_copy(w_h, w_mine, loc.at[4]).start()

        @pl.when(c != t)
        def _():
            remote(w_h, w_mine, s_w.at[4], r_w.at[6], mate).start()

    def wq_part(core, j):
        return wq_h.at[:, pl.ds(pl.multiple_of((4 * core + j) * 256, 256), 256)]

    def wq_own(j, t):
        dst = wq_s.at[j, rows(me, 256), :]
        return [remote(wq_part(t, j), dst, s_q.at[j, t], r_q.at[j, c], 2 * cx + t),
                remote(wq_part(t, j), dst, s_q.at[j, 2 + t], r_q.at[j, 2 + c], 2 * cy + t)]

    def wq_mate(j):
        return remote(wq_part(1 - c, j), wq_s.at[j, rows(me, 256), :], s_q.at[j, 4], r_q.at[j, 6], mate)

    def wq_local(j):
        return pltpu.make_async_copy(wq_part(c, j), wq_s.at[j, rows(me, 256), :], loc.at[5 + j])

    def wq_relay(j):
        fx, fy = wq_s.at[j, rows(2 * cx, 256), :], wq_s.at[j, rows(2 * cy + 1, 256), :]
        return [remote(fx, fx, s_q.at[j, 5], r_q.at[j, 4], yn), remote(fy, fy, s_q.at[j, 6], r_q.at[j, 5], xn)]

    def start(ts):
        for t in ts:
            t.start()

    def a_rows(i):
        return a_s.at[pl.ds(pl.multiple_of(c * own + i * 256, 256), 256), :]

    def a_copy(i):
        return remote(a_rows(i), a_rows(i), s_a.at[i], r_a.at[i], mate)

    start(wq_own(0, 0))
    gain = gain_ref[...].astype(F32)[None]
    for i in range(4):
        loads[i].wait()

        def norm(n, _):
            at = pl.multiple_of(i * 256 + n * 64, 64)
            wide = x_s[pl.ds(at, 64), :].astype(F32)
            scale = lax.rsqrt(jnp.mean(wide * wide, -1, keepdims=True) + 1e-6)
            a_s[pl.ds(pl.multiple_of(c * own + at, 64), 64), :] = (wide * scale * gain).astype(BF16)

        lax.fori_loop(0, 4, norm, None)
        a_copy(i).start()

    def angles(n, _):
        at = pl.multiple_of(n * 64, 64)
        place = (p * 2048 + at + lax.broadcasted_iota(jnp.int32, (64, 128), 0)).astype(F32)
        angle = place * freq_ref[...]
        cos_s[pl.ds(at, 64), :] = jnp.cos(angle)
        sin_s[pl.ds(at, 64), :] = jnp.sin(angle)

    lax.fori_loop(0, 16, angles, None)

    for i in range(4):
        arrived(w_s.at[rows(0, 256), :], r_w.at[i])
    fx, fy = w_s.at[rows(2 * cx, 256), :], w_s.at[rows(2 * cy + 1, 256), :]
    relays_w = [remote(fx, fx, s_w.at[5], r_w.at[4], yn), remote(fy, fy, s_w.at[6], r_w.at[5], xn)]
    start(relays_w)
    start(wq_own(0, 1) + wq_own(1, 0))
    for j in range(4):
        wq_mate(j).start()
        wq_local(j).start()
    lax.fori_loop(16, 32, angles, None)
    for i in range(4):
        arrived(a_rows(0), r_a.at[i])
        arrived(a_rows(0), s_a.at[i])
    arrived(w_mine, loc.at[4])
    for i in (6, 4, 5):
        arrived(w_mine, r_w.at[i])

    def turn(r, at):
        r = r.astype(BF16).astype(F32)
        lo, hi = r[:, :128], r[:, 128:]
        cos, sin = cos_s[pl.ds(at, r.shape[0]), :], sin_s[pl.ds(at, r.shape[0]), :]
        return jnp.concatenate([lo * cos - hi * sin, hi * cos + lo * sin], -1).astype(BF16)

    def piece(n):
        return kv_s.at[c, rows(n, B), :]

    def kv_fwd(n):
        return remote(piece(n), piece(n), f_kv.at[n], g_kv.at[n], mate)

    def kv_own(i, way):
        ref = piece(2 * p + i)
        return remote(ref, ref, s_kv.at[2 * way + i], r_kv.at[2 * way + i], (xn, yn)[way])

    def kvproj(i, _):
        at = pl.multiple_of(i * 512, 512)
        to = pl.ds(pl.multiple_of(p * 2048 + at, 512), 512)
        r = _dot(a_s[pl.ds(at, 512), :], w_s[...], 1, 0)

        @pl.when(c == 0)
        def _():
            kv_s[0, to, :] = turn(r, at)

        @pl.when(c == 1)
        def _():
            kv_s[1, to, :] = r.astype(BF16)

        @pl.when(lax.rem(i, 2) == 1)
        def _():
            kv_fwd(2 * p + lax.div(i, 2)).start()

    lax.fori_loop(0, 4, kvproj, None)
    for i in (5, 6):
        arrived(w_mine, s_w.at[i])

    e = HEAD**-0.5 * LOG2E

    def strips(todo, new):
        scores = [[_dot(q_s[pl.ds(at, W), :], kv_s[0, pl.ds(k, n), :], 1, 1) for k, n in keys] for at, keys, _ in todo]
        weights, keeps = [], []
        for (at, keys, edge), parts in zip(todo, scores):
            s = [t[:, i : i + 128] for t in parts for i in range(0, t.shape[1], 128)]
            if edge:
                gap = lax.broadcasted_iota(jnp.int32, (W, 128), 0) - lax.broadcasted_iota(jnp.int32, (W, 128), 1)
                s[-2] = jnp.where(gap >= 0, s[-2], HIDDEN)
                s[-1] = jnp.where(gap >= 128, s[-1], HIDDEN)
            most = s[0]
            for t in s[1:]:
                most = jnp.maximum(most, t)
            top = jnp.broadcast_to(most.max(axis=1, keepdims=True), (W, 128))
            if not new:
                old = top_s[pl.ds(at, W), :]
                top = jnp.maximum(old, top)
                keeps.append(jnp.exp2((old - top) * e))
            top_s[pl.ds(at, W), :] = top
            w = [jnp.exp2((t - top) * e) for t in s]
            total = w[0]
            for t in w[1:]:
                total = total + t
            sum_s[pl.ds(at, W), :] = total if new else sum_s[pl.ds(at, W), :] * keeps[-1] + total
            weights.append(jnp.concatenate([t.astype(BF16) for t in w], 1))
        for i, (at, keys, _) in enumerate(todo):
            more, col = None, 0
            for k, n in keys:
                r = _dot(weights[i][:, col : col + n], kv_s[1, pl.ds(k, n), :], 1, 0)
                more, col = r if more is None else more + r, col + n
            acc_s[pl.ds(at, W), :] = more if new else acc_s[pl.ds(at, W), :] * jnp.concatenate([keeps[i], keeps[i]], 1) + more

    def wo_rows(dev, half):
        return pl.ds(pl.multiple_of(dev * 256 + half * 128, 128), 128)

    def wo_own(half, way):
        return remote(wo_h.at[rows(half, 128), :], wo_s.at[wo_rows(me, half), :], s_wo.at[2 * way + half], r_wo.at[2 * way + half],
                      (xn, yn, mate)[way])

    def wo_local(half):
        return pltpu.make_async_copy(wo_h.at[rows(half, 128), :], wo_s.at[wo_rows(me, half), :], loc.at[9 + half])

    def wo_fwd(k, half):
        ref = wo_s.at[wo_rows((xn, yn, 2 * cd + c)[k], half), :]
        return remote(ref, ref, f_wo.at[2 * k + half], g_wo.at[2 * k + half], mate)

    def wo_relay(way):
        ref = wo_s.at[wo_rows((xn, yn)[way], way), :]
        return remote(ref, ref, s_wo.at[6 + way], r_wo.at[6 + way], (yn, xn)[way])

    wo_any = wo_s.at[rows(0, 128), :]
    piece_any = piece(0)

    def take(k):
        way, i = (k % 2, k // 2) if k < 4 else (2, k - 4)
        chip = chips[way]
        ref = piece(2 * chip + i)
        slot = 2 * way + i

        @pl.when(chip < p)
        def _():
            arrived(piece_any, r_kv.at[slot])
            kv_fwd(2 * chip + i).start()

        if way == 0:

            @pl.when((p == 3) | (p == 2) & (i == 0))
            def _():
                remote(ref, ref, s_kv.at[4 + i], r_kv.at[4 + i], yn).start()

        if way == 1 and i == 1:

            @pl.when(p == 1)
            def _():
                remote(ref, ref, s_kv.at[4 + i], r_kv.at[4 + i], xn).start()

    def o_copy(j):
        h = 4 * c + j
        dst = wq_s.at[lax.div(h, 2), pl.ds(pl.multiple_of(lax.rem(h, 2) * own, own), own), :]
        return remote(q_s.at[pl.ds(pl.multiple_of(j * 2048 + (1 - c) * own, own), own), :], dst, s_o.at[j], r_o.at[j], mate)

    def wq_pass(j):
        for i in (0, 1, 2, 3):
            arrived(wq_s.at[j, rows(0, 256), :], r_q.at[j, i])
        start(wq_relay(j))

    def work(m, _):
        late = m >= 7
        j = jnp.where(late, m - 5, m)
        heads = (m < 3) | late & (m < 10)
        projects = heads & (m != 2) & (m != 9)

        def at_step(n):
            return pl.when(m == n)

        @at_step(0)
        def _():
            wq_pass(0)
            start(wq_own(1, 1))

        @at_step(1)
        def _():
            wq_pass(1)
            for way, at_0 in enumerate((px == 0, py == 0)):

                @pl.when(at_0)
                def _():
                    start([kv_own(i, way) for i in range(2)])

            start(wq_own(2, 0) + wq_own(2, 1) + wq_own(3, 0) + wq_own(3, 1))
            for i in range(2):
                arrived(piece(0), g_kv.at[2 * p + i])

        @at_step(6)
        def _():
            wq_pass(2)
            start([wo_own(0, 0), wo_own(1, 1)])

        @at_step(7)
        def _():
            wq_pass(3)
            start([wo_own(1, 0), wo_own(0, 1)])
            for half in range(2):
                wo_local(half).start()
                wo_own(half, 2).start()

        @pl.when(heads & (m != 0) & (m != 7))
        def _():
            base, first = (j - 1) * 2048, pl.multiple_of(p * 2048, 2048)
            strips([(pl.multiple_of(base + i * W, W), [(first, (i + 1) * W)], True) for i in range(7, -1, -1)], True)

        @pl.when(projects)
        def _():
            arrived(wq_s.at[j, rows(0, 256), :], loc.at[5 + j])
            for i in (6, 4, 5):
                arrived(wq_s.at[j, rows(0, 256), :], r_q.at[j, i])

            def project(n, _):
                at = pl.multiple_of(n * 512, 512)
                r = _dot(a_s[pl.ds(at, 512), :], wq_s[j], 1, 0)
                q_s[pl.ds(pl.multiple_of(j * 2048 + at, 512), 512), :] = turn(r, at)

            lax.fori_loop(0, 4, project, None)

        @at_step(3)
        def _():
            take(0)
            take(1)

        @at_step(5)
        def _():
            take(2)
            take(3)

        @at_step(10)
        def _():
            for n in range(4):
                for k in (5, 6):
                    arrived(wq_s.at[0, rows(0, 256), :], s_q.at[n, k])
            pl.semaphore_signal(free, inc=1, device_id={"sp": mate}, device_id_type=pl.DeviceIdType.MESH)

        @at_step(14)
        def _():
            pl.semaphore_wait(free, 1)

        @at_step(12)
        def _():
            take(4)
            take(5)

        @at_step(11)
        def _():
            for way in range(2):
                arrived(wo_any, r_wo.at[2 * way + way])
                wo_relay(way).start()
                wo_fwd(way, way).start()

        @at_step(13)
        def _():
            for way in range(2):
                arrived(wo_any, r_wo.at[2 * way + 1 - way])
                wo_fwd(way, 1 - way).start()

        @at_step(15)
        def _():
            for half in range(2):
                arrived(wo_any, r_wo.at[6 + half])
                wo_fwd(2, half).start()

        last = m >= 14
        n = jnp.where(late, m - 10, m - 3)
        t = jnp.where(last, 2, lax.div(n, 2))
        j = jnp.where(last, m - 14, 2 * jnp.where(late, 1, 0) + lax.rem(n, 2))
        lone = jnp.where(p == 1, cy, jnp.where(last, cd, cx))
        both = (p == 3) & (t < 2)
        n_a, n_b = jnp.where(both, 2 * cx + t, 2 * lone), jnp.where(both, 2 * cy + t, 2 * lone + 1)
        active = jnp.logical_not(heads) & ((p == 3) | (p == 2) & (t > 0) | (p == 1) & (t == 1))

        @pl.when(active & ((m == 3) | (m == 5) | (m == 14)))
        def _():
            arrived(piece_any, g_kv.at[n_a])
            arrived(piece_any, g_kv.at[n_b])

        @pl.when(active)
        def _():
            keys = [(pl.multiple_of(n_a * B, B), B), (pl.multiple_of(n_b * B, B), B)]

            def group(g, _):
                first = pl.multiple_of(j * 2048 + g * own, own)
                strips([(pl.multiple_of(first + i * W, W), keys, False) for i in range(4)], False)

            lax.fori_loop(0, 2, group, None)

        def seen(half, i):
            at = pl.ds(pl.multiple_of(j * 2048 + half * own + i * W, W), W)
            return at, (acc_s[at, :] * (1 / sum_s[at, :].sum(axis=1, keepdims=True))).astype(BF16)

        @pl.when(last)
        def _():
            for i in range(4):
                at, r = seen(1 - c, i)
                q_s[at, :] = r
            o_copy(j).start()
            h = 4 * c + j
            for i in range(4):
                _, r = seen(c, i)
                wq_s[lax.div(h, 2), pl.ds(pl.multiple_of(lax.rem(h, 2) * own + i * W, W), W), :] = r

    lax.fori_loop(0, 18, work, None)
    for half in range(2):
        arrived(wo_any, loc.at[9 + half])
        arrived(wo_any, r_wo.at[4 + half])
        for k in range(3):
            arrived(wo_any, g_wo.at[2 * k + half])
    for j in range(4):
        arrived(q_s.at[:own, :], r_o.at[j])

    def y_copy(i):
        return pltpu.make_async_copy(x_s.at[rows(i, 256), :], y_h.at[rows(i, 256), :], loc.at[i])

    def out(i, _):
        at = pl.multiple_of(i * 256, 256)
        seen = jnp.concatenate([wq_s[h // 2, pl.ds(pl.multiple_of(h % 2 * own + at, 256), 256), :] for h in range(8)], 1)
        for n in range(4):
            cols = slice(512 * n, 512 * (n + 1))
            r = _dot(seen, wo_s[:, cols], 1, 0)
            x_s[pl.ds(at, 256), cols] = (x_s[pl.ds(at, 256), cols].astype(F32) + r).astype(BF16)
        y_copy(i).start()

    lax.fori_loop(0, 4, out, None)

    def left(ref, sem):
        pltpu.make_async_copy(ref, ref, sem).wait()

    for i in range(4):
        left(q_s.at[:own, :], s_o.at[i])
        for k in range(5):
            left(wq_s.at[0, rows(0, 256), :], s_q.at[i, k])
    for i in range(5):
        left(w_mine, s_w.at[i])
    for lot, sent in enumerate((px == 0, py == 0, p > 0)):

        @pl.when(sent)
        def _():
            def one(i, _):
                left(piece_any, s_kv.at[2 * lot + i])

            lo, hi = (0, 2) if lot < 2 else (jnp.where(p == 1, 1, 0), jnp.where(p == 2, 1, 2))
            lax.fori_loop(lo, hi, one, None)

    def forwarded(i, _):
        left(piece_any, f_kv.at[i])

    lax.fori_loop(0, 2 * p + 2, forwarded, None)
    for i in range(8):
        left(wo_any, s_wo.at[i])
    for i in range(6):
        left(wo_any, f_wo.at[i])
    for i in range(4):
        y_copy(i).wait()


def solution(mesh):
    def step(x, gain, wq, wk, wv, wo):
        half = HEAD // 2
        freq = np.asarray([THETA ** (-i / half) for i in range(half)], np.float32)[None]
        hbm, vmem = pl.BlockSpec(memory_space=pl.ANY), pl.BlockSpec(memory_space=pltpu.VMEM)
        dma = pltpu.SemaphoreType.DMA
        return pl.pallas_call(
            _kernel,
            out_shape=jax.ShapeDtypeStruct(x.shape, x.dtype),
            in_specs=[hbm, vmem, vmem, hbm, hbm, hbm, hbm],
            out_specs=hbm,
            scratch_shapes=[
                pltpu.VMEM((2048, 2048), BF16),
                pltpu.VMEM((1024, 2048), BF16),
                pltpu.VMEM((4, 2048, 256), BF16),
                pltpu.VMEM((2, 8192, 256), BF16),
                pltpu.VMEM((4 * 2048, 256), BF16),
                pltpu.VMEM((2048, 2048), BF16),
                pltpu.VMEM((2048, 128), F32),
                pltpu.VMEM((2048, 128), F32),
                pltpu.VMEM((4 * 2048, 256), F32),
                pltpu.VMEM((4 * 2048, 128), F32),
                pltpu.VMEM((4 * 2048, 128), F32),
                dma((11,)),
                dma((4,)), dma((4,)),
                dma((7,)), dma((7,)),
                dma((4, 7)), dma((4, 7)),
                dma((6,)), dma((6,)), dma((8,)), dma((8,)),
                dma((8,)), dma((8,)), dma((6,)), dma((6,)),
                dma((4,)), dma((4,)),
                pltpu.SemaphoreType.REGULAR,
            ],
            compiler_params=pltpu.CompilerParams(collective_id=0, has_side_effects=True, vmem_limit_bytes=67043328),
            name="half_layer",
        )(x, gain, freq, wq, wk, wv, wo)

    tokens, whole = P(("dp", "sp"), None), P("sp", None)
    return jax.shard_map(
        step,
        mesh=mesh,
        in_specs=(tokens, P(None), whole, whole, whole, whole),
        out_specs=tokens,
        check_vma=False,
    )
```

```python
import jax
import jax.numpy as jnp
import numpy as np
from jax import lax
from jax.experimental import pallas as pl
from jax.experimental.pallas import tpu as pltpu
from jax.sharding import PartitionSpec as P

NEG = -1e30
HIDDEN = 2 * NEG
LOG2E = 1.4426950408889634
HEAD = 256
THETA = 10000
W = 256
B = 1024
F32, BF16 = jnp.float32, jnp.bfloat16


def _dot(a, b, ca, cb):
    return lax.dot_general(a, b, (((ca,), (cb,)), ((), ())), preferred_element_type=F32)


def _kernel(x_h, gain_ref, freq_ref, wq_h, wk_h, wv_h, wo_h, y_h,
            a_s, x_s, wq_s, kv_s, q_s, wo_s, cos_s, sin_s, acc_s, top_s, sum_s,
            loc, s_a, r_a, s_w, r_w, s_q, r_q, s_kv, r_kv, f_kv, g_kv, s_wo, r_wo, f_wo, g_wo, s_o, r_o, free):
    me = lax.axis_index("sp")
    c = lax.rem(me, 2)
    p = lax.div(me, 2)
    px, py = lax.div(p, 2), lax.rem(p, 2)
    cx, cy, cd = 2 * (1 - px) + py, 2 * px + 1 - py, 2 * (1 - px) + 1 - py
    chips = (cx, cy, cd)
    mate = 2 * p + 1 - c
    xn, yn = 2 * cx + c, 2 * cy + c
    own = 1024
    w_s = wo_s.at[:, :256]

    def remote(src, dst, ss, rs, dev):
        return pltpu.make_async_remote_copy(src_ref=src, dst_ref=dst, send_sem=ss, recv_sem=rs, device_id={"sp": dev},
                                            device_id_type=pl.DeviceIdType.MESH)

    def arrived(ref, sem):
        pltpu.make_async_copy(ref, ref, sem).wait()

    def rows(i, n):
        return pl.ds(pl.multiple_of(i * n, n), n)

    loads = [pltpu.make_async_copy(x_h.at[rows(i, 256), :], x_s.at[rows(i, 256), :], loc.at[i]) for i in range(4)]
    for t in loads:
        t.start()

    barrier = pltpu.get_barrier_semaphore()
    for dev in (mate, 2 * cx, 2 * cx + 1, 2 * cy, 2 * cy + 1):
        pl.semaphore_signal(barrier, inc=1, device_id={"sp": dev}, device_id_type=pl.DeviceIdType.MESH)
    pl.semaphore_wait(barrier, 5)

    w_mine = w_s.at[rows(me, 256), :]
    for t, w_h in enumerate((wk_h, wv_h)):
        remote(w_h, w_mine, s_w.at[t], r_w.at[c], 2 * cx + t).start()
        remote(w_h, w_mine, s_w.at[2 + t], r_w.at[2 + c], 2 * cy + t).start()

        @pl.when(c == t)
        def _():
            pltpu.make_async_copy(w_h, w_mine, loc.at[4]).start()

        @pl.when(c != t)
        def _():
            remote(w_h, w_mine, s_w.at[4], r_w.at[6], mate).start()

    def wq_part(core, j):
        return wq_h.at[:, pl.ds(pl.multiple_of((4 * core + j) * 256, 256), 256)]

    def wq_own(j, t):
        dst = wq_s.at[j, rows(me, 256), :]
        return [remote(wq_part(t, j), dst, s_q.at[j, t], r_q.at[j, c], 2 * cx + t),
                remote(wq_part(t, j), dst, s_q.at[j, 2 + t], r_q.at[j, 2 + c], 2 * cy + t)]

    def wq_mate(j):
        return remote(wq_part(1 - c, j), wq_s.at[j, rows(me, 256), :], s_q.at[j, 4], r_q.at[j, 6], mate)

    def wq_local(j):
        return pltpu.make_async_copy(wq_part(c, j), wq_s.at[j, rows(me, 256), :], loc.at[5 + j])

    def wq_relay(j):
        fx, fy = wq_s.at[j, rows(2 * cx, 256), :], wq_s.at[j, rows(2 * cy + 1, 256), :]
        return [remote(fx, fx, s_q.at[j, 5], r_q.at[j, 4], yn), remote(fy, fy, s_q.at[j, 6], r_q.at[j, 5], xn)]

    def start(ts):
        for t in ts:
            t.start()

    def a_rows(i):
        return a_s.at[pl.ds(pl.multiple_of(c * own + i * 256, 256), 256), :]

    def a_copy(i):
        return remote(a_rows(i), a_rows(i), s_a.at[i], r_a.at[i], mate)

    start(wq_own(0, 0))
    gain = gain_ref[...].astype(F32)[None]
    for i in range(4):
        loads[i].wait()

        def norm(n, _):
            at = pl.multiple_of(i * 256 + n * 64, 64)
            wide = x_s[pl.ds(at, 64), :].astype(F32)
            scale = lax.rsqrt(jnp.mean(wide * wide, -1, keepdims=True) + 1e-6)
            a_s[pl.ds(pl.multiple_of(c * own + at, 64), 64), :] = (wide * scale * gain).astype(BF16)

        lax.fori_loop(0, 4, norm, None)
        a_copy(i).start()

    def angles(n, _):
        at = pl.multiple_of(n * 64, 64)
        place = (p * 2048 + at + lax.broadcasted_iota(jnp.int32, (64, 128), 0)).astype(F32)
        angle = place * freq_ref[...]
        cos_s[pl.ds(at, 64), :] = jnp.cos(angle)
        sin_s[pl.ds(at, 64), :] = jnp.sin(angle)

    lax.fori_loop(0, 16, angles, None)

    for i in range(4):
        arrived(w_s.at[rows(0, 256), :], r_w.at[i])
    fx, fy = w_s.at[rows(2 * cx, 256), :], w_s.at[rows(2 * cy + 1, 256), :]
    relays_w = [remote(fx, fx, s_w.at[5], r_w.at[4], yn), remote(fy, fy, s_w.at[6], r_w.at[5], xn)]
    start(relays_w)
    start(wq_own(0, 1) + wq_own(1, 0))
    for j in range(4):
        wq_mate(j).start()
        wq_local(j).start()
    lax.fori_loop(16, 32, angles, None)
    for i in range(4):
        arrived(a_rows(0), r_a.at[i])
        arrived(a_rows(0), s_a.at[i])
    arrived(w_mine, loc.at[4])
    for i in (6, 4, 5):
        arrived(w_mine, r_w.at[i])

    def turn(r, at):
        r = r.astype(BF16).astype(F32)
        lo, hi = r[:, :128], r[:, 128:]
        cos, sin = cos_s[pl.ds(at, r.shape[0]), :], sin_s[pl.ds(at, r.shape[0]), :]
        return jnp.concatenate([lo * cos - hi * sin, hi * cos + lo * sin], -1).astype(BF16)

    def piece(n):
        return kv_s.at[c, rows(n, B), :]

    def kv_fwd(n):
        return remote(piece(n), piece(n), f_kv.at[n], g_kv.at[n], mate)

    def kv_own(i, way):
        ref = piece(2 * p + i)
        return remote(ref, ref, s_kv.at[2 * way + i], r_kv.at[2 * way + i], (xn, yn)[way])

    def kvproj(i, _):
        at = pl.multiple_of(i * 512, 512)
        to = pl.ds(pl.multiple_of(p * 2048 + at, 512), 512)
        r = _dot(a_s[pl.ds(at, 512), :], w_s[...], 1, 0)

        @pl.when(c == 0)
        def _():
            kv_s[0, to, :] = turn(r, at)

        @pl.when(c == 1)
        def _():
            kv_s[1, to, :] = r.astype(BF16)

        @pl.when(lax.rem(i, 2) == 1)
        def _():
            kv_fwd(2 * p + lax.div(i, 2)).start()

    lax.fori_loop(0, 4, kvproj, None)
    for i in (5, 6):
        arrived(w_mine, s_w.at[i])

    e = HEAD**-0.5 * LOG2E

    def strips(todo, new):
        scores = [[_dot(q_s[pl.ds(at, W), :], kv_s[0, pl.ds(k, n), :], 1, 1) for k, n in keys] for at, keys, _ in todo]
        weights, keeps = [], []
        for (at, keys, edge), parts in zip(todo, scores):
            s = [t[:, i : i + 128] for t in parts for i in range(0, t.shape[1], 128)]
            if edge:
                gap = lax.broadcasted_iota(jnp.int32, (W, 128), 0) - lax.broadcasted_iota(jnp.int32, (W, 128), 1)
                s[-2] = jnp.where(gap >= 0, s[-2], HIDDEN)
                s[-1] = jnp.where(gap >= 128, s[-1], HIDDEN)
            most = s[0]
            for t in s[1:]:
                most = jnp.maximum(most, t)
            top = jnp.broadcast_to(most.max(axis=1, keepdims=True), (W, 128))
            if not new:
                old = top_s[pl.ds(at, W), :]
                top = jnp.maximum(old, top)
                keeps.append(jnp.exp2((old - top) * e))
            top_s[pl.ds(at, W), :] = top
            w = [jnp.exp2((t - top) * e) for t in s]
            total = w[0]
            for t in w[1:]:
                total = total + t
            sum_s[pl.ds(at, W), :] = total if new else sum_s[pl.ds(at, W), :] * keeps[-1] + total
            weights.append(jnp.concatenate([t.astype(BF16) for t in w], 1))
        for i, (at, keys, _) in enumerate(todo):
            more, col = None, 0
            for k, n in keys:
                r = _dot(weights[i][:, col : col + n], kv_s[1, pl.ds(k, n), :], 1, 0)
                more, col = r if more is None else more + r, col + n
            acc_s[pl.ds(at, W), :] = more if new else acc_s[pl.ds(at, W), :] * jnp.concatenate([keeps[i], keeps[i]], 1) + more

    def wo_rows(dev, half):
        return pl.ds(pl.multiple_of(dev * 256 + half * 128, 128), 128)

    def wo_own(half, way):
        return remote(wo_h.at[rows(half, 128), :], wo_s.at[wo_rows(me, half), :], s_wo.at[2 * way + half], r_wo.at[2 * way + half],
                      (xn, yn, mate)[way])

    def wo_local(half):
        return pltpu.make_async_copy(wo_h.at[rows(half, 128), :], wo_s.at[wo_rows(me, half), :], loc.at[9 + half])

    def wo_fwd(k, half):
        ref = wo_s.at[wo_rows((xn, yn, 2 * cd + c)[k], half), :]
        return remote(ref, ref, f_wo.at[2 * k + half], g_wo.at[2 * k + half], mate)

    def wo_relay(way):
        ref = wo_s.at[wo_rows((xn, yn)[way], way), :]
        return remote(ref, ref, s_wo.at[6 + way], r_wo.at[6 + way], (yn, xn)[way])

    wo_any = wo_s.at[rows(0, 128), :]
    piece_any = piece(0)

    def take(k):
        way, i = (k % 2, k // 2) if k < 4 else (2, k - 4)
        chip = chips[way]
        ref = piece(2 * chip + i)
        slot = 2 * way + i

        @pl.when(chip < p)
        def _():
            arrived(piece_any, r_kv.at[slot])
            kv_fwd(2 * chip + i).start()

        if way == 0:

            @pl.when((p == 3) | (p == 2) & (i == 0))
            def _():
                remote(ref, ref, s_kv.at[4 + i], r_kv.at[4 + i], yn).start()

        if way == 1 and i == 1:

            @pl.when(p == 1)
            def _():
                remote(ref, ref, s_kv.at[4 + i], r_kv.at[4 + i], xn).start()

    def o_copy(j):
        h = 4 * c + j
        dst = wq_s.at[lax.div(h, 2), pl.ds(pl.multiple_of(lax.rem(h, 2) * own, own), own), :]
        return remote(q_s.at[pl.ds(pl.multiple_of(j * 2048 + (1 - c) * own, own), own), :], dst, s_o.at[j], r_o.at[j], mate)

    def wq_pass(j):
        for i in (0, 1, 2, 3):
            arrived(wq_s.at[j, rows(0, 256), :], r_q.at[j, i])
        start(wq_relay(j))

    def work(m, _):
        def at_step(n):
            return pl.when(m == n)

        @pl.when(m < 3)
        def _():
            @at_step(0)
            def _():
                wq_pass(0)
                start(wq_own(1, 1) + wq_own(2, 0))

            @at_step(1)
            def _():
                wq_pass(1)
                start(wq_own(2, 1))
                for i in range(2):
                    arrived(piece(0), g_kv.at[2 * p + i])

            @at_step(2)
            def _():
                wq_pass(2)
                for way, at_0 in enumerate((px == 0, py == 0)):

                    @pl.when(at_0)
                    def _():
                        start([kv_own(i, way) for i in range(2)])

                start(wq_own(3, 0) + wq_own(3, 1))

        heads = (m < 4) | (m == 10) | (m == 11)
        late = m >= 10

        @pl.when(heads)
        def _():
            j = jnp.where(late, m - 7, m)

            @pl.when((m != 0) & (m != 10))
            def _():
                base, first = (j - 1) * 2048, pl.multiple_of(p * 2048, 2048)
                strips([(pl.multiple_of(base + i * W, W), [(first, (i + 1) * W)], True) for i in range(7, -1, -1)], True)

            @pl.when((m != 3) & (m != 11))
            def _():
                arrived(wq_s.at[j, rows(0, 256), :], loc.at[5 + j])
                for i in (6, 4, 5):
                    arrived(wq_s.at[j, rows(0, 256), :], r_q.at[j, i])

                def project(n, _):
                    at = pl.multiple_of(n * 512, 512)
                    r = _dot(a_s[pl.ds(at, 512), :], wq_s[j], 1, 0)
                    q_s[pl.ds(pl.multiple_of(j * 2048 + at, 512), 512), :] = turn(r, at)

                lax.fori_loop(0, 4, project, None)

        @pl.when((m >= 4) & (m < 10))
        def _():
            @at_step(4)
            def _():
                take(0)
                take(1)

            @at_step(7)
            def _():
                take(2)
                take(3)

            @at_step(8)
            def _():
                wq_pass(3)
                start([wo_own(0, 0), wo_own(1, 1), wo_own(1, 0), wo_own(0, 1)])
                for half in range(2):
                    wo_local(half).start()
                    wo_own(half, 2).start()

        @pl.when(m >= 12)
        def _():
            @at_step(12)
            def _():
                take(4)
                take(5)
                for way in range(2):
                    arrived(wo_any, r_wo.at[2 * way + way])
                    wo_relay(way).start()
                    wo_fwd(way, way).start()
                for n in range(4):
                    for k in (5, 6):
                        arrived(wq_s.at[0, rows(0, 256), :], s_q.at[n, k])
                pl.semaphore_signal(free, inc=1, device_id={"sp": mate}, device_id_type=pl.DeviceIdType.MESH)

            @at_step(14)
            def _():
                pl.semaphore_wait(free, 1)
                for way in range(2):
                    arrived(wo_any, r_wo.at[2 * way + 1 - way])
                    wo_fwd(way, 1 - way).start()

            @at_step(16)
            def _():
                for half in range(2):
                    arrived(wo_any, r_wo.at[6 + half])
                    wo_fwd(2, half).start()

        last = m >= 14
        n = m - 4
        t = jnp.where(last, 2, jnp.where(late, m - 12, lax.div(n, 3)))
        j = jnp.where(last, m - 14, jnp.where(late, 3, lax.rem(n, 3)))
        lone = jnp.where(p == 1, cy, jnp.where(last, cd, cx))
        both = (p == 3) & (t < 2)
        n_a, n_b = jnp.where(both, 2 * cx + t, 2 * lone), jnp.where(both, 2 * cy + t, 2 * lone + 1)
        active = jnp.logical_not(heads) & ((p == 3) | (p == 2) & (t > 0) | (p == 1) & (t == 1))

        @pl.when(active & ((m == 4) | (m == 7) | (m == 14)))
        def _():
            arrived(piece_any, g_kv.at[n_a])
            arrived(piece_any, g_kv.at[n_b])

        def seen(first, i):
            at = pl.ds(pl.multiple_of(first + i * W, W), W)
            return at, (acc_s[at, :] * (1 / sum_s[at, :].sum(axis=1, keepdims=True))).astype(BF16)

        @pl.when(active | last)
        def _():
            keys = [(pl.multiple_of(n_a * B, B), B), (pl.multiple_of(n_b * B, B), B)]

            def group(g, _):
                first = pl.multiple_of(j * 2048 + jnp.where(g == 0, 1 - c, c) * own, own)

                @pl.when(active)
                def _():
                    strips([(pl.multiple_of(first + i * W, W), keys, False) for i in range(4)], False)

                @pl.when(last & (g == 0))
                def _():
                    for i in range(4):
                        at, r = seen(first, i)
                        q_s[at, :] = r
                    o_copy(j).start()

                @pl.when(last & (g == 1))
                def _():
                    h = 4 * c + j
                    for i in range(4):
                        _, r = seen(first, i)
                        wq_s[lax.div(h, 2), pl.ds(pl.multiple_of(lax.rem(h, 2) * own + i * W, W), W), :] = r

            lax.fori_loop(0, 2, group, None)

    lax.fori_loop(0, 18, work, None)
    for half in range(2):
        arrived(wo_any, loc.at[9 + half])
        arrived(wo_any, r_wo.at[4 + half])
        for k in range(3):
            arrived(wo_any, g_wo.at[2 * k + half])
    for j in range(4):
        arrived(q_s.at[:own, :], r_o.at[j])

    def y_copy(i):
        return pltpu.make_async_copy(x_s.at[rows(i, 256), :], y_h.at[rows(i, 256), :], loc.at[i])

    def out(i, _):
        at = pl.multiple_of(i * 256, 256)
        seen = jnp.concatenate([wq_s[h // 2, pl.ds(pl.multiple_of(h % 2 * own + at, 256), 256), :] for h in range(8)], 1)
        for n in range(4):
            cols = slice(512 * n, 512 * (n + 1))
            r = _dot(seen, wo_s[:, cols], 1, 0)
            x_s[pl.ds(at, 256), cols] = (x_s[pl.ds(at, 256), cols].astype(F32) + r).astype(BF16)
        y_copy(i).start()

    lax.fori_loop(0, 4, out, None)

    def left(ref, sem):
        pltpu.make_async_copy(ref, ref, sem).wait()

    for i in range(4):
        left(q_s.at[:own, :], s_o.at[i])
        for k in range(5):
            left(wq_s.at[0, rows(0, 256), :], s_q.at[i, k])
    for i in range(5):
        left(w_mine, s_w.at[i])
    for lot, sent in enumerate((px == 0, py == 0, p > 0)):

        @pl.when(sent)
        def _():
            def one(i, _):
                left(piece_any, s_kv.at[2 * lot + i])

            lo, hi = (0, 2) if lot < 2 else (jnp.where(p == 1, 1, 0), jnp.where(p == 2, 1, 2))
            lax.fori_loop(lo, hi, one, None)

    def forwarded(i, _):
        left(piece_any, f_kv.at[i])

    lax.fori_loop(0, 2 * p + 2, forwarded, None)
    for i in range(8):
        left(wo_any, s_wo.at[i])
    for i in range(6):
        left(wo_any, f_wo.at[i])
    for i in range(4):
        y_copy(i).wait()


def solution(mesh):
    def step(x, gain, wq, wk, wv, wo):
        half = HEAD // 2
        freq = np.asarray([THETA ** (-i / half) for i in range(half)], np.float32)[None]
        hbm, vmem = pl.BlockSpec(memory_space=pl.ANY), pl.BlockSpec(memory_space=pltpu.VMEM)
        dma = pltpu.SemaphoreType.DMA
        return pl.pallas_call(
            _kernel,
            out_shape=jax.ShapeDtypeStruct(x.shape, x.dtype),
            in_specs=[hbm, vmem, vmem, hbm, hbm, hbm, hbm],
            out_specs=hbm,
            scratch_shapes=[
                pltpu.VMEM((2048, 2048), BF16),
                pltpu.VMEM((1024, 2048), BF16),
                pltpu.VMEM((4, 2048, 256), BF16),
                pltpu.VMEM((2, 8192, 256), BF16),
                pltpu.VMEM((4 * 2048, 256), BF16),
                pltpu.VMEM((2048, 2048), BF16),
                pltpu.VMEM((2048, 128), F32),
                pltpu.VMEM((2048, 128), F32),
                pltpu.VMEM((4 * 2048, 256), F32),
                pltpu.VMEM((4 * 2048, 128), F32),
                pltpu.VMEM((4 * 2048, 128), F32),
                dma((11,)),
                dma((4,)), dma((4,)),
                dma((7,)), dma((7,)),
                dma((4, 7)), dma((4, 7)),
                dma((6,)), dma((6,)), dma((8,)), dma((8,)),
                dma((8,)), dma((8,)), dma((6,)), dma((6,)),
                dma((4,)), dma((4,)),
                pltpu.SemaphoreType.REGULAR,
            ],
            compiler_params=pltpu.CompilerParams(collective_id=0, has_side_effects=True, vmem_limit_bytes=67043328),
            name="half_layer",
        )(x, gain, freq, wq, wk, wv, wo)

    tokens, whole = P(("dp", "sp"), None), P("sp", None)
    return jax.shard_map(
        step,
        mesh=mesh,
        in_specs=(tokens, P(None), whole, whole, whole, whole),
        out_specs=tokens,
        check_vma=False,
    )
```

```python
import jax
import jax.numpy as jnp
import numpy as np
from jax import lax
from jax.experimental import pallas as pl
from jax.experimental.pallas import tpu as pltpu
from jax.sharding import PartitionSpec as P

NEG = -1e30
HIDDEN = 2 * NEG
LOG2E = 1.4426950408889634
HEAD = 256
THETA = 10000
W = 256
B = 1024
F32, BF16 = jnp.float32, jnp.bfloat16


def _dot(a, b, ca, cb):
    return lax.dot_general(a, b, (((ca,), (cb,)), ((), ())), preferred_element_type=F32)


def _kernel(x_h, gain_ref, freq_ref, wq_h, wk_h, wv_h, wo_h, y_h,
            a_s, x_s, wq_s, kv_s, q_s, wo_s, cos_s, sin_s, acc_s, top_s, sum_s,
            loc, s_a, r_a, s_w, r_w, s_q, r_q, s_kv, r_kv, f_kv, g_kv, s_wo, r_wo, f_wo, g_wo, s_o, r_o, free):
    me = lax.axis_index("sp")
    c = lax.rem(me, 2)
    p = lax.div(me, 2)
    px, py = lax.div(p, 2), lax.rem(p, 2)
    cx, cy, cd = 2 * (1 - px) + py, 2 * px + 1 - py, 2 * (1 - px) + 1 - py
    chips = (cx, cy, cd)
    mate = 2 * p + 1 - c
    xn, yn = 2 * cx + c, 2 * cy + c
    own = 1024
    w_s = wo_s.at[:, :256]

    def remote(src, dst, ss, rs, dev):
        return pltpu.make_async_remote_copy(src_ref=src, dst_ref=dst, send_sem=ss, recv_sem=rs, device_id={"sp": dev},
                                            device_id_type=pl.DeviceIdType.MESH)

    def arrived(ref, sem):
        pltpu.make_async_copy(ref, ref, sem).wait()

    def rows(i, n):
        return pl.ds(pl.multiple_of(i * n, n), n)

    loads = [pltpu.make_async_copy(x_h.at[rows(i, 256), :], x_s.at[rows(i, 256), :], loc.at[i]) for i in range(4)]
    for t in loads:
        t.start()

    barrier = pltpu.get_barrier_semaphore()
    for dev in (mate, 2 * cx, 2 * cx + 1, 2 * cy, 2 * cy + 1):
        pl.semaphore_signal(barrier, inc=1, device_id={"sp": dev}, device_id_type=pl.DeviceIdType.MESH)
    pl.semaphore_wait(barrier, 5)

    w_mine = w_s.at[rows(me, 256), :]
    for t, w_h in enumerate((wk_h, wv_h)):
        remote(w_h, w_mine, s_w.at[t], r_w.at[c], 2 * cx + t).start()
        remote(w_h, w_mine, s_w.at[2 + t], r_w.at[2 + c], 2 * cy + t).start()

        @pl.when(c == t)
        def _():
            pltpu.make_async_copy(w_h, w_mine, loc.at[4]).start()

        @pl.when(c != t)
        def _():
            remote(w_h, w_mine, s_w.at[4], r_w.at[6], mate).start()

    def wq_part(core, j):
        return wq_h.at[:, pl.ds(pl.multiple_of((4 * core + j) * 256, 256), 256)]

    def wq_own(j, t):
        dst = wq_s.at[j, rows(me, 256), :]
        return [remote(wq_part(t, j), dst, s_q.at[j, t], r_q.at[j, c], 2 * cx + t),
                remote(wq_part(t, j), dst, s_q.at[j, 2 + t], r_q.at[j, 2 + c], 2 * cy + t)]

    def wq_mate(j):
        return remote(wq_part(1 - c, j), wq_s.at[j, rows(me, 256), :], s_q.at[j, 4], r_q.at[j, 6], mate)

    def wq_local(j):
        return pltpu.make_async_copy(wq_part(c, j), wq_s.at[j, rows(me, 256), :], loc.at[5 + j])

    def wq_relay(j):
        fx, fy = wq_s.at[j, rows(2 * cx, 256), :], wq_s.at[j, rows(2 * cy + 1, 256), :]
        return [remote(fx, fx, s_q.at[j, 5], r_q.at[j, 4], yn), remote(fy, fy, s_q.at[j, 6], r_q.at[j, 5], xn)]

    def start(ts):
        for t in ts:
            t.start()

    def a_rows(i):
        return a_s.at[pl.ds(pl.multiple_of(c * own + i * 256, 256), 256), :]

    def a_copy(i):
        return remote(a_rows(i), a_rows(i), s_a.at[i], r_a.at[i], mate)

    start(wq_own(0, 0))
    gain = gain_ref[...].astype(F32)[None]
    for i in range(4):
        loads[i].wait()

        def norm(n, _):
            at = pl.multiple_of(i * 256 + n * 64, 64)
            wide = x_s[pl.ds(at, 64), :].astype(F32)
            scale = lax.rsqrt(jnp.mean(wide * wide, -1, keepdims=True) + 1e-6)
            a_s[pl.ds(pl.multiple_of(c * own + at, 64), 64), :] = (wide * scale * gain).astype(BF16)

        lax.fori_loop(0, 4, norm, None)
        a_copy(i).start()

    def angles(n, _):
        at = pl.multiple_of(n * 64, 64)
        place = (p * 2048 + at + lax.broadcasted_iota(jnp.int32, (64, 128), 0)).astype(F32)
        angle = place * freq_ref[...]
        cos_s[pl.ds(at, 64), :] = jnp.cos(angle)
        sin_s[pl.ds(at, 64), :] = jnp.sin(angle)

    lax.fori_loop(0, 16, angles, None)

    for i in range(4):
        arrived(w_s.at[rows(0, 256), :], r_w.at[i])
    fx, fy = w_s.at[rows(2 * cx, 256), :], w_s.at[rows(2 * cy + 1, 256), :]
    relays_w = [remote(fx, fx, s_w.at[5], r_w.at[4], yn), remote(fy, fy, s_w.at[6], r_w.at[5], xn)]
    start(relays_w)
    start(wq_own(0, 1) + wq_own(1, 0))
    for j in range(4):
        wq_mate(j).start()
        wq_local(j).start()
    lax.fori_loop(16, 32, angles, None)
    for i in range(4):
        arrived(a_rows(0), r_a.at[i])
        arrived(a_rows(0), s_a.at[i])
    arrived(w_mine, loc.at[4])
    for i in (6, 4, 5):
        arrived(w_mine, r_w.at[i])

    def turn(r, at):
        r = r.astype(BF16).astype(F32)
        lo, hi = r[:, :128], r[:, 128:]
        cos, sin = cos_s[pl.ds(at, r.shape[0]), :], sin_s[pl.ds(at, r.shape[0]), :]
        return jnp.concatenate([lo * cos - hi * sin, hi * cos + lo * sin], -1).astype(BF16)

    def piece(n):
        return kv_s.at[c, rows(n, B), :]

    def kv_fwd(n):
        return remote(piece(n), piece(n), f_kv.at[n], g_kv.at[n], mate)

    def kv_own(i, way):
        ref = piece(2 * p + i)
        return remote(ref, ref, s_kv.at[2 * way + i], r_kv.at[2 * way + i], (xn, yn)[way])

    def kvproj(i, _):
        at = pl.multiple_of(i * 512, 512)
        to = pl.ds(pl.multiple_of(p * 2048 + at, 512), 512)
        r = _dot(a_s[pl.ds(at, 512), :], w_s[...], 1, 0)

        @pl.when(c == 0)
        def _():
            kv_s[0, to, :] = turn(r, at)

        @pl.when(c == 1)
        def _():
            kv_s[1, to, :] = r.astype(BF16)

        @pl.when(lax.rem(i, 2) == 1)
        def _():
            kv_fwd(2 * p + lax.div(i, 2)).start()

    lax.fori_loop(0, 4, kvproj, None)
    for i in (5, 6):
        arrived(w_mine, s_w.at[i])

    e = HEAD**-0.5 * LOG2E

    def strips(todo, new):
        scores = [[_dot(q_s[pl.ds(at, W), :], kv_s[0, pl.ds(k, n), :], 1, 1) for k, n in keys] for at, keys, _ in todo]
        weights, keeps = [], []
        for (at, keys, edge), parts in zip(todo, scores):
            s = [t[:, i : i + 128] for t in parts for i in range(0, t.shape[1], 128)]
            if edge:
                gap = lax.broadcasted_iota(jnp.int32, (W, 128), 0) - lax.broadcasted_iota(jnp.int32, (W, 128), 1)
                s[-2] = jnp.where(gap >= 0, s[-2], HIDDEN)
                s[-1] = jnp.where(gap >= 128, s[-1], HIDDEN)
            most = s[0]
            for t in s[1:]:
                most = jnp.maximum(most, t)
            top = jnp.broadcast_to(most.max(axis=1, keepdims=True), (W, 128))
            if not new:
                old = top_s[pl.ds(at, W), :]
                top = jnp.maximum(old, top)
                keeps.append(jnp.exp2((old - top) * e))
            top_s[pl.ds(at, W), :] = top
            w = [jnp.exp2((t - top) * e) for t in s]
            total = w[0]
            for t in w[1:]:
                total = total + t
            sum_s[pl.ds(at, W), :] = total if new else sum_s[pl.ds(at, W), :] * keeps[-1] + total
            weights.append(jnp.concatenate([t.astype(BF16) for t in w], 1))
        for i, (at, keys, _) in enumerate(todo):
            more, col = None, 0
            for k, n in keys:
                r = _dot(weights[i][:, col : col + n], kv_s[1, pl.ds(k, n), :], 1, 0)
                more, col = r if more is None else more + r, col + n
            acc_s[pl.ds(at, W), :] = more if new else acc_s[pl.ds(at, W), :] * jnp.concatenate([keeps[i], keeps[i]], 1) + more

    def wo_rows(dev, half):
        return pl.ds(pl.multiple_of(dev * 256 + half * 128, 128), 128)

    def wo_own(half, way):
        return remote(wo_h.at[rows(half, 128), :], wo_s.at[wo_rows(me, half), :], s_wo.at[2 * way + half], r_wo.at[2 * way + half],
                      (xn, yn, mate)[way])

    def wo_local(half):
        return pltpu.make_async_copy(wo_h.at[rows(half, 128), :], wo_s.at[wo_rows(me, half), :], loc.at[9 + half])

    def wo_fwd(k, half):
        ref = wo_s.at[wo_rows((xn, yn, 2 * cd + c)[k], half), :]
        return remote(ref, ref, f_wo.at[2 * k + half], g_wo.at[2 * k + half], mate)

    def wo_relay(way):
        ref = wo_s.at[wo_rows((xn, yn)[way], way), :]
        return remote(ref, ref, s_wo.at[6 + way], r_wo.at[6 + way], (yn, xn)[way])

    wo_any = wo_s.at[rows(0, 128), :]
    piece_any = piece(0)

    def take(k):
        way, i = (k % 2, k // 2) if k < 4 else (2, k - 4)
        chip = chips[way]
        ref = piece(2 * chip + i)
        slot = 2 * way + i

        @pl.when(chip < p)
        def _():
            arrived(piece_any, r_kv.at[slot])
            kv_fwd(2 * chip + i).start()

        if way == 0:

            @pl.when((p == 3) | (p == 2) & (i == 0))
            def _():
                remote(ref, ref, s_kv.at[4 + i], r_kv.at[4 + i], yn).start()

        if way == 1 and i == 1:

            @pl.when(p == 1)
            def _():
                remote(ref, ref, s_kv.at[4 + i], r_kv.at[4 + i], xn).start()

    def o_copy(j):
        h = 4 * c + j
        dst = wq_s.at[lax.div(h, 2), pl.ds(pl.multiple_of(lax.rem(h, 2) * own, own), own), :]
        return remote(q_s.at[pl.ds(pl.multiple_of(j * 2048 + (1 - c) * own, own), own), :], dst, s_o.at[j], r_o.at[j], mate)

    def wq_pass(j):
        for i in (0, 1, 2, 3):
            arrived(wq_s.at[j, rows(0, 256), :], r_q.at[j, i])
        start(wq_relay(j))

    def kv_send(i):
        for way, at_0 in enumerate((px == 0, py == 0)):

            @pl.when(at_0)
            def _():
                kv_own(i, way).start()

    def work(m, _):
        def at_step(n):
            return pl.when(m == n)

        @pl.when(m < 3)
        def _():
            @at_step(0)
            def _():
                wq_pass(0)
                start(wq_own(1, 1) + wq_own(2, 0))

            @at_step(1)
            def _():
                wq_pass(1)
                kv_send(0)
                start(wq_own(2, 1))
                for i in range(2):
                    arrived(piece(0), g_kv.at[2 * p + i])

        projects = (m < 2) | (m == 5) | (m == 11)
        meets = (m == 1) | (m == 2) | (m == 6) | (m == 12)
        heads = projects | meets

        @pl.when(heads)
        def _():
            @pl.when(meets)
            def _():
                j = jnp.where(m < 3, m - 1, jnp.where(m == 6, 2, 3))
                base, first = j * 2048, pl.multiple_of(p * 2048, 2048)
                strips([(pl.multiple_of(base + i * W, W), [(first, (i + 1) * W)], True) for i in range(7, -1, -1)], True)

            @pl.when(projects)
            def _():
                j = jnp.where(m < 2, m, jnp.where(m == 5, 2, 3))
                arrived(wq_s.at[j, rows(0, 256), :], loc.at[5 + j])
                for i in (6, 4, 5):
                    arrived(wq_s.at[j, rows(0, 256), :], r_q.at[j, i])

                def project(n, _):
                    at = pl.multiple_of(n * 512, 512)
                    r = _dot(a_s[pl.ds(at, 512), :], wq_s[j], 1, 0)
                    q_s[pl.ds(pl.multiple_of(j * 2048 + at, 512), 512), :] = turn(r, at)

                lax.fori_loop(0, 4, project, None)

        @pl.when((m >= 3) & (m < 10))
        def _():
            @at_step(3)
            def _():
                take(0)
                take(1)

            @at_step(4)
            def _():
                wq_pass(2)
                kv_send(1)
                start(wq_own(3, 0) + wq_own(3, 1))

            @pl.when((m == 7) & (p < 3))
            def _():
                take(2)
                take(3)

            @at_step(9)
            def _():
                wq_pass(3)
                start([wo_own(0, 0), wo_own(1, 1), wo_own(1, 0), wo_own(0, 1)])
                for half in range(2):
                    wo_local(half).start()
                    wo_own(half, 2).start()

        @pl.when(m >= 13)
        def _():
            @at_step(13)
            def _():
                take(4)
                take(5)
                for way in range(2):
                    arrived(wo_any, r_wo.at[2 * way + way])
                    wo_relay(way).start()
                    wo_fwd(way, way).start()
                for n in range(4):
                    for k in (5, 6):
                        arrived(wq_s.at[0, rows(0, 256), :], s_q.at[n, k])
                pl.semaphore_signal(free, inc=1, device_id={"sp": mate}, device_id_type=pl.DeviceIdType.MESH)

            @at_step(15)
            def _():
                pl.semaphore_wait(free, 1)
                for way in range(2):
                    arrived(wo_any, r_wo.at[2 * way + 1 - way])
                    wo_fwd(way, 1 - way).start()

            @at_step(17)
            def _():
                for half in range(2):
                    arrived(wo_any, r_wo.at[6 + half])
                    wo_fwd(2, half).start()

        last = m >= 15
        t = jnp.where(last, 2, jnp.where((m >= 8) & (m <= 10) | (m == 14), 1, 0))
        j = jnp.where(last, m - 15, jnp.where(m >= 13, 3, jnp.where(m >= 8, m - 8, jnp.where(m == 7, 2, m - 3))))
        lone = jnp.where(p == 1, cy, jnp.where(last, cd, cx))
        both = (p == 3) & (t < 2)
        n_a, n_b = jnp.where(both, 2 * cx + t, 2 * lone), jnp.where(both, 2 * cy + t, 2 * lone + 1)
        active = jnp.logical_not(heads) & ((p == 3) | (p == 2) & (t > 0) | (p == 1) & (t == 1))

        @pl.when(active & ((m == 3) | (m == 8) | (m == 15)))
        def _():
            arrived(piece_any, g_kv.at[n_a])
            arrived(piece_any, g_kv.at[n_b])

        def seen(first, i):
            at = pl.ds(pl.multiple_of(first + i * W, W), W)
            return at, (acc_s[at, :] * (1 / sum_s[at, :].sum(axis=1, keepdims=True))).astype(BF16)

        @pl.when(active | last)
        def _():
            keys = [(pl.multiple_of(n_a * B, B), B), (pl.multiple_of(n_b * B, B), B)]

            def group(g, _):
                first = pl.multiple_of(j * 2048 + jnp.where(g == 0, 1 - c, c) * own, own)

                @pl.when((m == 7) & (g == 1))
                def _():
                    take(2)
                    take(3)

                @pl.when(active)
                def _():
                    strips([(pl.multiple_of(first + i * W, W), keys, False) for i in range(4)], False)

                @pl.when(last & (g == 0))
                def _():
                    for i in range(4):
                        at, r = seen(first, i)
                        q_s[at, :] = r
                    o_copy(j).start()

                @pl.when(last & (g == 1))
                def _():
                    h = 4 * c + j
                    for i in range(4):
                        _, r = seen(first, i)
                        wq_s[lax.div(h, 2), pl.ds(pl.multiple_of(lax.rem(h, 2) * own + i * W, W), W), :] = r

            lax.fori_loop(0, 2, group, None)

    lax.fori_loop(0, 19, work, None)
    for half in range(2):
        arrived(wo_any, loc.at[9 + half])
        arrived(wo_any, r_wo.at[4 + half])
        for k in range(3):
            arrived(wo_any, g_wo.at[2 * k + half])
    for j in range(4):
        arrived(q_s.at[:own, :], r_o.at[j])

    def y_copy(i):
        return pltpu.make_async_copy(x_s.at[rows(i, 256), :], y_h.at[rows(i, 256), :], loc.at[i])

    def out(i, _):
        at = pl.multiple_of(i * 256, 256)
        seen = jnp.concatenate([wq_s[h // 2, pl.ds(pl.multiple_of(h % 2 * own + at, 256), 256), :] for h in range(8)], 1)
        for n in range(4):
            cols = slice(512 * n, 512 * (n + 1))
            r = _dot(seen, wo_s[:, cols], 1, 0)
            x_s[pl.ds(at, 256), cols] = (x_s[pl.ds(at, 256), cols].astype(F32) + r).astype(BF16)
        y_copy(i).start()

    lax.fori_loop(0, 4, out, None)

    def left(ref, sem):
        pltpu.make_async_copy(ref, ref, sem).wait()

    for i in range(4):
        left(q_s.at[:own, :], s_o.at[i])
        for k in range(5):
            left(wq_s.at[0, rows(0, 256), :], s_q.at[i, k])
    for i in range(5):
        left(w_mine, s_w.at[i])
    for lot, sent in enumerate((px == 0, py == 0, p > 0)):

        @pl.when(sent)
        def _():
            def one(i, _):
                left(piece_any, s_kv.at[2 * lot + i])

            lo, hi = (0, 2) if lot < 2 else (jnp.where(p == 1, 1, 0), jnp.where(p == 2, 1, 2))
            lax.fori_loop(lo, hi, one, None)

    def forwarded(i, _):
        left(piece_any, f_kv.at[i])

    lax.fori_loop(0, 2 * p + 2, forwarded, None)
    for i in range(8):
        left(wo_any, s_wo.at[i])
    for i in range(6):
        left(wo_any, f_wo.at[i])
    for i in range(4):
        y_copy(i).wait()


def solution(mesh):
    def step(x, gain, wq, wk, wv, wo):
        half = HEAD // 2
        freq = np.asarray([THETA ** (-i / half) for i in range(half)], np.float32)[None]
        hbm, vmem = pl.BlockSpec(memory_space=pl.ANY), pl.BlockSpec(memory_space=pltpu.VMEM)
        dma = pltpu.SemaphoreType.DMA
        return pl.pallas_call(
            _kernel,
            out_shape=jax.ShapeDtypeStruct(x.shape, x.dtype),
            in_specs=[hbm, vmem, vmem, hbm, hbm, hbm, hbm],
            out_specs=hbm,
            scratch_shapes=[
                pltpu.VMEM((2048, 2048), BF16),
                pltpu.VMEM((1024, 2048), BF16),
                pltpu.VMEM((4, 2048, 256), BF16),
                pltpu.VMEM((2, 8192, 256), BF16),
                pltpu.VMEM((4 * 2048, 256), BF16),
                pltpu.VMEM((2048, 2048), BF16),
                pltpu.VMEM((2048, 128), F32),
                pltpu.VMEM((2048, 128), F32),
                pltpu.VMEM((4 * 2048, 256), F32),
                pltpu.VMEM((4 * 2048, 128), F32),
                pltpu.VMEM((4 * 2048, 128), F32),
                dma((11,)),
                dma((4,)), dma((4,)),
                dma((7,)), dma((7,)),
                dma((4, 7)), dma((4, 7)),
                dma((6,)), dma((6,)), dma((8,)), dma((8,)),
                dma((8,)), dma((8,)), dma((6,)), dma((6,)),
                dma((4,)), dma((4,)),
                pltpu.SemaphoreType.REGULAR,
            ],
            compiler_params=pltpu.CompilerParams(collective_id=0, has_side_effects=True, vmem_limit_bytes=67043328),
            name="half_layer",
        )(x, gain, freq, wq, wk, wv, wo)

    tokens, whole = P(("dp", "sp"), None), P("sp", None)
    return jax.shard_map(
        step,
        mesh=mesh,
        in_specs=(tokens, P(None), whole, whole, whole, whole),
        out_specs=tokens,
        check_vma=False,
    )
```

```python
import jax
import jax.numpy as jnp
import numpy as np
from jax import lax
from jax.experimental import pallas as pl
from jax.experimental.pallas import tpu as pltpu
from jax.sharding import PartitionSpec as P

NEG = -1e30
HIDDEN = 2 * NEG
LOG2E = 1.4426950408889634
HEAD = 256
THETA = 10000
W = 256
B = 1024
F32, BF16 = jnp.float32, jnp.bfloat16


def _dot(a, b, ca, cb):
    return lax.dot_general(a, b, (((ca,), (cb,)), ((), ())), preferred_element_type=F32)


def _kernel(x_h, gain_ref, freq_ref, wq_h, wk_h, wv_h, wo_h, y_h,
            a_s, x_s, wq_s, kv_s, q_s, wo_s, cos_s, sin_s, acc_s, top_s, sum_s,
            loc, s_a, r_a, s_w, r_w, s_q, r_q, s_kv, r_kv, f_kv, g_kv, s_wo, r_wo, f_wo, g_wo, s_o, r_o, free):
    me = lax.axis_index("sp")
    c = lax.rem(me, 2)
    p = lax.div(me, 2)
    px, py = lax.div(p, 2), lax.rem(p, 2)
    cx, cy, cd = 2 * (1 - px) + py, 2 * px + 1 - py, 2 * (1 - px) + 1 - py
    chips = (cx, cy, cd)
    mate = 2 * p + 1 - c
    xn, yn = 2 * cx + c, 2 * cy + c
    own = 1024
    w_s = wo_s.at[:, :256]

    def remote(src, dst, ss, rs, dev):
        return pltpu.make_async_remote_copy(src_ref=src, dst_ref=dst, send_sem=ss, recv_sem=rs, device_id={"sp": dev},
                                            device_id_type=pl.DeviceIdType.MESH)

    def arrived(ref, sem):
        pltpu.make_async_copy(ref, ref, sem).wait()

    def rows(i, n):
        return pl.ds(pl.multiple_of(i * n, n), n)

    loads = [pltpu.make_async_copy(x_h.at[rows(i, 256), :], x_s.at[rows(i, 256), :], loc.at[i]) for i in range(4)]
    for t in loads:
        t.start()

    barrier = pltpu.get_barrier_semaphore()
    for dev in (mate, 2 * cx, 2 * cx + 1, 2 * cy, 2 * cy + 1):
        pl.semaphore_signal(barrier, inc=1, device_id={"sp": dev}, device_id_type=pl.DeviceIdType.MESH)
    pl.semaphore_wait(barrier, 5)

    w_mine = w_s.at[rows(me, 256), :]
    for t, w_h in enumerate((wk_h, wv_h)):
        remote(w_h, w_mine, s_w.at[t], r_w.at[c], 2 * cx + t).start()
        remote(w_h, w_mine, s_w.at[2 + t], r_w.at[2 + c], 2 * cy + t).start()

        @pl.when(c == t)
        def _():
            pltpu.make_async_copy(w_h, w_mine, loc.at[4]).start()

        @pl.when(c != t)
        def _():
            remote(w_h, w_mine, s_w.at[4], r_w.at[6], mate).start()

    def wq_part(core, j):
        return wq_h.at[:, pl.ds(pl.multiple_of((4 * core + j) * 256, 256), 256)]

    def wq_own(j, t):
        dst = wq_s.at[j, rows(me, 256), :]
        return [remote(wq_part(t, j), dst, s_q.at[j, t], r_q.at[j, c], 2 * cx + t),
                remote(wq_part(t, j), dst, s_q.at[j, 2 + t], r_q.at[j, 2 + c], 2 * cy + t)]

    def wq_mate(j):
        return remote(wq_part(1 - c, j), wq_s.at[j, rows(me, 256), :], s_q.at[j, 4], r_q.at[j, 6], mate)

    def wq_local(j):
        return pltpu.make_async_copy(wq_part(c, j), wq_s.at[j, rows(me, 256), :], loc.at[5 + j])

    def wq_relay(j):
        fx, fy = wq_s.at[j, rows(2 * cx, 256), :], wq_s.at[j, rows(2 * cy + 1, 256), :]
        return [remote(fx, fx, s_q.at[j, 5], r_q.at[j, 4], yn), remote(fy, fy, s_q.at[j, 6], r_q.at[j, 5], xn)]

    def start(ts):
        for t in ts:
            t.start()

    def a_rows(i):
        return a_s.at[pl.ds(pl.multiple_of(c * own + i * 256, 256), 256), :]

    def a_copy(i):
        return remote(a_rows(i), a_rows(i), s_a.at[i], r_a.at[i], mate)

    start(wq_own(0, 0))
    gain = gain_ref[...].astype(F32)[None]
    for i in range(4):
        loads[i].wait()

        def norm(n, _):
            at = pl.multiple_of(i * 256 + n * 64, 64)
            wide = x_s[pl.ds(at, 64), :].astype(F32)
            scale = lax.rsqrt(jnp.mean(wide * wide, -1, keepdims=True) + 1e-6)
            a_s[pl.ds(pl.multiple_of(c * own + at, 64), 64), :] = (wide * scale * gain).astype(BF16)

        lax.fori_loop(0, 4, norm, None)
        a_copy(i).start()

    def angles(n, _):
        at = pl.multiple_of(n * 64, 64)
        place = (p * 2048 + at + lax.broadcasted_iota(jnp.int32, (64, 128), 0)).astype(F32)
        angle = place * freq_ref[...]
        cos_s[pl.ds(at, 64), :] = jnp.cos(angle)
        sin_s[pl.ds(at, 64), :] = jnp.sin(angle)

    lax.fori_loop(0, 16, angles, None)

    for i in range(4):
        arrived(w_s.at[rows(0, 256), :], r_w.at[i])
    fx, fy = w_s.at[rows(2 * cx, 256), :], w_s.at[rows(2 * cy + 1, 256), :]
    relays_w = [remote(fx, fx, s_w.at[5], r_w.at[4], yn), remote(fy, fy, s_w.at[6], r_w.at[5], xn)]
    start(relays_w)
    start(wq_own(0, 1) + wq_own(1, 0))
    for j in range(4):
        wq_mate(j).start()
        wq_local(j).start()
    lax.fori_loop(16, 32, angles, None)
    for i in range(4):
        arrived(a_rows(0), r_a.at[i])
        arrived(a_rows(0), s_a.at[i])
    arrived(w_mine, loc.at[4])
    for i in (6, 4, 5):
        arrived(w_mine, r_w.at[i])

    def turn(r, at):
        r = r.astype(BF16).astype(F32)
        lo, hi = r[:, :128], r[:, 128:]
        cos, sin = cos_s[pl.ds(at, r.shape[0]), :], sin_s[pl.ds(at, r.shape[0]), :]
        return jnp.concatenate([lo * cos - hi * sin, hi * cos + lo * sin], -1).astype(BF16)

    def piece(n):
        return kv_s.at[c, rows(n, B), :]

    def kv_fwd(n):
        return remote(piece(n), piece(n), f_kv.at[n], g_kv.at[n], mate)

    def kv_own(i, way):
        ref = piece(2 * p + i)
        return remote(ref, ref, s_kv.at[2 * way + i], r_kv.at[2 * way + i], (xn, yn)[way])

    def kvproj(i, _):
        at = pl.multiple_of(i * 512, 512)
        to = pl.ds(pl.multiple_of(p * 2048 + at, 512), 512)
        r = _dot(a_s[pl.ds(at, 512), :], w_s[...], 1, 0)

        @pl.when(c == 0)
        def _():
            kv_s[0, to, :] = turn(r, at)

        @pl.when(c == 1)
        def _():
            kv_s[1, to, :] = r.astype(BF16)

        @pl.when(lax.rem(i, 2) == 1)
        def _():
            kv_fwd(2 * p + lax.div(i, 2)).start()

    lax.fori_loop(0, 4, kvproj, None)
    for i in (5, 6):
        arrived(w_mine, s_w.at[i])

    e = HEAD**-0.5 * LOG2E

    def strips(todo, new):
        scores = [[_dot(q_s[pl.ds(at, W), :], kv_s[0, pl.ds(k, n), :], 1, 1) for k, n in keys] for at, keys, _ in todo]
        weights, keeps = [], []
        for (at, keys, edge), parts in zip(todo, scores):
            s = [t[:, i : i + 128] for t in parts for i in range(0, t.shape[1], 128)]
            if edge:
                gap = lax.broadcasted_iota(jnp.int32, (W, 128), 0) - lax.broadcasted_iota(jnp.int32, (W, 128), 1)
                s[-2] = jnp.where(gap >= 0, s[-2], HIDDEN)
                s[-1] = jnp.where(gap >= 128, s[-1], HIDDEN)
            most = s[0]
            for t in s[1:]:
                most = jnp.maximum(most, t)
            top = jnp.broadcast_to(most.max(axis=1, keepdims=True), (W, 128))
            if not new:
                old = top_s[pl.ds(at, W), :]
                top = jnp.maximum(old, top)
                keeps.append(jnp.exp2((old - top) * e))
            top_s[pl.ds(at, W), :] = top
            w = [jnp.exp2((t - top) * e) for t in s]
            total = w[0]
            for t in w[1:]:
                total = total + t
            sum_s[pl.ds(at, W), :] = total if new else sum_s[pl.ds(at, W), :] * keeps[-1] + total
            weights.append(jnp.concatenate([t.astype(BF16) for t in w], 1))
        for i, (at, keys, _) in enumerate(todo):
            more, col = None, 0
            for k, n in keys:
                r = _dot(weights[i][:, col : col + n], kv_s[1, pl.ds(k, n), :], 1, 0)
                more, col = r if more is None else more + r, col + n
            acc_s[pl.ds(at, W), :] = more if new else acc_s[pl.ds(at, W), :] * jnp.concatenate([keeps[i], keeps[i]], 1) + more

    def wo_rows(dev, half):
        return pl.ds(pl.multiple_of(dev * 256 + half * 128, 128), 128)

    def wo_own(half, way):
        return remote(wo_h.at[rows(half, 128), :], wo_s.at[wo_rows(me, half), :], s_wo.at[2 * way + half], r_wo.at[2 * way + half],
                      (xn, yn, mate)[way])

    def wo_local(half):
        return pltpu.make_async_copy(wo_h.at[rows(half, 128), :], wo_s.at[wo_rows(me, half), :], loc.at[9 + half])

    def wo_fwd(k, half):
        ref = wo_s.at[wo_rows((xn, yn, 2 * cd + c)[k], half), :]
        return remote(ref, ref, f_wo.at[2 * k + half], g_wo.at[2 * k + half], mate)

    def wo_relay(way):
        ref = wo_s.at[wo_rows((xn, yn)[way], way), :]
        return remote(ref, ref, s_wo.at[6 + way], r_wo.at[6 + way], (yn, xn)[way])

    wo_any = wo_s.at[rows(0, 128), :]
    piece_any = piece(0)

    def take(k):
        way, i = (k % 2, k // 2) if k < 4 else (2, k - 4)
        chip = chips[way]
        ref = piece(2 * chip + i)
        slot = 2 * way + i

        @pl.when(chip < p)
        def _():
            arrived(piece_any, r_kv.at[slot])
            kv_fwd(2 * chip + i).start()

        if way == 0:

            @pl.when((p == 3) | (p == 2) & (i == 0))
            def _():
                remote(ref, ref, s_kv.at[4 + i], r_kv.at[4 + i], yn).start()

        if way == 1 and i == 1:

            @pl.when(p == 1)
            def _():
                remote(ref, ref, s_kv.at[4 + i], r_kv.at[4 + i], xn).start()

    def o_copy(j):
        h = 4 * c + j
        dst = wq_s.at[lax.div(h, 2), pl.ds(pl.multiple_of(lax.rem(h, 2) * own, own), own), :]
        return remote(q_s.at[pl.ds(pl.multiple_of(j * 2048 + (1 - c) * own, own), own), :], dst, s_o.at[j], r_o.at[j], mate)

    def wq_pass(j):
        for i in (0, 1, 2, 3):
            arrived(wq_s.at[j, rows(0, 256), :], r_q.at[j, i])
        start(wq_relay(j))

    def work(m, _):
        def at_step(n):
            return pl.when(m == n)

        @pl.when(m < 3)
        def _():
            @at_step(0)
            def _():
                wq_pass(0)
                start(wq_own(1, 1) + wq_own(2, 0))

            @at_step(1)
            def _():
                wq_pass(1)
                start(wq_own(2, 1))
                for i in range(2):
                    arrived(piece(0), g_kv.at[2 * p + i])

            @at_step(2)
            def _():
                wq_pass(2)
                for way, at_0 in enumerate((px == 0, py == 0)):

                    @pl.when(at_0)
                    def _():
                        start([kv_own(i, way) for i in range(2)])

                start(wq_own(3, 0) + wq_own(3, 1))

        heads = (m < 4) | (m == 10) | (m == 11)
        late = m >= 10

        @pl.when(heads)
        def _():
            j = jnp.where(late, m - 7, m)

            @pl.when((m != 0) & (m != 10))
            def _():
                base, first = (j - 1) * 2048, pl.multiple_of(p * 2048, 2048)
                strips([(pl.multiple_of(base + i * W, W), [(first, (i + 1) * W)], True) for i in range(7, -1, -1)], True)

            @pl.when((m != 3) & (m != 11))
            def _():
                arrived(wq_s.at[j, rows(0, 256), :], loc.at[5 + j])
                for i in (6, 4, 5):
                    arrived(wq_s.at[j, rows(0, 256), :], r_q.at[j, i])

                def project(n, _):
                    at = pl.multiple_of(n * 512, 512)
                    r = _dot(a_s[pl.ds(at, 512), :], wq_s[j], 1, 0)
                    q_s[pl.ds(pl.multiple_of(j * 2048 + at, 512), 512), :] = turn(r, at)

                lax.fori_loop(0, 4, project, None)

        @pl.when((m >= 4) & (m < 10))
        def _():
            @at_step(4)
            def _():
                take(0)
                take(1)

            @at_step(6)
            def _():
                take(2)
                take(3)

            @at_step(8)
            def _():
                wq_pass(3)
                start([wo_own(0, 0), wo_own(1, 1), wo_own(1, 0), wo_own(0, 1)])
                for half in range(2):
                    wo_local(half).start()
                    wo_own(half, 2).start()

        @pl.when(m >= 12)
        def _():
            @at_step(12)
            def _():
                take(4)
                take(5)
                for way in range(2):
                    arrived(wo_any, r_wo.at[2 * way + way])
                    wo_relay(way).start()
                    wo_fwd(way, way).start()
                for n in range(4):
                    for k in (5, 6):
                        arrived(wq_s.at[0, rows(0, 256), :], s_q.at[n, k])
                pl.semaphore_signal(free, inc=1, device_id={"sp": mate}, device_id_type=pl.DeviceIdType.MESH)

            @at_step(14)
            def _():
                pl.semaphore_wait(free, 1)
                for way in range(2):
                    arrived(wo_any, r_wo.at[2 * way + 1 - way])
                    wo_fwd(way, 1 - way).start()

            @at_step(16)
            def _():
                for half in range(2):
                    arrived(wo_any, r_wo.at[6 + half])
                    wo_fwd(2, half).start()

        last = m >= 14
        n = m - 4
        t = jnp.where(last, 2, jnp.where(late, m - 12, lax.div(n, 3)))
        j = jnp.where(last, m - 14, jnp.where(late, 3, lax.rem(n, 3)))
        lone = jnp.where(p == 1, cy, jnp.where(last, cd, cx))
        both = (p == 3) & (t < 2)
        n_a, n_b = jnp.where(both, 2 * cx + t, 2 * lone), jnp.where(both, 2 * cy + t, 2 * lone + 1)
        active = jnp.logical_not(heads) & ((p == 3) | (p == 2) & (t > 0) | (p == 1) & (t == 1))

        @pl.when(active & ((m == 4) | (m == 7) | (m == 14)))
        def _():
            arrived(piece_any, g_kv.at[n_a])
            arrived(piece_any, g_kv.at[n_b])

        def seen(first, i):
            at = pl.ds(pl.multiple_of(first + i * W, W), W)
            return at, (acc_s[at, :] * (1 / sum_s[at, :].sum(axis=1, keepdims=True))).astype(BF16)

        @pl.when(active | last)
        def _():
            keys = [(pl.multiple_of(n_a * B, B), B), (pl.multiple_of(n_b * B, B), B)]

            def group(g, _):
                first = pl.multiple_of(j * 2048 + jnp.where(g == 0, 1 - c, c) * own, own)

                @pl.when(active)
                def _():
                    strips([(pl.multiple_of(first + i * W, W), keys, False) for i in range(4)], False)

                @pl.when(last & (g == 0))
                def _():
                    for i in range(4):
                        at, r = seen(first, i)
                        q_s[at, :] = r
                    o_copy(j).start()

                @pl.when(last & (g == 1))
                def _():
                    h = 4 * c + j
                    for i in range(4):
                        _, r = seen(first, i)
                        wq_s[lax.div(h, 2), pl.ds(pl.multiple_of(lax.rem(h, 2) * own + i * W, W), W), :] = r

            lax.fori_loop(0, 2, group, None)

    lax.fori_loop(0, 18, work, None)
    for half in range(2):
        arrived(wo_any, loc.at[9 + half])
        arrived(wo_any, r_wo.at[4 + half])
        for k in range(3):
            arrived(wo_any, g_wo.at[2 * k + half])
    for j in range(4):
        arrived(q_s.at[:own, :], r_o.at[j])

    def y_copy(i):
        return pltpu.make_async_copy(x_s.at[rows(i, 256), :], y_h.at[rows(i, 256), :], loc.at[i])

    def out(i, _):
        at = pl.multiple_of(i * 256, 256)
        seen = jnp.concatenate([wq_s[h // 2, pl.ds(pl.multiple_of(h % 2 * own + at, 256), 256), :] for h in range(8)], 1)
        for n in range(4):
            cols = slice(512 * n, 512 * (n + 1))
            r = _dot(seen, wo_s[:, cols], 1, 0)
            x_s[pl.ds(at, 256), cols] = (x_s[pl.ds(at, 256), cols].astype(F32) + r).astype(BF16)
        y_copy(i).start()

    lax.fori_loop(0, 4, out, None)

    def left(ref, sem):
        pltpu.make_async_copy(ref, ref, sem).wait()

    for i in range(4):
        left(q_s.at[:own, :], s_o.at[i])
        for k in range(5):
            left(wq_s.at[0, rows(0, 256), :], s_q.at[i, k])
    for i in range(5):
        left(w_mine, s_w.at[i])
    for lot, sent in enumerate((px == 0, py == 0, p > 0)):

        @pl.when(sent)
        def _():
            def one(i, _):
                left(piece_any, s_kv.at[2 * lot + i])

            lo, hi = (0, 2) if lot < 2 else (jnp.where(p == 1, 1, 0), jnp.where(p == 2, 1, 2))
            lax.fori_loop(lo, hi, one, None)

    def forwarded(i, _):
        left(piece_any, f_kv.at[i])

    lax.fori_loop(0, 2 * p + 2, forwarded, None)
    for i in range(8):
        left(wo_any, s_wo.at[i])
    for i in range(6):
        left(wo_any, f_wo.at[i])
    for i in range(4):
        y_copy(i).wait()


def solution(mesh):
    def step(x, gain, wq, wk, wv, wo):
        half = HEAD // 2
        freq = np.asarray([THETA ** (-i / half) for i in range(half)], np.float32)[None]
        hbm, vmem = pl.BlockSpec(memory_space=pl.ANY), pl.BlockSpec(memory_space=pltpu.VMEM)
        dma = pltpu.SemaphoreType.DMA
        return pl.pallas_call(
            _kernel,
            out_shape=jax.ShapeDtypeStruct(x.shape, x.dtype),
            in_specs=[hbm, vmem, vmem, hbm, hbm, hbm, hbm],
            out_specs=hbm,
            scratch_shapes=[
                pltpu.VMEM((2048, 2048), BF16),
                pltpu.VMEM((1024, 2048), BF16),
                pltpu.VMEM((4, 2048, 256), BF16),
                pltpu.VMEM((2, 8192, 256), BF16),
                pltpu.VMEM((4 * 2048, 256), BF16),
                pltpu.VMEM((2048, 2048), BF16),
                pltpu.VMEM((2048, 128), F32),
                pltpu.VMEM((2048, 128), F32),
                pltpu.VMEM((4 * 2048, 256), F32),
                pltpu.VMEM((4 * 2048, 128), F32),
                pltpu.VMEM((4 * 2048, 128), F32),
                dma((11,)),
                dma((4,)), dma((4,)),
                dma((7,)), dma((7,)),
                dma((4, 7)), dma((4, 7)),
                dma((6,)), dma((6,)), dma((8,)), dma((8,)),
                dma((8,)), dma((8,)), dma((6,)), dma((6,)),
                dma((4,)), dma((4,)),
                pltpu.SemaphoreType.REGULAR,
            ],
            compiler_params=pltpu.CompilerParams(collective_id=0, has_side_effects=True, vmem_limit_bytes=67043328),
            name="half_layer",
        )(x, gain, freq, wq, wk, wv, wo)

    tokens, whole = P(("dp", "sp"), None), P("sp", None)
    return jax.shard_map(
        step,
        mesh=mesh,
        in_specs=(tokens, P(None), whole, whole, whole, whole),
        out_specs=tokens,
        check_vma=False,
    )
```

```python
import jax
import jax.numpy as jnp
import numpy as np
from jax import lax
from jax.experimental import pallas as pl
from jax.experimental.pallas import tpu as pltpu
from jax.sharding import PartitionSpec as P

NEG = -1e30
HIDDEN = 2 * NEG
LOG2E = 1.4426950408889634
HEAD = 256
THETA = 10000
W = 256
B = 1024
F32, BF16 = jnp.float32, jnp.bfloat16


def _dot(a, b, ca, cb):
    return lax.dot_general(a, b, (((ca,), (cb,)), ((), ())), preferred_element_type=F32)


def _kernel(x_h, gain_ref, freq_ref, wq_h, wk_h, wv_h, wo_h, y_h,
            a_s, x_s, wq_s, kv_s, q_s, wo_s, cos_s, sin_s, acc_s, top_s, sum_s,
            loc, s_a, r_a, s_w, r_w, s_q, r_q, s_kv, r_kv, f_kv, g_kv, s_wo, r_wo, f_wo, g_wo, s_o, r_o, free):
    me = lax.axis_index("sp")
    c = lax.rem(me, 2)
    p = lax.div(me, 2)
    px, py = lax.div(p, 2), lax.rem(p, 2)
    cx, cy, cd = 2 * (1 - px) + py, 2 * px + 1 - py, 2 * (1 - px) + 1 - py
    chips = (cx, cy, cd)
    mate = 2 * p + 1 - c
    xn, yn = 2 * cx + c, 2 * cy + c
    own = 1024
    w_s = wo_s.at[:, :256]

    def remote(src, dst, ss, rs, dev):
        return pltpu.make_async_remote_copy(src_ref=src, dst_ref=dst, send_sem=ss, recv_sem=rs, device_id={"sp": dev},
                                            device_id_type=pl.DeviceIdType.MESH)

    def arrived(ref, sem):
        pltpu.make_async_copy(ref, ref, sem).wait()

    def rows(i, n):
        return pl.ds(pl.multiple_of(i * n, n), n)

    loads = [pltpu.make_async_copy(x_h.at[rows(i, 256), :], x_s.at[rows(i, 256), :], loc.at[i]) for i in range(4)]
    for t in loads:
        t.start()

    barrier = pltpu.get_barrier_semaphore()
    for dev in (mate, 2 * cx, 2 * cx + 1, 2 * cy, 2 * cy + 1):
        pl.semaphore_signal(barrier, inc=1, device_id={"sp": dev}, device_id_type=pl.DeviceIdType.MESH)
    pl.semaphore_wait(barrier, 5)

    w_mine = w_s.at[rows(me, 256), :]
    for t, w_h in enumerate((wk_h, wv_h)):
        remote(w_h, w_mine, s_w.at[t], r_w.at[c], 2 * cx + t).start()
        remote(w_h, w_mine, s_w.at[2 + t], r_w.at[2 + c], 2 * cy + t).start()

        @pl.when(c == t)
        def _():
            pltpu.make_async_copy(w_h, w_mine, loc.at[4]).start()

        @pl.when(c != t)
        def _():
            remote(w_h, w_mine, s_w.at[4], r_w.at[6], mate).start()

    def wq_part(core, j):
        return wq_h.at[:, pl.ds(pl.multiple_of((4 * core + j) * 256, 256), 256)]

    def wq_own(j, t):
        dst = wq_s.at[j, rows(me, 256), :]
        return [remote(wq_part(t, j), dst, s_q.at[j, t], r_q.at[j, c], 2 * cx + t),
                remote(wq_part(t, j), dst, s_q.at[j, 2 + t], r_q.at[j, 2 + c], 2 * cy + t)]

    def wq_mate(j):
        return remote(wq_part(1 - c, j), wq_s.at[j, rows(me, 256), :], s_q.at[j, 4], r_q.at[j, 6], mate)

    def wq_local(j):
        return pltpu.make_async_copy(wq_part(c, j), wq_s.at[j, rows(me, 256), :], loc.at[5 + j])

    def wq_relay(j):
        fx, fy = wq_s.at[j, rows(2 * cx, 256), :], wq_s.at[j, rows(2 * cy + 1, 256), :]
        return [remote(fx, fx, s_q.at[j, 5], r_q.at[j, 4], yn), remote(fy, fy, s_q.at[j, 6], r_q.at[j, 5], xn)]

    def start(ts):
        for t in ts:
            t.start()

    def a_rows(i):
        return a_s.at[pl.ds(pl.multiple_of(c * own + i * 256, 256), 256), :]

    def a_copy(i):
        return remote(a_rows(i), a_rows(i), s_a.at[i], r_a.at[i], mate)

    start(wq_own(0, 0))
    gain = gain_ref[...].astype(F32)[None]
    for i in range(4):
        loads[i].wait()

        def norm(n, _):
            at = pl.multiple_of(i * 256 + n * 64, 64)
            wide = x_s[pl.ds(at, 64), :].astype(F32)
            scale = lax.rsqrt(jnp.mean(wide * wide, -1, keepdims=True) + 1e-6)
            a_s[pl.ds(pl.multiple_of(c * own + at, 64), 64), :] = (wide * scale * gain).astype(BF16)

        lax.fori_loop(0, 4, norm, None)
        a_copy(i).start()

    def angles(n, _):
        at = pl.multiple_of(n * 64, 64)
        place = (p * 2048 + at + lax.broadcasted_iota(jnp.int32, (64, 128), 0)).astype(F32)
        angle = place * freq_ref[...]
        cos_s[pl.ds(at, 64), :] = jnp.cos(angle)
        sin_s[pl.ds(at, 64), :] = jnp.sin(angle)

    lax.fori_loop(0, 16, angles, None)

    for i in range(4):
        arrived(w_s.at[rows(0, 256), :], r_w.at[i])
    fx, fy = w_s.at[rows(2 * cx, 256), :], w_s.at[rows(2 * cy + 1, 256), :]
    relays_w = [remote(fx, fx, s_w.at[5], r_w.at[4], yn), remote(fy, fy, s_w.at[6], r_w.at[5], xn)]
    start(relays_w)
    start(wq_own(0, 1) + wq_own(1, 0))
    for j in range(4):
        wq_mate(j).start()
        wq_local(j).start()
    lax.fori_loop(16, 32, angles, None)
    for i in range(4):
        arrived(a_rows(0), r_a.at[i])
        arrived(a_rows(0), s_a.at[i])
    arrived(w_mine, loc.at[4])
    for i in (6, 4, 5):
        arrived(w_mine, r_w.at[i])

    def turn(r, at):
        r = r.astype(BF16).astype(F32)
        lo, hi = r[:, :128], r[:, 128:]
        cos, sin = cos_s[pl.ds(at, r.shape[0]), :], sin_s[pl.ds(at, r.shape[0]), :]
        return jnp.concatenate([lo * cos - hi * sin, hi * cos + lo * sin], -1).astype(BF16)

    def piece(n):
        return kv_s.at[c, rows(n, B), :]

    def kv_fwd(n):
        return remote(piece(n), piece(n), f_kv.at[n], g_kv.at[n], mate)

    def kv_own(i, way):
        ref = piece(2 * p + i)
        return remote(ref, ref, s_kv.at[2 * way + i], r_kv.at[2 * way + i], (xn, yn)[way])

    def kv_start(h):
        ref = kv_s.at[c, rows(4 * p + h, B // 2), :]
        for way, at_0 in enumerate((px == 0, py == 0)):

            @pl.when(at_0)
            def _():
                remote(ref, ref, s_kv.at[2 * way], r_kv.at[2 * way], (xn, yn)[way]).start()

    def kvproj(i, _):
        at = pl.multiple_of(i * 512, 512)
        to = pl.ds(pl.multiple_of(p * 2048 + at, 512), 512)
        r = _dot(a_s[pl.ds(at, 512), :], w_s[...], 1, 0)

        @pl.when(c == 0)
        def _():
            kv_s[0, to, :] = turn(r, at)

        @pl.when(c == 1)
        def _():
            kv_s[1, to, :] = r.astype(BF16)

        @pl.when(lax.rem(i, 2) == 1)
        def _():
            kv_fwd(2 * p + lax.div(i, 2)).start()

    lax.fori_loop(0, 4, kvproj, None)
    for i in (5, 6):
        arrived(w_mine, s_w.at[i])

    e = HEAD**-0.5 * LOG2E

    def strips(todo, new):
        scores = [[_dot(q_s[pl.ds(at, W), :], kv_s[0, pl.ds(k, n), :], 1, 1) for k, n in keys] for at, keys, _ in todo]
        weights, keeps = [], []
        for (at, keys, edge), parts in zip(todo, scores):
            s = [t[:, i : i + 128] for t in parts for i in range(0, t.shape[1], 128)]
            if edge:
                gap = lax.broadcasted_iota(jnp.int32, (W, 128), 0) - lax.broadcasted_iota(jnp.int32, (W, 128), 1)
                s[-2] = jnp.where(gap >= 0, s[-2], HIDDEN)
                s[-1] = jnp.where(gap >= 128, s[-1], HIDDEN)
            most = s[0]
            for t in s[1:]:
                most = jnp.maximum(most, t)
            top = jnp.broadcast_to(most.max(axis=1, keepdims=True), (W, 128))
            if not new:
                old = top_s[pl.ds(at, W), :]
                top = jnp.maximum(old, top)
                keeps.append(jnp.exp2((old - top) * e))
            top_s[pl.ds(at, W), :] = top
            w = [jnp.exp2((t - top) * e) for t in s]
            total = w[0]
            for t in w[1:]:
                total = total + t
            sum_s[pl.ds(at, W), :] = total if new else sum_s[pl.ds(at, W), :] * keeps[-1] + total
            weights.append(jnp.concatenate([t.astype(BF16) for t in w], 1))
        for i, (at, keys, _) in enumerate(todo):
            more, col = None, 0
            for k, n in keys:
                r = _dot(weights[i][:, col : col + n], kv_s[1, pl.ds(k, n), :], 1, 0)
                more, col = r if more is None else more + r, col + n
            acc_s[pl.ds(at, W), :] = more if new else acc_s[pl.ds(at, W), :] * jnp.concatenate([keeps[i], keeps[i]], 1) + more

    def wo_rows(dev, half):
        return pl.ds(pl.multiple_of(dev * 256 + half * 128, 128), 128)

    def wo_own(half, way):
        return remote(wo_h.at[rows(half, 128), :], wo_s.at[wo_rows(me, half), :], s_wo.at[2 * way + half], r_wo.at[2 * way + half],
                      (xn, yn, mate)[way])

    def wo_local(half):
        return pltpu.make_async_copy(wo_h.at[rows(half, 128), :], wo_s.at[wo_rows(me, half), :], loc.at[9 + half])

    def wo_fwd(k, half):
        ref = wo_s.at[wo_rows((xn, yn, 2 * cd + c)[k], half), :]
        return remote(ref, ref, f_wo.at[2 * k + half], g_wo.at[2 * k + half], mate)

    def wo_relay(way):
        ref = wo_s.at[wo_rows((xn, yn)[way], way), :]
        return remote(ref, ref, s_wo.at[6 + way], r_wo.at[6 + way], (yn, xn)[way])

    wo_any = wo_s.at[rows(0, 128), :]
    piece_any = piece(0)

    def take(k):
        way, i = (k % 2, k // 2) if k < 4 else (2, k - 4)
        chip = chips[way]
        ref = piece(2 * chip + i)
        slot = 2 * way + i

        @pl.when(chip < p)
        def _():
            arrived(piece_any, r_kv.at[slot])
            kv_fwd(2 * chip + i).start()

        if way == 0:

            @pl.when((p == 3) | (p == 2) & (i == 0))
            def _():
                remote(ref, ref, s_kv.at[4 + i], r_kv.at[4 + i], yn).start()

        if way == 1 and i == 1:

            @pl.when(p == 1)
            def _():
                remote(ref, ref, s_kv.at[4 + i], r_kv.at[4 + i], xn).start()

    def o_copy(j):
        h = 4 * c + j
        dst = wq_s.at[lax.div(h, 2), pl.ds(pl.multiple_of(lax.rem(h, 2) * own, own), own), :]
        return remote(q_s.at[pl.ds(pl.multiple_of(j * 2048 + (1 - c) * own, own), own), :], dst, s_o.at[j], r_o.at[j], mate)

    def wq_pass(j):
        for i in (0, 1, 2, 3):
            arrived(wq_s.at[j, rows(0, 256), :], r_q.at[j, i])
        start(wq_relay(j))

    def work(m, _):
        def at_step(n):
            return pl.when(m == n)

        @pl.when(m < 3)
        def _():
            @at_step(0)
            def _():
                wq_pass(0)
                start(wq_own(1, 1) + wq_own(2, 0))

            @at_step(1)
            def _():
                wq_pass(1)
                start(wq_own(2, 1))
                kv_start(0)
                for i in range(2):
                    arrived(piece(0), g_kv.at[2 * p + i])

            @at_step(2)
            def _():
                wq_pass(2)
                kv_start(1)
                for way, at_0 in enumerate((px == 0, py == 0)):

                    @pl.when(at_0)
                    def _():
                        kv_own(1, way).start()

                start(wq_own(3, 0) + wq_own(3, 1))

        heads = (m < 4) | (m == 10) | (m == 11)
        late = m >= 10

        @pl.when(heads)
        def _():
            j = jnp.where(late, m - 7, m)

            @pl.when((m != 0) & (m != 10))
            def _():
                base, first = (j - 1) * 2048, pl.multiple_of(p * 2048, 2048)
                strips([(pl.multiple_of(base + i * W, W), [(first, (i + 1) * W)], True) for i in range(7, -1, -1)], True)

            @pl.when((m != 3) & (m != 11))
            def _():
                arrived(wq_s.at[j, rows(0, 256), :], loc.at[5 + j])
                for i in (6, 4, 5):
                    arrived(wq_s.at[j, rows(0, 256), :], r_q.at[j, i])

                def project(n, _):
                    at = pl.multiple_of(n * 512, 512)
                    r = _dot(a_s[pl.ds(at, 512), :], wq_s[j], 1, 0)
                    q_s[pl.ds(pl.multiple_of(j * 2048 + at, 512), 512), :] = turn(r, at)

                lax.fori_loop(0, 4, project, None)

        @pl.when((m >= 4) & (m < 10))
        def _():
            @at_step(4)
            def _():
                take(0)
                take(1)

            @at_step(6)
            def _():
                take(2)
                take(3)

            @at_step(8)
            def _():
                wq_pass(3)
                start([wo_own(0, 0), wo_own(1, 1), wo_own(1, 0), wo_own(0, 1)])
                for half in range(2):
                    wo_local(half).start()
                    wo_own(half, 2).start()

        @pl.when(m >= 12)
        def _():
            @at_step(12)
            def _():
                take(4)
                take(5)
                for way in range(2):
                    arrived(wo_any, r_wo.at[2 * way + way])
                    wo_relay(way).start()
                    wo_fwd(way, way).start()
                for n in range(4):
                    for k in (5, 6):
                        arrived(wq_s.at[0, rows(0, 256), :], s_q.at[n, k])
                pl.semaphore_signal(free, inc=1, device_id={"sp": mate}, device_id_type=pl.DeviceIdType.MESH)

            @at_step(14)
            def _():
                pl.semaphore_wait(free, 1)
                for way in range(2):
                    arrived(wo_any, r_wo.at[2 * way + 1 - way])
                    wo_fwd(way, 1 - way).start()

            @at_step(16)
            def _():
                for half in range(2):
                    arrived(wo_any, r_wo.at[6 + half])
                    wo_fwd(2, half).start()

        last = m >= 14
        n = m - 4
        t = jnp.where(last, 2, jnp.where(late, m - 12, lax.div(n, 3)))
        j = jnp.where(last, m - 14, jnp.where(late, 3, lax.rem(n, 3)))
        lone = jnp.where(p == 1, cy, jnp.where(last, cd, cx))
        both = (p == 3) & (t < 2)
        n_a, n_b = jnp.where(both, 2 * cx + t, 2 * lone), jnp.where(both, 2 * cy + t, 2 * lone + 1)
        active = jnp.logical_not(heads) & ((p == 3) | (p == 2) & (t > 0) | (p == 1) & (t == 1))

        @pl.when(active & ((m == 4) | (m == 7) | (m == 14)))
        def _():
            arrived(piece_any, g_kv.at[n_a])
            arrived(piece_any, g_kv.at[n_b])

        def seen(first, i):
            at = pl.ds(pl.multiple_of(first + i * W, W), W)
            return at, (acc_s[at, :] * (1 / sum_s[at, :].sum(axis=1, keepdims=True))).astype(BF16)

        @pl.when(active | last)
        def _():
            keys = [(pl.multiple_of(n_a * B, B), B), (pl.multiple_of(n_b * B, B), B)]

            def group(g, _):
                first = pl.multiple_of(j * 2048 + jnp.where(g == 0, 1 - c, c) * own, own)

                @pl.when(active)
                def _():
                    strips([(pl.multiple_of(first + i * W, W), keys, False) for i in range(4)], False)

                @pl.when(last & (g == 0))
                def _():
                    for i in range(4):
                        at, r = seen(first, i)
                        q_s[at, :] = r
                    o_copy(j).start()

                @pl.when(last & (g == 1))
                def _():
                    h = 4 * c + j
                    for i in range(4):
                        _, r = seen(first, i)
                        wq_s[lax.div(h, 2), pl.ds(pl.multiple_of(lax.rem(h, 2) * own + i * W, W), W), :] = r

            lax.fori_loop(0, 2, group, None)

    lax.fori_loop(0, 18, work, None)
    for half in range(2):
        arrived(wo_any, loc.at[9 + half])
        arrived(wo_any, r_wo.at[4 + half])
        for k in range(3):
            arrived(wo_any, g_wo.at[2 * k + half])
    for j in range(4):
        arrived(q_s.at[:own, :], r_o.at[j])

    def y_copy(i):
        return pltpu.make_async_copy(x_s.at[rows(i, 256), :], y_h.at[rows(i, 256), :], loc.at[i])

    def out(i, _):
        at = pl.multiple_of(i * 256, 256)
        seen = jnp.concatenate([wq_s[h // 2, pl.ds(pl.multiple_of(h % 2 * own + at, 256), 256), :] for h in range(8)], 1)
        for n in range(4):
            cols = slice(512 * n, 512 * (n + 1))
            r = _dot(seen, wo_s[:, cols], 1, 0)
            x_s[pl.ds(at, 256), cols] = (x_s[pl.ds(at, 256), cols].astype(F32) + r).astype(BF16)
        y_copy(i).start()

    lax.fori_loop(0, 4, out, None)

    def left(ref, sem):
        pltpu.make_async_copy(ref, ref, sem).wait()

    for i in range(4):
        left(q_s.at[:own, :], s_o.at[i])
        for k in range(5):
            left(wq_s.at[0, rows(0, 256), :], s_q.at[i, k])
    for i in range(5):
        left(w_mine, s_w.at[i])
    for lot, sent in enumerate((px == 0, py == 0, p > 0)):

        @pl.when(sent)
        def _():
            def one(i, _):
                left(piece_any, s_kv.at[2 * lot + i])

            lo, hi = (0, 2) if lot < 2 else (jnp.where(p == 1, 1, 0), jnp.where(p == 2, 1, 2))
            lax.fori_loop(lo, hi, one, None)

    def forwarded(i, _):
        left(piece_any, f_kv.at[i])

    lax.fori_loop(0, 2 * p + 2, forwarded, None)
    for i in range(8):
        left(wo_any, s_wo.at[i])
    for i in range(6):
        left(wo_any, f_wo.at[i])
    for i in range(4):
        y_copy(i).wait()


def solution(mesh):
    def step(x, gain, wq, wk, wv, wo):
        half = HEAD // 2
        freq = np.asarray([THETA ** (-i / half) for i in range(half)], np.float32)[None]
        hbm, vmem = pl.BlockSpec(memory_space=pl.ANY), pl.BlockSpec(memory_space=pltpu.VMEM)
        dma = pltpu.SemaphoreType.DMA
        return pl.pallas_call(
            _kernel,
            out_shape=jax.ShapeDtypeStruct(x.shape, x.dtype),
            in_specs=[hbm, vmem, vmem, hbm, hbm, hbm, hbm],
            out_specs=hbm,
            scratch_shapes=[
                pltpu.VMEM((2048, 2048), BF16),
                pltpu.VMEM((1024, 2048), BF16),
                pltpu.VMEM((4, 2048, 256), BF16),
                pltpu.VMEM((2, 8192, 256), BF16),
                pltpu.VMEM((4 * 2048, 256), BF16),
                pltpu.VMEM((2048, 2048), BF16),
                pltpu.VMEM((2048, 128), F32),
                pltpu.VMEM((2048, 128), F32),
                pltpu.VMEM((4 * 2048, 256), F32),
                pltpu.VMEM((4 * 2048, 128), F32),
                pltpu.VMEM((4 * 2048, 128), F32),
                dma((11,)),
                dma((4,)), dma((4,)),
                dma((7,)), dma((7,)),
                dma((4, 7)), dma((4, 7)),
                dma((6,)), dma((6,)), dma((8,)), dma((8,)),
                dma((8,)), dma((8,)), dma((6,)), dma((6,)),
                dma((4,)), dma((4,)),
                pltpu.SemaphoreType.REGULAR,
            ],
            compiler_params=pltpu.CompilerParams(collective_id=0, has_side_effects=True, vmem_limit_bytes=67043328),
            name="half_layer",
        )(x, gain, freq, wq, wk, wv, wo)

    tokens, whole = P(("dp", "sp"), None), P("sp", None)
    return jax.shard_map(
        step,
        mesh=mesh,
        in_specs=(tokens, P(None), whole, whole, whole, whole),
        out_specs=tokens,
        check_vma=False,
    )
```

```python
import jax
import jax.numpy as jnp
import numpy as np
from jax import lax
from jax.experimental import pallas as pl
from jax.experimental.pallas import tpu as pltpu
from jax.sharding import PartitionSpec as P

NEG = -1e30
HIDDEN = 2 * NEG
LOG2E = 1.4426950408889634
HEAD = 256
THETA = 10000
W = 256
B = 1024
F32, BF16 = jnp.float32, jnp.bfloat16


def _dot(a, b, ca, cb):
    return lax.dot_general(a, b, (((ca,), (cb,)), ((), ())), preferred_element_type=F32)


def _kernel(x_h, gain_ref, freq_ref, wq_h, wk_h, wv_h, wo_h, y_h,
            a_s, x_s, wq_s, kv_s, q_s, wo_s, cos_s, sin_s, acc_s, top_s, sum_s,
            loc, s_a, r_a, s_w, r_w, s_q, r_q, s_kv, r_kv, f_kv, g_kv, s_wo, r_wo, f_wo, g_wo, s_o, r_o, free):
    me = lax.axis_index("sp")
    c = lax.rem(me, 2)
    p = lax.div(me, 2)
    px, py = lax.div(p, 2), lax.rem(p, 2)
    cx, cy, cd = 2 * (1 - px) + py, 2 * px + 1 - py, 2 * (1 - px) + 1 - py
    chips = (cx, cy, cd)
    mate = 2 * p + 1 - c
    xn, yn = 2 * cx + c, 2 * cy + c
    own = 1024
    w_s = wo_s.at[:, :256]

    def remote(src, dst, ss, rs, dev):
        return pltpu.make_async_remote_copy(src_ref=src, dst_ref=dst, send_sem=ss, recv_sem=rs, device_id={"sp": dev},
                                            device_id_type=pl.DeviceIdType.MESH)

    def arrived(ref, sem):
        pltpu.make_async_copy(ref, ref, sem).wait()

    def rows(i, n):
        return pl.ds(pl.multiple_of(i * n, n), n)

    loads = [pltpu.make_async_copy(x_h.at[rows(i, 256), :], x_s.at[rows(i, 256), :], loc.at[i]) for i in range(4)]
    for t in loads:
        t.start()

    barrier = pltpu.get_barrier_semaphore()
    for dev in (mate, 2 * cx, 2 * cx + 1, 2 * cy, 2 * cy + 1):
        pl.semaphore_signal(barrier, inc=1, device_id={"sp": dev}, device_id_type=pl.DeviceIdType.MESH)
    pl.semaphore_wait(barrier, 5)

    w_mine = w_s.at[rows(me, 256), :]
    for t, w_h in enumerate((wk_h, wv_h)):
        remote(w_h, w_mine, s_w.at[t], r_w.at[c], 2 * cx + t).start()
        remote(w_h, w_mine, s_w.at[2 + t], r_w.at[2 + c], 2 * cy + t).start()

        @pl.when(c == t)
        def _():
            pltpu.make_async_copy(w_h, w_mine, loc.at[4]).start()

        @pl.when(c != t)
        def _():
            remote(w_h, w_mine, s_w.at[4], r_w.at[6], mate).start()

    def wq_part(core, j):
        return wq_h.at[:, pl.ds(pl.multiple_of((4 * core + j) * 256, 256), 256)]

    def wq_own(j, t):
        dst = wq_s.at[j, rows(me, 256), :]
        return [remote(wq_part(t, j), dst, s_q.at[j, t], r_q.at[j, c], 2 * cx + t),
                remote(wq_part(t, j), dst, s_q.at[j, 2 + t], r_q.at[j, 2 + c], 2 * cy + t)]

    def wq_mate(j):
        return remote(wq_part(1 - c, j), wq_s.at[j, rows(me, 256), :], s_q.at[j, 4], r_q.at[j, 6], mate)

    def wq_local(j):
        return pltpu.make_async_copy(wq_part(c, j), wq_s.at[j, rows(me, 256), :], loc.at[5 + j])

    def wq_relay(j):
        fx, fy = wq_s.at[j, rows(2 * cx, 256), :], wq_s.at[j, rows(2 * cy + 1, 256), :]
        return [remote(fx, fx, s_q.at[j, 5], r_q.at[j, 4], yn), remote(fy, fy, s_q.at[j, 6], r_q.at[j, 5], xn)]

    def start(ts):
        for t in ts:
            t.start()

    def a_rows(i):
        return a_s.at[pl.ds(pl.multiple_of(c * own + i * 256, 256), 256), :]

    def a_copy(i):
        return remote(a_rows(i), a_rows(i), s_a.at[i], r_a.at[i], mate)

    start(wq_own(0, 0))
    gain = gain_ref[...].astype(F32)[None]
    for i in range(4):
        loads[i].wait()

        def norm(n, _):
            at = pl.multiple_of(i * 256 + n * 64, 64)
            wide = x_s[pl.ds(at, 64), :].astype(F32)
            scale = lax.rsqrt(jnp.mean(wide * wide, -1, keepdims=True) + 1e-6)
            a_s[pl.ds(pl.multiple_of(c * own + at, 64), 64), :] = (wide * scale * gain).astype(BF16)

        lax.fori_loop(0, 4, norm, None)
        a_copy(i).start()

    def angles(n, _):
        at = pl.multiple_of(n * 64, 64)
        place = (p * 2048 + at + lax.broadcasted_iota(jnp.int32, (64, 128), 0)).astype(F32)
        angle = place * freq_ref[...]
        cos_s[pl.ds(at, 64), :] = jnp.cos(angle)
        sin_s[pl.ds(at, 64), :] = jnp.sin(angle)

    lax.fori_loop(0, 16, angles, None)

    for i in range(4):
        arrived(w_s.at[rows(0, 256), :], r_w.at[i])
    fx, fy = w_s.at[rows(2 * cx, 256), :], w_s.at[rows(2 * cy + 1, 256), :]
    relays_w = [remote(fx, fx, s_w.at[5], r_w.at[4], yn), remote(fy, fy, s_w.at[6], r_w.at[5], xn)]
    start(relays_w)
    start(wq_own(0, 1) + wq_own(1, 0))
    for j in range(4):
        wq_mate(j).start()
        wq_local(j).start()
    lax.fori_loop(16, 32, angles, None)
    for i in range(4):
        arrived(a_rows(0), r_a.at[i])
        arrived(a_rows(0), s_a.at[i])
    arrived(w_mine, loc.at[4])
    for i in (6, 4, 5):
        arrived(w_mine, r_w.at[i])

    def turn(r, at):
        r = r.astype(BF16).astype(F32)
        lo, hi = r[:, :128], r[:, 128:]
        cos, sin = cos_s[pl.ds(at, r.shape[0]), :], sin_s[pl.ds(at, r.shape[0]), :]
        return jnp.concatenate([lo * cos - hi * sin, hi * cos + lo * sin], -1).astype(BF16)

    def piece(n):
        return kv_s.at[c, rows(n, B), :]

    def kv_fwd(n):
        return remote(piece(n), piece(n), f_kv.at[n], g_kv.at[n], mate)

    def kv_own(i, way):
        ref = piece(2 * p + i)
        return remote(ref, ref, s_kv.at[2 * way + i], r_kv.at[2 * way + i], (xn, yn)[way])

    def kv_start(h):
        ref = kv_s.at[c, pl.ds(pl.multiple_of(2048 * p + 256 * h, 256), 256 + 512 * h), :]
        for way, at_0 in enumerate((px == 0, py == 0)):

            @pl.when(at_0)
            def _():
                remote(ref, ref, s_kv.at[2 * way], r_kv.at[2 * way], (xn, yn)[way]).start()

    def kvproj(i, _):
        at = pl.multiple_of(i * 512, 512)
        to = pl.ds(pl.multiple_of(p * 2048 + at, 512), 512)
        r = _dot(a_s[pl.ds(at, 512), :], w_s[...], 1, 0)

        @pl.when(c == 0)
        def _():
            kv_s[0, to, :] = turn(r, at)

        @pl.when(c == 1)
        def _():
            kv_s[1, to, :] = r.astype(BF16)

        @pl.when(lax.rem(i, 2) == 1)
        def _():
            kv_fwd(2 * p + lax.div(i, 2)).start()

    lax.fori_loop(0, 4, kvproj, None)
    for i in (5, 6):
        arrived(w_mine, s_w.at[i])

    e = HEAD**-0.5 * LOG2E

    def strips(todo, new):
        scores = [[_dot(q_s[pl.ds(at, W), :], kv_s[0, pl.ds(k, n), :], 1, 1) for k, n in keys] for at, keys, _ in todo]
        weights, keeps = [], []
        for (at, keys, edge), parts in zip(todo, scores):
            s = [t[:, i : i + 128] for t in parts for i in range(0, t.shape[1], 128)]
            if edge:
                gap = lax.broadcasted_iota(jnp.int32, (W, 128), 0) - lax.broadcasted_iota(jnp.int32, (W, 128), 1)
                s[-2] = jnp.where(gap >= 0, s[-2], HIDDEN)
                s[-1] = jnp.where(gap >= 128, s[-1], HIDDEN)
            most = s[0]
            for t in s[1:]:
                most = jnp.maximum(most, t)
            top = jnp.broadcast_to(most.max(axis=1, keepdims=True), (W, 128))
            if not new:
                old = top_s[pl.ds(at, W), :]
                top = jnp.maximum(old, top)
                keeps.append(jnp.exp2((old - top) * e))
            top_s[pl.ds(at, W), :] = top
            w = [jnp.exp2((t - top) * e) for t in s]
            total = w[0]
            for t in w[1:]:
                total = total + t
            sum_s[pl.ds(at, W), :] = total if new else sum_s[pl.ds(at, W), :] * keeps[-1] + total
            weights.append(jnp.concatenate([t.astype(BF16) for t in w], 1))
        for i, (at, keys, _) in enumerate(todo):
            more, col = None, 0
            for k, n in keys:
                r = _dot(weights[i][:, col : col + n], kv_s[1, pl.ds(k, n), :], 1, 0)
                more, col = r if more is None else more + r, col + n
            acc_s[pl.ds(at, W), :] = more if new else acc_s[pl.ds(at, W), :] * jnp.concatenate([keeps[i], keeps[i]], 1) + more

    def wo_rows(dev, half):
        return pl.ds(pl.multiple_of(dev * 256 + half * 128, 128), 128)

    def wo_own(half, way):
        return remote(wo_h.at[rows(half, 128), :], wo_s.at[wo_rows(me, half), :], s_wo.at[2 * way + half], r_wo.at[2 * way + half],
                      (xn, yn, mate)[way])

    def wo_local(half):
        return pltpu.make_async_copy(wo_h.at[rows(half, 128), :], wo_s.at[wo_rows(me, half), :], loc.at[9 + half])

    def wo_fwd(k, half):
        ref = wo_s.at[wo_rows((xn, yn, 2 * cd + c)[k], half), :]
        return remote(ref, ref, f_wo.at[2 * k + half], g_wo.at[2 * k + half], mate)

    def wo_relay(way):
        ref = wo_s.at[wo_rows((xn, yn)[way], way), :]
        return remote(ref, ref, s_wo.at[6 + way], r_wo.at[6 + way], (yn, xn)[way])

    wo_any = wo_s.at[rows(0, 128), :]
    piece_any = piece(0)

    def take(k):
        way, i = (k % 2, k // 2) if k < 4 else (2, k - 4)
        chip = chips[way]
        ref = piece(2 * chip + i)
        slot = 2 * way + i

        @pl.when(chip < p)
        def _():
            arrived(piece_any, r_kv.at[slot])
            kv_fwd(2 * chip + i).start()

        if way == 0:

            @pl.when((p == 3) | (p == 2) & (i == 0))
            def _():
                remote(ref, ref, s_kv.at[4 + i], r_kv.at[4 + i], yn).start()

        if way == 1 and i == 1:

            @pl.when(p == 1)
            def _():
                remote(ref, ref, s_kv.at[4 + i], r_kv.at[4 + i], xn).start()

    def o_copy(j):
        h = 4 * c + j
        dst = wq_s.at[lax.div(h, 2), pl.ds(pl.multiple_of(lax.rem(h, 2) * own, own), own), :]
        return remote(q_s.at[pl.ds(pl.multiple_of(j * 2048 + (1 - c) * own, own), own), :], dst, s_o.at[j], r_o.at[j], mate)

    def wq_pass(j):
        for i in (0, 1, 2, 3):
            arrived(wq_s.at[j, rows(0, 256), :], r_q.at[j, i])
        start(wq_relay(j))

    def work(m, _):
        def at_step(n):
            return pl.when(m == n)

        @pl.when(m < 3)
        def _():
            @at_step(0)
            def _():
                wq_pass(0)
                start(wq_own(1, 1) + wq_own(2, 0))

            @at_step(1)
            def _():
                wq_pass(1)
                start(wq_own(2, 1))
                kv_start(0)
                for i in range(2):
                    arrived(piece(0), g_kv.at[2 * p + i])

            @at_step(2)
            def _():
                wq_pass(2)
                kv_start(1)
                for way, at_0 in enumerate((px == 0, py == 0)):

                    @pl.when(at_0)
                    def _():
                        kv_own(1, way).start()

                start(wq_own(3, 0) + wq_own(3, 1))

        heads = (m < 4) | (m == 10) | (m == 11)
        late = m >= 10

        @pl.when(heads)
        def _():
            j = jnp.where(late, m - 7, m)

            @pl.when((m != 0) & (m != 10))
            def _():
                base, first = (j - 1) * 2048, pl.multiple_of(p * 2048, 2048)
                strips([(pl.multiple_of(base + i * W, W), [(first, (i + 1) * W)], True) for i in range(7, -1, -1)], True)

            @pl.when((m != 3) & (m != 11))
            def _():
                arrived(wq_s.at[j, rows(0, 256), :], loc.at[5 + j])
                for i in (6, 4, 5):
                    arrived(wq_s.at[j, rows(0, 256), :], r_q.at[j, i])

                def project(n, _):
                    at = pl.multiple_of(n * 1024, 1024)
                    r = _dot(a_s[pl.ds(at, 1024), :], wq_s[j], 1, 0)
                    q_s[pl.ds(pl.multiple_of(j * 2048 + at, 1024), 1024), :] = turn(r, at)

                lax.fori_loop(0, 2, project, None)

        @pl.when((m >= 4) & (m < 10))
        def _():
            @at_step(4)
            def _():
                take(0)
                take(1)

            @at_step(6)
            def _():
                take(2)
                take(3)

            @at_step(8)
            def _():
                wq_pass(3)
                start([wo_own(0, 0), wo_own(1, 1), wo_own(1, 0), wo_own(0, 1)])
                for half in range(2):
                    wo_local(half).start()
                    wo_own(half, 2).start()

        @pl.when(m >= 12)
        def _():
            @at_step(12)
            def _():
                take(4)
                take(5)
                for way in range(2):
                    arrived(wo_any, r_wo.at[2 * way + way])
                    wo_relay(way).start()
                    wo_fwd(way, way).start()
                for n in range(4):
                    for k in (5, 6):
                        arrived(wq_s.at[0, rows(0, 256), :], s_q.at[n, k])
                pl.semaphore_signal(free, inc=1, device_id={"sp": mate}, device_id_type=pl.DeviceIdType.MESH)

            @at_step(14)
            def _():
                pl.semaphore_wait(free, 1)
                for way in range(2):
                    arrived(wo_any, r_wo.at[2 * way + 1 - way])
                    wo_fwd(way, 1 - way).start()

            @at_step(16)
            def _():
                for half in range(2):
                    arrived(wo_any, r_wo.at[6 + half])
                    wo_fwd(2, half).start()

        last = m >= 14
        n = m - 4
        t = jnp.where(last, 2, jnp.where(late, m - 12, lax.div(n, 3)))
        j = jnp.where(last, m - 14, jnp.where(late, 3, lax.rem(n, 3)))
        lone = jnp.where(p == 1, cy, jnp.where(last, cd, cx))
        both = (p == 3) & (t < 2)
        n_a, n_b = jnp.where(both, 2 * cx + t, 2 * lone), jnp.where(both, 2 * cy + t, 2 * lone + 1)
        active = jnp.logical_not(heads) & ((p == 3) | (p == 2) & (t > 0) | (p == 1) & (t == 1))

        @pl.when(active & ((m == 4) | (m == 7) | (m == 14)))
        def _():
            arrived(piece_any, g_kv.at[n_a])
            arrived(piece_any, g_kv.at[n_b])

        def seen(first, i):
            at = pl.ds(pl.multiple_of(first + i * W, W), W)
            return at, (acc_s[at, :] * (1 / sum_s[at, :].sum(axis=1, keepdims=True))).astype(BF16)

        @pl.when(active | last)
        def _():
            keys = [(pl.multiple_of(n_a * B, B), B), (pl.multiple_of(n_b * B, B), B)]

            def group(g, _):
                first = pl.multiple_of(j * 2048 + jnp.where(g == 0, 1 - c, c) * own, own)

                @pl.when(active)
                def _():
                    strips([(pl.multiple_of(first + i * W, W), keys, False) for i in range(4)], False)

                @pl.when(last & (g == 0))
                def _():
                    for i in range(4):
                        at, r = seen(first, i)
                        q_s[at, :] = r
                    o_copy(j).start()

                @pl.when(last & (g == 1))
                def _():
                    h = 4 * c + j
                    for i in range(4):
                        _, r = seen(first, i)
                        wq_s[lax.div(h, 2), pl.ds(pl.multiple_of(lax.rem(h, 2) * own + i * W, W), W), :] = r

            lax.fori_loop(0, 2, group, None)

    lax.fori_loop(0, 18, work, None)
    for half in range(2):
        arrived(wo_any, loc.at[9 + half])
        arrived(wo_any, r_wo.at[4 + half])
        for k in range(3):
            arrived(wo_any, g_wo.at[2 * k + half])
    for j in range(4):
        arrived(q_s.at[:own, :], r_o.at[j])

    def y_copy(i):
        return pltpu.make_async_copy(x_s.at[rows(i, 256), :], y_h.at[rows(i, 256), :], loc.at[i])

    def out(i, _):
        at = pl.multiple_of(i * 256, 256)
        seen = jnp.concatenate([wq_s[h // 2, pl.ds(pl.multiple_of(h % 2 * own + at, 256), 256), :] for h in range(8)], 1)
        for n in range(4):
            cols = slice(512 * n, 512 * (n + 1))
            r = _dot(seen, wo_s[:, cols], 1, 0)
            x_s[pl.ds(at, 256), cols] = (x_s[pl.ds(at, 256), cols].astype(F32) + r).astype(BF16)
        y_copy(i).start()

    lax.fori_loop(0, 4, out, None)

    def left(ref, sem):
        pltpu.make_async_copy(ref, ref, sem).wait()

    for i in range(4):
        left(q_s.at[:own, :], s_o.at[i])
        for k in range(5):
            left(wq_s.at[0, rows(0, 256), :], s_q.at[i, k])
    for i in range(5):
        left(w_mine, s_w.at[i])
    for lot, sent in enumerate((px == 0, py == 0, p > 0)):

        @pl.when(sent)
        def _():
            def one(i, _):
                left(piece_any, s_kv.at[2 * lot + i])

            lo, hi = (0, 2) if lot < 2 else (jnp.where(p == 1, 1, 0), jnp.where(p == 2, 1, 2))
            lax.fori_loop(lo, hi, one, None)

    def forwarded(i, _):
        left(piece_any, f_kv.at[i])

    lax.fori_loop(0, 2 * p + 2, forwarded, None)
    for i in range(8):
        left(wo_any, s_wo.at[i])
    for i in range(6):
        left(wo_any, f_wo.at[i])
    for i in range(4):
        y_copy(i).wait()


def solution(mesh):
    def step(x, gain, wq, wk, wv, wo):
        half = HEAD // 2
        freq = np.asarray([THETA ** (-i / half) for i in range(half)], np.float32)[None]
        hbm, vmem = pl.BlockSpec(memory_space=pl.ANY), pl.BlockSpec(memory_space=pltpu.VMEM)
        dma = pltpu.SemaphoreType.DMA
        return pl.pallas_call(
            _kernel,
            out_shape=jax.ShapeDtypeStruct(x.shape, x.dtype),
            in_specs=[hbm, vmem, vmem, hbm, hbm, hbm, hbm],
            out_specs=hbm,
            scratch_shapes=[
                pltpu.VMEM((2048, 2048), BF16),
                pltpu.VMEM((1024, 2048), BF16),
                pltpu.VMEM((4, 2048, 256), BF16),
                pltpu.VMEM((2, 8192, 256), BF16),
                pltpu.VMEM((4 * 2048, 256), BF16),
                pltpu.VMEM((2048, 2048), BF16),
                pltpu.VMEM((2048, 128), F32),
                pltpu.VMEM((2048, 128), F32),
                pltpu.VMEM((4 * 2048, 256), F32),
                pltpu.VMEM((4 * 2048, 128), F32),
                pltpu.VMEM((4 * 2048, 128), F32),
                dma((11,)),
                dma((4,)), dma((4,)),
                dma((7,)), dma((7,)),
                dma((4, 7)), dma((4, 7)),
                dma((6,)), dma((6,)), dma((8,)), dma((8,)),
                dma((8,)), dma((8,)), dma((6,)), dma((6,)),
                dma((4,)), dma((4,)),
                pltpu.SemaphoreType.REGULAR,
            ],
            compiler_params=pltpu.CompilerParams(collective_id=0, has_side_effects=True, vmem_limit_bytes=67043328),
            name="half_layer",
        )(x, gain, freq, wq, wk, wv, wo)

    tokens, whole = P(("dp", "sp"), None), P("sp", None)
    return jax.shard_map(
        step,
        mesh=mesh,
        in_specs=(tokens, P(None), whole, whole, whole, whole),
        out_specs=tokens,
        check_vma=False,
    )
```

```python
import jax
import jax.numpy as jnp
import numpy as np
from jax import lax
from jax.experimental import pallas as pl
from jax.experimental.pallas import tpu as pltpu
from jax.sharding import PartitionSpec as P

NEG = -1e30
HIDDEN = 2 * NEG
LOG2E = 1.4426950408889634
HEAD = 256
THETA = 10000
W = 256
B = 1024
F32, BF16 = jnp.float32, jnp.bfloat16


def _dot(a, b, ca, cb):
    return lax.dot_general(a, b, (((ca,), (cb,)), ((), ())), preferred_element_type=F32)


def _kernel(x_h, gain_ref, freq_ref, wq_h, wk_h, wv_h, wo_h, y_h,
            a_s, x_s, wq_s, kv_s, q_s, wo_s, cos_s, sin_s, acc_s, top_s, sum_s,
            loc, s_a, r_a, s_w, r_w, s_q, r_q, s_kv, r_kv, f_kv, g_kv, s_wo, r_wo, f_wo, g_wo, s_o, r_o, free):
    me = lax.axis_index("sp")
    c = lax.rem(me, 2)
    p = lax.div(me, 2)
    px, py = lax.div(p, 2), lax.rem(p, 2)
    cx, cy, cd = 2 * (1 - px) + py, 2 * px + 1 - py, 2 * (1 - px) + 1 - py
    chips = (cx, cy, cd)
    mate = 2 * p + 1 - c
    xn, yn = 2 * cx + c, 2 * cy + c
    own = 1024
    w_s = wo_s.at[:, :256]

    def remote(src, dst, ss, rs, dev):
        return pltpu.make_async_remote_copy(src_ref=src, dst_ref=dst, send_sem=ss, recv_sem=rs, device_id={"sp": dev},
                                            device_id_type=pl.DeviceIdType.MESH)

    def arrived(ref, sem):
        pltpu.make_async_copy(ref, ref, sem).wait()

    def rows(i, n):
        return pl.ds(pl.multiple_of(i * n, n), n)

    loads = [pltpu.make_async_copy(x_h.at[rows(i, 256), :], x_s.at[rows(i, 256), :], loc.at[i]) for i in range(4)]
    for t in loads:
        t.start()

    barrier = pltpu.get_barrier_semaphore()
    for dev in (mate, 2 * cx, 2 * cx + 1, 2 * cy, 2 * cy + 1):
        pl.semaphore_signal(barrier, inc=1, device_id={"sp": dev}, device_id_type=pl.DeviceIdType.MESH)
    pl.semaphore_wait(barrier, 5)

    w_mine = w_s.at[rows(me, 256), :]
    for t, w_h in enumerate((wk_h, wv_h)):
        remote(w_h, w_mine, s_w.at[t], r_w.at[c], 2 * cx + t).start()
        remote(w_h, w_mine, s_w.at[2 + t], r_w.at[2 + c], 2 * cy + t).start()

        @pl.when(c == t)
        def _():
            pltpu.make_async_copy(w_h, w_mine, loc.at[4]).start()

        @pl.when(c != t)
        def _():
            remote(w_h, w_mine, s_w.at[4], r_w.at[6], mate).start()

    def wq_part(core, j):
        return wq_h.at[:, pl.ds(pl.multiple_of((4 * core + j) * 256, 256), 256)]

    def wq_own(j, t):
        dst = wq_s.at[j, rows(me, 256), :]
        return [remote(wq_part(t, j), dst, s_q.at[j, t], r_q.at[j, c], 2 * cx + t),
                remote(wq_part(t, j), dst, s_q.at[j, 2 + t], r_q.at[j, 2 + c], 2 * cy + t)]

    def wq_mate(j):
        return remote(wq_part(1 - c, j), wq_s.at[j, rows(me, 256), :], s_q.at[j, 4], r_q.at[j, 6], mate)

    def wq_local(j):
        return pltpu.make_async_copy(wq_part(c, j), wq_s.at[j, rows(me, 256), :], loc.at[5 + j])

    def wq_relay(j):
        fx, fy = wq_s.at[j, rows(2 * cx, 256), :], wq_s.at[j, rows(2 * cy + 1, 256), :]
        return [remote(fx, fx, s_q.at[j, 5], r_q.at[j, 4], yn), remote(fy, fy, s_q.at[j, 6], r_q.at[j, 5], xn)]

    def start(ts):
        for t in ts:
            t.start()

    def a_rows(i):
        return a_s.at[pl.ds(pl.multiple_of(c * own + i * 256, 256), 256), :]

    def a_copy(i):
        return remote(a_rows(i), a_rows(i), s_a.at[i], r_a.at[i], mate)

    start(wq_own(0, 0))
    gain = gain_ref[...].astype(F32)[None]
    for i in range(4):
        loads[i].wait()

        def norm(n, _):
            at = pl.multiple_of(i * 256 + n * 64, 64)
            wide = x_s[pl.ds(at, 64), :].astype(F32)
            scale = lax.rsqrt(jnp.mean(wide * wide, -1, keepdims=True) + 1e-6)
            a_s[pl.ds(pl.multiple_of(c * own + at, 64), 64), :] = (wide * scale * gain).astype(BF16)

        lax.fori_loop(0, 4, norm, None)
        a_copy(i).start()

    def angles(n, _):
        at = pl.multiple_of(n * 64, 64)
        place = (p * 2048 + at + lax.broadcasted_iota(jnp.int32, (64, 128), 0)).astype(F32)
        angle = place * freq_ref[...]
        cos_s[pl.ds(at, 64), :] = jnp.cos(angle)
        sin_s[pl.ds(at, 64), :] = jnp.sin(angle)

    lax.fori_loop(0, 16, angles, None)

    for i in range(4):
        arrived(w_s.at[rows(0, 256), :], r_w.at[i])
    fx, fy = w_s.at[rows(2 * cx, 256), :], w_s.at[rows(2 * cy + 1, 256), :]
    relays_w = [remote(fx, fx, s_w.at[5], r_w.at[4], yn), remote(fy, fy, s_w.at[6], r_w.at[5], xn)]
    start(relays_w)
    start(wq_own(0, 1) + wq_own(1, 0))
    for j in range(4):
        wq_mate(j).start()
        wq_local(j).start()
    lax.fori_loop(16, 32, angles, None)
    for i in range(4):
        arrived(a_rows(0), r_a.at[i])
        arrived(a_rows(0), s_a.at[i])
    arrived(w_mine, loc.at[4])
    for i in (6, 4, 5):
        arrived(w_mine, r_w.at[i])

    def turn(r, at):
        r = r.astype(BF16).astype(F32)
        lo, hi = r[:, :128], r[:, 128:]
        cos, sin = cos_s[pl.ds(at, r.shape[0]), :], sin_s[pl.ds(at, r.shape[0]), :]
        return jnp.concatenate([lo * cos - hi * sin, hi * cos + lo * sin], -1).astype(BF16)

    def piece(n):
        return kv_s.at[c, rows(n, B), :]

    def kv_fwd(n):
        return remote(piece(n), piece(n), f_kv.at[n], g_kv.at[n], mate)

    def kv_own(i, way):
        ref = piece(2 * p + i)
        return remote(ref, ref, s_kv.at[2 * way + i], r_kv.at[2 * way + i], (xn, yn)[way])

    def kv_start(h):
        ref = kv_s.at[c, pl.ds(pl.multiple_of(2048 * p + 256 * h, 256), 256 + 512 * h), :]
        for way, at_0 in enumerate((px == 0, py == 0)):

            @pl.when(at_0)
            def _():
                remote(ref, ref, s_kv.at[2 * way], r_kv.at[2 * way], (xn, yn)[way]).start()

    def kvproj(i, _):
        at = pl.multiple_of(i * B, B)
        to = pl.ds(pl.multiple_of(p * 2048 + at, B), B)
        r = _dot(a_s[pl.ds(at, B), :], w_s[...], 1, 0)

        @pl.when(c == 0)
        def _():
            kv_s[0, to, :] = turn(r, at)

        @pl.when(c == 1)
        def _():
            kv_s[1, to, :] = r.astype(BF16)

        kv_fwd(2 * p + i).start()

    lax.fori_loop(0, 2, kvproj, None)
    for i in (5, 6):
        arrived(w_mine, s_w.at[i])

    e = HEAD**-0.5 * LOG2E

    def strips(todo, new):
        scores = [[_dot(q_s[pl.ds(at, W), :], kv_s[0, pl.ds(k, n), :], 1, 1) for k, n in keys] for at, keys, _ in todo]
        weights, keeps = [], []
        for (at, keys, edge), parts in zip(todo, scores):
            s = [t[:, i : i + 128] for t in parts for i in range(0, t.shape[1], 128)]
            if edge:
                gap = lax.broadcasted_iota(jnp.int32, (W, 128), 0) - lax.broadcasted_iota(jnp.int32, (W, 128), 1)
                s[-2] = jnp.where(gap >= 0, s[-2], HIDDEN)
                s[-1] = jnp.where(gap >= 128, s[-1], HIDDEN)
            most = s[0]
            for t in s[1:]:
                most = jnp.maximum(most, t)
            top = jnp.broadcast_to(most.max(axis=1, keepdims=True), (W, 128))
            if not new:
                old = top_s[pl.ds(at, W), :]
                top = jnp.maximum(old, top)
                keeps.append(jnp.exp2((old - top) * e))
            top_s[pl.ds(at, W), :] = top
            w = [jnp.exp2((t - top) * e) for t in s]
            total = w[0]
            for t in w[1:]:
                total = total + t
            sum_s[pl.ds(at, W), :] = total if new else sum_s[pl.ds(at, W), :] * keeps[-1] + total
            weights.append(jnp.concatenate([t.astype(BF16) for t in w], 1))
        for i, (at, keys, _) in enumerate(todo):
            more, col = None, 0
            for k, n in keys:
                r = _dot(weights[i][:, col : col + n], kv_s[1, pl.ds(k, n), :], 1, 0)
                more, col = r if more is None else more + r, col + n
            acc_s[pl.ds(at, W), :] = more if new else acc_s[pl.ds(at, W), :] * jnp.concatenate([keeps[i], keeps[i]], 1) + more

    def wo_rows(dev, half):
        return pl.ds(pl.multiple_of(dev * 256 + half * 128, 128), 128)

    def wo_own(half, way):
        return remote(wo_h.at[rows(half, 128), :], wo_s.at[wo_rows(me, half), :], s_wo.at[2 * way + half], r_wo.at[2 * way + half],
                      (xn, yn, mate)[way])

    def wo_local(half):
        return pltpu.make_async_copy(wo_h.at[rows(half, 128), :], wo_s.at[wo_rows(me, half), :], loc.at[9 + half])

    def wo_fwd(k, half):
        ref = wo_s.at[wo_rows((xn, yn, 2 * cd + c)[k], half), :]
        return remote(ref, ref, f_wo.at[2 * k + half], g_wo.at[2 * k + half], mate)

    def wo_relay(way):
        ref = wo_s.at[wo_rows((xn, yn)[way], way), :]
        return remote(ref, ref, s_wo.at[6 + way], r_wo.at[6 + way], (yn, xn)[way])

    wo_any = wo_s.at[rows(0, 128), :]
    piece_any = piece(0)

    def take(k):
        way, i = (k % 2, k // 2) if k < 4 else (2, k - 4)
        chip = chips[way]
        ref = piece(2 * chip + i)
        slot = 2 * way + i

        @pl.when(chip < p)
        def _():
            arrived(piece_any, r_kv.at[slot])
            kv_fwd(2 * chip + i).start()

        if way == 0:

            @pl.when((p == 3) | (p == 2) & (i == 0))
            def _():
                remote(ref, ref, s_kv.at[4 + i], r_kv.at[4 + i], yn).start()

        if way == 1 and i == 1:

            @pl.when(p == 1)
            def _():
                remote(ref, ref, s_kv.at[4 + i], r_kv.at[4 + i], xn).start()

    def o_copy(j):
        h = 4 * c + j
        dst = wq_s.at[lax.div(h, 2), pl.ds(pl.multiple_of(lax.rem(h, 2) * own, own), own), :]
        return remote(q_s.at[pl.ds(pl.multiple_of(j * 2048 + (1 - c) * own, own), own), :], dst, s_o.at[j], r_o.at[j], mate)

    def wq_pass(j):
        for i in (0, 1, 2, 3):
            arrived(wq_s.at[j, rows(0, 256), :], r_q.at[j, i])
        start(wq_relay(j))

    def work(m, _):
        def at_step(n):
            return pl.when(m == n)

        @pl.when(m < 3)
        def _():
            @at_step(0)
            def _():
                wq_pass(0)
                start(wq_own(1, 1) + wq_own(2, 0))

            @at_step(1)
            def _():
                wq_pass(1)
                start(wq_own(2, 1))
                kv_start(0)
                for i in range(2):
                    arrived(piece(0), g_kv.at[2 * p + i])

            @at_step(2)
            def _():
                wq_pass(2)
                kv_start(1)
                for way, at_0 in enumerate((px == 0, py == 0)):

                    @pl.when(at_0)
                    def _():
                        kv_own(1, way).start()

                start(wq_own(3, 0) + wq_own(3, 1))

        heads = (m < 4) | (m == 10) | (m == 11)
        late = m >= 10

        @pl.when(heads)
        def _():
            j = jnp.where(late, m - 7, m)

            @pl.when((m != 0) & (m != 10))
            def _():
                base, first = (j - 1) * 2048, pl.multiple_of(p * 2048, 2048)
                strips([(pl.multiple_of(base + i * W, W), [(first, (i + 1) * W)], True) for i in range(7, -1, -1)], True)

            @pl.when((m != 3) & (m != 11))
            def _():
                arrived(wq_s.at[j, rows(0, 256), :], loc.at[5 + j])
                for i in (6, 4, 5):
                    arrived(wq_s.at[j, rows(0, 256), :], r_q.at[j, i])

                def project(n, _):
                    at = pl.multiple_of(n * 1024, 1024)
                    r = _dot(a_s[pl.ds(at, 1024), :], wq_s[j], 1, 0)
                    q_s[pl.ds(pl.multiple_of(j * 2048 + at, 1024), 1024), :] = turn(r, at)

                lax.fori_loop(0, 2, project, None)

        @pl.when((m >= 4) & (m < 10))
        def _():
            @at_step(4)
            def _():
                take(0)
                take(1)

            @at_step(6)
            def _():
                take(2)
                take(3)

            @at_step(8)
            def _():
                wq_pass(3)
                start([wo_own(0, 0), wo_own(1, 1), wo_own(1, 0), wo_own(0, 1)])
                for half in range(2):
                    wo_local(half).start()
                    wo_own(half, 2).start()

        @pl.when(m >= 12)
        def _():
            @at_step(12)
            def _():
                take(4)
                take(5)
                for way in range(2):
                    arrived(wo_any, r_wo.at[2 * way + way])
                    wo_relay(way).start()
                    wo_fwd(way, way).start()
                for n in range(4):
                    for k in (5, 6):
                        arrived(wq_s.at[0, rows(0, 256), :], s_q.at[n, k])
                pl.semaphore_signal(free, inc=1, device_id={"sp": mate}, device_id_type=pl.DeviceIdType.MESH)

            @at_step(14)
            def _():
                pl.semaphore_wait(free, 1)
                for way in range(2):
                    arrived(wo_any, r_wo.at[2 * way + 1 - way])
                    wo_fwd(way, 1 - way).start()

            @at_step(16)
            def _():
                for half in range(2):
                    arrived(wo_any, r_wo.at[6 + half])
                    wo_fwd(2, half).start()

        last = m >= 14
        n = m - 4
        t = jnp.where(last, 2, jnp.where(late, m - 12, lax.div(n, 3)))
        j = jnp.where(last, m - 14, jnp.where(late, 3, lax.rem(n, 3)))
        lone = jnp.where(p == 1, cy, jnp.where(last, cd, cx))
        both = (p == 3) & (t < 2)
        n_a, n_b = jnp.where(both, 2 * cx + t, 2 * lone), jnp.where(both, 2 * cy + t, 2 * lone + 1)
        active = jnp.logical_not(heads) & ((p == 3) | (p == 2) & (t > 0) | (p == 1) & (t == 1))

        @pl.when(active & ((m == 4) | (m == 7) | (m == 14)))
        def _():
            arrived(piece_any, g_kv.at[n_a])
            arrived(piece_any, g_kv.at[n_b])

        def seen(first, i):
            at = pl.ds(pl.multiple_of(first + i * W, W), W)
            return at, (acc_s[at, :] * (1 / sum_s[at, :].sum(axis=1, keepdims=True))).astype(BF16)

        @pl.when(active | last)
        def _():
            keys = [(pl.multiple_of(n_a * B, B), B), (pl.multiple_of(n_b * B, B), B)]

            def group(g, _):
                first = pl.multiple_of(j * 2048 + jnp.where(g == 0, 1 - c, c) * own, own)

                @pl.when(active)
                def _():
                    strips([(pl.multiple_of(first + i * W, W), keys, False) for i in range(4)], False)

                @pl.when(last & (g == 0))
                def _():
                    for i in range(4):
                        at, r = seen(first, i)
                        q_s[at, :] = r
                    o_copy(j).start()

                @pl.when(last & (g == 1))
                def _():
                    h = 4 * c + j
                    for i in range(4):
                        _, r = seen(first, i)
                        wq_s[lax.div(h, 2), pl.ds(pl.multiple_of(lax.rem(h, 2) * own + i * W, W), W), :] = r

            lax.fori_loop(0, 2, group, None)

    lax.fori_loop(0, 18, work, None)
    for half in range(2):
        arrived(wo_any, loc.at[9 + half])
        arrived(wo_any, r_wo.at[4 + half])
        for k in range(3):
            arrived(wo_any, g_wo.at[2 * k + half])
    for j in range(4):
        arrived(q_s.at[:own, :], r_o.at[j])

    def y_copy(i):
        return pltpu.make_async_copy(x_s.at[rows(i, 256), :], y_h.at[rows(i, 256), :], loc.at[i])

    def out(i, _):
        at = pl.multiple_of(i * 256, 256)
        seen = jnp.concatenate([wq_s[h // 2, pl.ds(pl.multiple_of(h % 2 * own + at, 256), 256), :] for h in range(8)], 1)
        for n in range(4):
            cols = slice(512 * n, 512 * (n + 1))
            r = _dot(seen, wo_s[:, cols], 1, 0)
            x_s[pl.ds(at, 256), cols] = (x_s[pl.ds(at, 256), cols].astype(F32) + r).astype(BF16)
        y_copy(i).start()

    lax.fori_loop(0, 4, out, None)

    def left(ref, sem):
        pltpu.make_async_copy(ref, ref, sem).wait()

    for i in range(4):
        left(q_s.at[:own, :], s_o.at[i])
        for k in range(5):
            left(wq_s.at[0, rows(0, 256), :], s_q.at[i, k])
    for i in range(5):
        left(w_mine, s_w.at[i])
    for lot, sent in enumerate((px == 0, py == 0, p > 0)):

        @pl.when(sent)
        def _():
            def one(i, _):
                left(piece_any, s_kv.at[2 * lot + i])

            lo, hi = (0, 2) if lot < 2 else (jnp.where(p == 1, 1, 0), jnp.where(p == 2, 1, 2))
            lax.fori_loop(lo, hi, one, None)

    def forwarded(i, _):
        left(piece_any, f_kv.at[i])

    lax.fori_loop(0, 2 * p + 2, forwarded, None)
    for i in range(8):
        left(wo_any, s_wo.at[i])
    for i in range(6):
        left(wo_any, f_wo.at[i])
    for i in range(4):
        y_copy(i).wait()


def solution(mesh):
    def step(x, gain, wq, wk, wv, wo):
        half = HEAD // 2
        freq = np.asarray([THETA ** (-i / half) for i in range(half)], np.float32)[None]
        hbm, vmem = pl.BlockSpec(memory_space=pl.ANY), pl.BlockSpec(memory_space=pltpu.VMEM)
        dma = pltpu.SemaphoreType.DMA
        return pl.pallas_call(
            _kernel,
            out_shape=jax.ShapeDtypeStruct(x.shape, x.dtype),
            in_specs=[hbm, vmem, vmem, hbm, hbm, hbm, hbm],
            out_specs=hbm,
            scratch_shapes=[
                pltpu.VMEM((2048, 2048), BF16),
                pltpu.VMEM((1024, 2048), BF16),
                pltpu.VMEM((4, 2048, 256), BF16),
                pltpu.VMEM((2, 8192, 256), BF16),
                pltpu.VMEM((4 * 2048, 256), BF16),
                pltpu.VMEM((2048, 2048), BF16),
                pltpu.VMEM((2048, 128), F32),
                pltpu.VMEM((2048, 128), F32),
                pltpu.VMEM((4 * 2048, 256), F32),
                pltpu.VMEM((4 * 2048, 128), F32),
                pltpu.VMEM((4 * 2048, 128), F32),
                dma((11,)),
                dma((4,)), dma((4,)),
                dma((7,)), dma((7,)),
                dma((4, 7)), dma((4, 7)),
                dma((6,)), dma((6,)), dma((8,)), dma((8,)),
                dma((8,)), dma((8,)), dma((6,)), dma((6,)),
                dma((4,)), dma((4,)),
                pltpu.SemaphoreType.REGULAR,
            ],
            compiler_params=pltpu.CompilerParams(collective_id=0, has_side_effects=True, vmem_limit_bytes=67043328),
            name="half_layer",
        )(x, gain, freq, wq, wk, wv, wo)

    tokens, whole = P(("dp", "sp"), None), P("sp", None)
    return jax.shard_map(
        step,
        mesh=mesh,
        in_specs=(tokens, P(None), whole, whole, whole, whole),
        out_specs=tokens,
        check_vma=False,
    )
```
